32 devices in a mesh: slab: 16 (over z, x, core), grp: 2 (over y).
Axes of the slice: x: 2, y: 2, z: 4, core: 2. Of those that a mesh axis runs over, the one named last changes fastest.
Arguments:
- capture: float32 [2, 262144], P(None, ('slab', 'grp')), may hold values from -6 to 6
- dropped: int32 [16], P('slab'), may hold values from 0 to 8191
Outputs:
- max_held: float32 [128, 128, 128], P('slab', 'grp')
- coherent: float32 [2, 128, 128, 128], P(None, 'slab', 'grp')
The draws below stay inside these ranges and needn't reach their ends.
All inputs are finite; a program needn't handle non-finite values.
Results may differ from the reference program's by a relative error of at most 0.0001.
Values sent between devices are 32-bit elements; how exact they have to be, the bound alone decides.
No kernel may reach another device: no remote copies, remote signals or barrier semaphores. Data moves between devices by JAX's collectives and lax.ppermute only.
A program may use at most 128 MiB of HBM per device.

```python
import math
import jax
import jax.numpy as jnp
from jax import lax

NCH = 256
HOP = 64
KW = 128
LW = 128
Q = 128
BLOCKS = 2
SAMPLES = 262144
N_SLAB = 16


def set_ends(values, own_key, smallest, top_value):
    shape = values.shape
    place = [jax.random.randint(jax.random.fold_in(own_key, axis), (), 0, shape[axis]) for axis in range(len(shape))]
    values = values.at[tuple(place)].set(smallest)
    longest = shape.index(max(shape))
    place[longest] = (place[longest] + 1) % shape[longest]
    return values.at[tuple(place)].set(top_value)


def steps_of(rng, extent, pieces, low, high):
    def one(position, parts):
        draws = jax.random.uniform(jax.random.fold_in(jax.random.fold_in(rng, 6), position), (parts,), jnp.float32, low / len(pieces), high / len(pieces))
        return jnp.repeat(jnp.exp(draws), extent[position] // parts).reshape((-1,) + (1,) * (len(extent) - position - 1))

    loudness = one(*pieces[0])
    for cut in pieces[1:]:
        loudness = loudness * one(*cut)
    return loudness


def gaussian(rng, dims, scale, bound, pieces=(), kind=jnp.bfloat16):
    loudness = steps_of(rng, dims, pieces, -0.22, 0.18) if pieces else 1.0
    array = jax.random.normal(rng, dims, jnp.float32) * scale * loudness
    return jnp.minimum(jnp.maximum(array, -bound), bound).astype(kind)


def setup_inputs(seed: int = 0) -> dict:
    streams_of = jax.random.split(jax.random.key(seed), 3)
    return {
        "capture": gaussian(streams_of[0], (2, SAMPLES), 1.0, 6.0, ((1, 32),), jnp.float32),
        "dropped": set_ends(jax.random.randint(streams_of[1], (N_SLAB,), 0, Q * HOP), jax.random.fold_in(streams_of[1], 1), 0, (Q * HOP) - 1).astype(jnp.int32),
    }


def reference(capture, dropped):
    lead_hops = NCH // HOP - 1
    slab_hops = BLOCKS * Q
    total_hops = N_SLAB * slab_hops
    padded = jnp.concatenate([jnp.zeros((2, lead_hops * HOP), capture.dtype), capture], axis=1)
    hop_rows = padded.reshape(2, total_hops + lead_hops, HOP)
    frames = jnp.concatenate([hop_rows[:, lag_index:lag_index + total_hops] for lag_index in range(lead_hops + 1)], axis=2)
    tap_index = jnp.arange(NCH, dtype=jnp.int32).astype(jnp.float32)
    window = 0.5 - 0.5 * jnp.cos(2.0 * math.pi * tap_index / NCH)
    scaling = 1.0 / jnp.sqrt(jnp.sum(window * window))
    signal = lax.complex(frames[0] * window, frames[1] * window)
    spectra = jnp.fft.fft(signal, axis=-1)[:, :KW + LW] * scaling
    stamps = jnp.arange(N_SLAB, dtype=jnp.int32) * (BLOCKS * Q * HOP) + jnp.cumsum(dropped).astype(jnp.int32)
    hop_start = jnp.arange(slab_hops, dtype=jnp.int32) * HOP
    clock_mod = ((stamps[:, None] % NCH + hop_start[None, :]) % NCH).reshape(total_hops)
    channels = jnp.arange(KW + LW, dtype=jnp.int32)
    chan_turns = (clock_mod[:, None] * channels[None, :] % NCH).astype(jnp.float32) * (2.0 * math.pi / NCH)
    shifted = spectra * lax.complex(jnp.cos(chan_turns), -jnp.sin(chan_turns))
    shifted = shifted.reshape(N_SLAB, BLOCKS, Q, KW + LW)
    clock_period = Q * HOP
    freq_bins = jnp.arange(Q, dtype=jnp.int32)
    cycle_turns = (freq_bins[None, :] * (stamps % clock_period)[:, None] % clock_period).astype(jnp.float32) * (2.0 * math.pi / clock_period)
    rotation = lax.complex(jnp.cos(cycle_turns), -jnp.sin(cycle_turns))

    def accumulate(state_pair, slab_item):
        largest, running = state_pair
        slab_spectra, slab_rotation = slab_item
        lower_bank = slab_spectra[:, :, :KW]
        upper_bank = slab_spectra[:, :, KW:]
        products = lower_bank[:, :, :, None] * jnp.conj(upper_bank)[:, :, None, :]
        surfaces = jnp.fft.fft(products, axis=1) / math.sqrt(Q)
        largest = jnp.maximum(largest, lax.optimization_barrier(jnp.max(jnp.abs(surfaces), axis=0)))
        running = running + slab_rotation[:, None, None] * lax.optimization_barrier(jnp.sum(surfaces, axis=0))
        return ((largest, running), None)
    empty_surface = jnp.zeros((Q, KW, LW), jnp.float32)
    (largest, running), unused = lax.scan(accumulate, (empty_surface, lax.complex(empty_surface, empty_surface)), (shifted, rotation))
    norm_scale = 1.0 / math.sqrt(N_SLAB * BLOCKS)
    coherent = jnp.stack([jnp.real(running), jnp.imag(running)]) * norm_scale
    return (largest, coherent)
```

```python
import math

import jax
import jax.numpy as jnp
import ml_dtypes
import numpy as np
from jax import lax
from jax.experimental import pallas as pl
from jax.experimental.pallas import tpu as pltpu
from jax.sharding import PartitionSpec as P

NCH = 256
HOP = 64
KW = 128
LW = 128
Q = 128
BLOCKS = 2
PERIOD = Q * HOP
TURN = 2 * PERIOD
LANES = 128
PAD = 8


def halves(table):
    high = table.astype(ml_dtypes.bfloat16)
    low = (table - high.astype(np.float64)).astype(ml_dtypes.bfloat16)
    return high, low


def lower_order(width):
    quarter = width // 4
    return np.concatenate([4 * np.arange(quarter) + kappa for kappa in (0, 2, 1, 3)])


def upper_order():
    return np.concatenate([np.arange(0, LW, 2), np.arange(1, LW, 2)])


def window_rows():
    taps = np.arange(NCH)
    window = 0.5 - 0.5 * np.cos(2.0 * np.pi * taps / NCH)
    scaled = window / np.sqrt(np.sum(window * window))
    rows = np.zeros((8, LANES))
    for lag in range(NCH // HOP):
        piece = scaled[lag * HOP : (lag + 1) * HOP]
        rows[lag] = np.concatenate([piece, piece])
    return rows.astype(np.float32)


def channel_tables(groups):
    width = KW // groups
    half = width // 2
    taps = np.arange(NCH // 2)
    even = np.zeros((groups, NCH, NCH))
    odd = np.zeros((groups, NCH, NCH))

    def columns(channels):
        turns = 2.0 * np.pi * (taps[:, None] * channels[None, :] % NCH) / NCH
        cosine, sine = np.cos(turns), np.sin(turns)
        real = np.concatenate([cosine[:HOP], sine[:HOP], cosine[HOP:], sine[HOP:]])
        imag = np.concatenate([-sine[:HOP], cosine[:HOP], -sine[HOP:], cosine[HOP:]])
        return real, imag

    upper = KW + upper_order()
    for group in range(groups):
        lower = group * width + lower_order(width)
        real, imag = columns(upper[: LW // 2])
        even[group, :, 0:64], even[group, :, 64:128] = real, imag
        real, imag = columns(upper[LW // 2 :])
        odd[group, :, 0:64], odd[group, :, 64:128] = imag, real
        real, imag = columns(lower[:half])
        even[group, :, 128 : 128 + half] = real
        even[group, :, 192 : 192 + half] = imag
        real, imag = columns(lower[half:])
        odd[group, :, 128 + half : 128 + width] = real
        odd[group, :, 192 + half : 192 + width] = imag
    return halves(even) + halves(odd)


def turn_tables(bins, width):
    pairs = bins // 2
    rows = -(-(6 + pairs) // 8) * 8
    frame = np.arange(LANES)
    fixed = np.zeros((3, rows, LANES), np.int64)
    ticks = np.zeros((3, rows, LANES), np.int64)
    for place, kappa in enumerate((0, 2, 1, 3)):
        ticks[0, place] = bins - 1
        ticks[1, place] = 2 * bins
        fixed[0, place] = (bins - 1) * HOP * frame + (TURN // 4) * kappa * frame
        fixed[1, place] = 2 * bins * HOP * frame
    for pair in range(pairs):
        ticks[0, 4 + pair] = 2 * pair + 1
        fixed[0, 4 + pair] = (2 * pair + 1) * HOP * frame
    order = lower_order(width)
    scale = TURN // NCH
    ticks[0, 4 + pairs] = scale * np.concatenate([order, order])
    ticks[2, 4 + pairs] = scale * width
    ticks[0, 5 + pairs] = scale * (KW + upper_order())
    return fixed.astype(np.int32), ticks.astype(np.int32)


def cos_sin(angle):
    shifted = angle + TURN // 8
    quadrant = lax.shift_right_logical(shifted, int(math.log2(TURN // 4))) & 3
    remain = (shifted & (TURN // 4 - 1)) - TURN // 8
    x = remain.astype(jnp.float32) * np.float32(2.0 * math.pi / TURN)
    y = x * x
    sine = x * (1.0 + y * (-1.0 / 6 + y * (1.0 / 120 + y * (-1.0 / 5040 + y * (1.0 / 362880)))))
    cosine = 1.0 + y * (-0.5 + y * (1.0 / 24 + y * (-1.0 / 720 + y * (1.0 / 40320))))
    swap = (quadrant & 1) == 1
    out_cos = jnp.where(swap, sine, cosine)
    out_sin = jnp.where(swap, cosine, sine)
    out_cos = jnp.where((quadrant == 1) | (quadrant == 2), -out_cos, out_cos)
    out_sin = jnp.where(quadrant >= 2, -out_sin, out_sin)
    return out_cos, out_sin


def split(value):
    high = value.astype(jnp.bfloat16)
    low = (value - high.astype(jnp.float32)).astype(jnp.bfloat16)
    return high, low


def dot32(left, right):
    return lax.dot_general(
        left, right, (((1,), (0,)), ((), ())), preferred_element_type=jnp.float32
    )


def dot3(left, right):
    return dot32(left[0], right[0]) + dot32(left[1], right[0]) + dot32(left[0], right[1])


def surfaces(places, pieces, slabs, groups, piece_count):
    bins = Q // slabs
    pairs = bins // 2
    width = KW // groups
    blocks = slabs * BLOCKS
    fixed, ticks = turn_tables(bins, width)
    rows = fixed.shape[1]
    weights = channel_tables(groups)
    window = window_rows()
    arrays = len(pieces)
    depth = pieces[0].shape[0]
    order = KW + upper_order()
    phase = (np.arange(8)[:, None] * order[None, :]) % 4
    quarter_cos = np.array([1.0, 0.0, -1.0, 0.0])[phase].astype(np.float32)
    quarter_sin = np.array([0.0, 1.0, 0.0, -1.0])[phase].astype(np.float32)
    sign = np.where(np.arange(LANES) < width, 1.0, -1.0)[None, :].astype(np.float32)
    small = np.concatenate([window, quarter_cos, quarter_sin, np.tile(sign, (8, 1))])
    norm = 1.0 / math.sqrt(Q)
    blend = 1.0 / math.sqrt(slabs * BLOCKS)

    def kernel(place_ref, fixed_ref, ticks_ref, small_ref, even_h, even_l, odd_h, odd_l, *rest):
        piece_refs = rest[:arrays]
        held_ref, coherent_ref = rest[arrays : arrays + 2]
        frames, drops, cos_ref, sin_ref, acc_re, acc_im, acc_sq, sems = rest[arrays + 2 :]
        copies = []
        for array in range(arrays):
            for item in range(depth):
                number = array * depth + item
                place = place_ref[2 + number]
                start = pl.multiple_of(PAD + place * Q, 8)
                copies.append(
                    pltpu.make_async_copy(
                        piece_refs[array].at[item, pl.ds(0, Q)],
                        frames.at[pl.ds(start, Q)],
                        sems.at[0, number],
                    )
                )
                copies.append(
                    pltpu.make_async_copy(
                        piece_refs[array].at[item, pl.ds(Q, PAD)],
                        drops.at[pl.ds(pl.multiple_of(place * PAD, 8), PAD)],
                        sems.at[1, number],
                    )
                )
        for copy in copies:
            copy.start()
        frames[pl.ds(0, PAD), :] = jnp.zeros((PAD, LANES), jnp.float32)
        acc_re[...] = jnp.zeros_like(acc_re)
        acc_im[...] = jnp.zeros_like(acc_im)
        acc_sq[...] = jnp.zeros_like(acc_sq)
        slab = place_ref[0]
        group = place_ref[1]
        base = fixed_ref[0] + slab * fixed_ref[1] + group * fixed_ref[2]
        rate = ticks_ref[0] + slab * ticks_ref[1] + group * ticks_ref[2]
        for copy in copies:
            copy.wait()

        def stamp_step(n, total):
            dropped = drops[pl.ds(pl.multiple_of(n * BLOCKS * PAD, 8), PAD), :].astype(jnp.int32)
            total = (total + dropped) & (PERIOD - 1)
            wide = jnp.concatenate([total] * (rows // PAD), axis=0)
            cosine, sine = cos_sin((base + rate * wide) & (TURN - 1))
            at = pl.ds(pl.multiple_of(n * rows, 8), rows)
            cos_ref[at, :] = cosine
            sin_ref[at, :] = sine
            return total

        lax.fori_loop(0, slabs, stamp_step, jnp.zeros((PAD, LANES), jnp.int32))
        lane = lax.broadcasted_iota(jnp.int32, (Q, LANES), 1)
        left_half = lane < LANES // 2

        def slab_step(n, carry):
            cos_rows = cos_ref[pl.ds(pl.multiple_of(n * rows, 8), rows), :]
            sin_rows = sin_ref[pl.ds(pl.multiple_of(n * rows, 8), rows), :]
            row_k, row_l = 4 + pairs, 5 + pairs
            low_cos = cos_rows[row_k : row_k + 1]
            low_sin = sin_rows[row_k : row_k + 1] * small_ref[24:25]
            up_cos = cos_rows[row_l : row_l + 1]
            up_sin = sin_rows[row_l : row_l + 1]
            table_cos = small_ref[8:16] * up_cos - small_ref[16:24] * up_sin
            table_sin = small_ref[16:24] * up_cos + small_ref[8:16] * up_sin
            table_cos = jnp.concatenate([table_cos] * (Q // 8), axis=0)
            table_sin = jnp.concatenate([table_sin] * (Q // 8), axis=0)
            lhs = []
            rhs = []
            for block in range(BLOCKS):
                start = pl.multiple_of((n * BLOCKS + block) * Q, Q)
                lags = [
                    frames[pl.ds(start + (PAD - 3 + lag), Q), :] * small_ref[lag : lag + 1]
                    for lag in range(4)
                ]
                even = split(jnp.concatenate([lags[0] + lags[2], lags[1] + lags[3]], axis=1))
                odd = split(jnp.concatenate([lags[0] - lags[2], lags[1] - lags[3]], axis=1))
                from_even = dot3(even, (even_h[0], even_l[0]))
                from_odd = dot3(odd, (odd_h[0], odd_l[0]))
                up_even, up_odd = from_even[:, :LANES], from_odd[:, :LANES]
                up_re = jnp.where(left_half, up_even, up_odd)
                up_im = pltpu.roll(jnp.where(left_half, up_odd, up_even), LANES // 2, 1)
                re = up_re * table_cos + up_im * table_sin
                im = up_im * table_cos - up_re * table_sin
                re_h, re_l = split(re)
                im_h, im_l = split(im)
                right = []
                for real, imag in ((re_h, im_h), (re_l, im_l)):
                    top = jnp.concatenate([real, -imag], axis=1)
                    bottom = jnp.concatenate([imag, real], axis=1)
                    right.append(jnp.concatenate([top, bottom], axis=0))
                rhs.append(right)
                low = from_even[:, LANES:] + from_odd[:, LANES:]
                low = low * low_cos + pltpu.roll(low, LANES // 2, 1) * low_sin
                low = low.T * norm
                low_re, low_im = low[:width], low[width:]
                quarter = width // 4
                center_re = []
                center_im = []
                for place in range(4):
                    part = slice(place * quarter, (place + 1) * quarter)
                    c = cos_rows[place : place + 1]
                    s = sin_rows[place : place + 1]
                    center_re.append(low_re[part] * c + low_im[part] * s)
                    center_im.append(low_im[part] * c - low_re[part] * s)
                lhs.append((jnp.concatenate(center_re, axis=0), jnp.concatenate(center_im, axis=0)))
            for pair in range(pairs):
                c = cos_rows[4 + pair : 5 + pair]
                s = sin_rows[4 + pair : 5 + pair]
                above = (pairs + pair) * width
                below = (pairs - 1 - pair) * width
                sums = []
                for block in range(BLOCKS):
                    t1 = lhs[block][0] * c
                    t2 = lhs[block][1] * s
                    t3 = lhs[block][1] * c
                    t4 = lhs[block][0] * s
                    top = jnp.concatenate([t1 + t2, t3 - t4], axis=1)
                    bottom = jnp.concatenate([t1 - t2, t3 + t4], axis=1)
                    left = split(jnp.concatenate([top, bottom], axis=0))
                    sums.append(dot3(left, rhs[block]))
                total = sums[0] + sums[1]
                largest = jnp.maximum(
                    sums[0][:, :LW] * sums[0][:, :LW] + sums[0][:, LW:] * sums[0][:, LW:],
                    sums[1][:, :LW] * sums[1][:, :LW] + sums[1][:, LW:] * sums[1][:, LW:],
                )
                for side, at in enumerate((above, below)):
                    put = slice(at, at + width)
                    take = slice(side * width, (side + 1) * width)
                    acc_re[put] = acc_re[put] + total[take, :LW]
                    acc_im[put] = acc_im[put] + total[take, LW:]
                    acc_sq[put] = jnp.maximum(acc_sq[put], largest[take])
            return carry

        lax.fori_loop(0, slabs, slab_step, 0)
        quarter = width // 4
        lanes = lax.broadcasted_iota(jnp.int32, (quarter, LW), 1)
        source = lax.shift_right_logical(lanes, 1) + (LW // 2) * (lanes & 1)
        for bin_index in range(bins):
            for place, kappa in enumerate((0, 2, 1, 3)):
                take = slice(bin_index * width + place * quarter, bin_index * width + (place + 1) * quarter)
                put = pl.ds(kappa, quarter, stride=4)

                def natural(value):
                    return jnp.take_along_axis(value, source, axis=1, mode="promise_in_bounds")

                held_ref[bin_index, put, :] = natural(jnp.sqrt(acc_sq[take]))
                coherent_ref[0, bin_index, put, :] = natural(acc_re[take] * blend)
                coherent_ref[1, bin_index, put, :] = natural(acc_im[take] * blend)

    def whole(shape):
        return pl.BlockSpec(shape, lambda i, places: (0,) * len(shape))

    own = pl.BlockSpec((1, NCH, NCH), lambda i, places: (places[1], 0, 0))
    grid_spec = pltpu.PrefetchScalarGridSpec(
        num_scalar_prefetch=1,
        grid=(1,),
        in_specs=[whole(fixed.shape), whole(ticks.shape), whole(small.shape)]
        + [own] * 4
        + [pl.BlockSpec(memory_space=pl.ANY)] * arrays,
        out_specs=[whole((bins, width, LW)), whole((2, bins, width, LW))],
        scratch_shapes=[
            pltpu.VMEM((PAD + blocks * Q, LANES), jnp.float32),
            pltpu.VMEM((piece_count * PAD, LANES), jnp.float32),
            pltpu.VMEM((slabs * rows, LANES), jnp.float32),
            pltpu.VMEM((slabs * rows, LANES), jnp.float32),
            pltpu.VMEM((bins * width, LW), jnp.float32),
            pltpu.VMEM((bins * width, LW), jnp.float32),
            pltpu.VMEM((bins * width, LW), jnp.float32),
            pltpu.SemaphoreType.DMA((2, piece_count)),
        ],
    )
    return pl.pallas_call(
        kernel,
        grid_spec=grid_spec,
        out_shape=[
            jax.ShapeDtypeStruct((bins, width, LW), jnp.float32),
            jax.ShapeDtypeStruct((2, bins, width, LW), jnp.float32),
        ],
        compiler_params=pltpu.CompilerParams(vmem_limit_bytes=48 * 1024 * 1024),
        name="surfaces",
    )(
        places,
        jnp.asarray(fixed),
        jnp.asarray(ticks),
        jnp.asarray(small),
        *[jnp.asarray(table) for table in weights],
        *pieces,
    )


def on_device(capture, dropped):
    slabs = lax.axis_size("slab")
    groups = lax.axis_size("grp")
    slab = lax.axis_index("slab")
    group = lax.axis_index("grp")
    axes = ("slab", "grp")
    total = slabs * groups
    outer = slabs // 4
    hops = capture.shape[1] // HOP
    own = capture.reshape(2, hops, HOP).transpose(1, 0, 2).reshape(hops, 2 * HOP)
    ticks = jnp.broadcast_to(dropped.astype(jnp.float32)[:, None], (PAD, LANES))
    own = jnp.concatenate([own, ticks], axis=0)[None]

    def split_index(flat):
        return flat // (4 * groups), (flat // (2 * groups)) % 2, (flat // groups) % 2, flat % groups

    def joined(far, side, core, member):
        return ((far * 2 + side) * 2 + core) * groups + member

    def moved(array, by):
        pairs = []
        for flat in range(total):
            far, side, core, member = split_index(flat)
            target = joined(
                (far + by[0]) % outer, (side + by[1]) % 2, (core + by[2]) % 2, (member + by[3]) % groups
            )
            pairs.append((flat, target))
        return lax.ppermute(array, axes, pairs)

    line = [own] + [moved(own, (step, 0, 0, 0)) for step in range(1, outer)]
    line = jnp.concatenate(line, axis=0)
    steps = [(side, member) for member in range(groups) for side in range(2)]
    arrays = []
    offsets = []
    for side, member in steps:
        arrays.append(moved(line, (0, side, 0, member)) if (side, member) != (0, 0) else line)
        offsets.append((side, 0, member))
    for index, (side, member) in enumerate(steps):
        arrays.append(moved(arrays[index], (0, 0, 1, 0)))
        offsets.append((side, 1, member))
    me_far, me_side, me_core, me_member = split_index(slab * groups + group)
    places = [slab, group]
    for side, core, member in offsets:
        for step in range(outer):
            places.append(
                joined(
                    (me_far - step) % outer,
                    (me_side - side) % 2,
                    (me_core - core) % 2,
                    (me_member - member) % groups,
                )
            )
    places = jnp.stack([jnp.asarray(place, jnp.int32) for place in places])
    held, coherent = surfaces(places, arrays, slabs, groups, total)
    return held, coherent


def solution(mesh):
    in_specs = (P(None, ("slab", "grp")), P("slab"))
    out_specs = (P("slab", "grp", None), P(None, "slab", "grp", None))
    return jax.shard_map(
        on_device, mesh=mesh, in_specs=in_specs, out_specs=out_specs, check_vma=False
    )
```

```python
import math

import jax
import jax.numpy as jnp
import ml_dtypes
import numpy as np
from jax import lax
from jax.experimental import pallas as pl
from jax.experimental.pallas import tpu as pltpu
from jax.sharding import PartitionSpec as P

NCH = 256
HOP = 64
KW = 128
LW = 128
Q = 128
BLOCKS = 2
PERIOD = Q * HOP
TURN = 2 * PERIOD
LANES = 128
PAD = 8


def halves(table):
    high = table.astype(ml_dtypes.bfloat16)
    low = (table - high.astype(np.float64)).astype(ml_dtypes.bfloat16)
    return high, low


def lower_order(width):
    quarter = width // 4
    return np.concatenate([4 * np.arange(quarter) + kappa for kappa in (0, 2, 1, 3)])


def upper_order():
    return np.concatenate([np.arange(0, LW, 2), np.arange(1, LW, 2)])


def window_rows():
    taps = np.arange(NCH)
    window = 0.5 - 0.5 * np.cos(2.0 * np.pi * taps / NCH)
    scaled = window / np.sqrt(np.sum(window * window))
    rows = np.zeros((8, LANES))
    for lag in range(NCH // HOP):
        piece = scaled[lag * HOP : (lag + 1) * HOP]
        rows[lag] = np.concatenate([piece, piece])
    return rows.astype(np.float32)


def channel_tables(groups):
    width = KW // groups
    half = width // 2
    taps = np.arange(NCH // 2)
    even = np.zeros((groups, NCH, NCH))
    odd = np.zeros((groups, NCH, NCH))

    def columns(channels):
        turns = 2.0 * np.pi * (taps[:, None] * channels[None, :] % NCH) / NCH
        cosine, sine = np.cos(turns), np.sin(turns)
        real = np.concatenate([cosine[:HOP], sine[:HOP], cosine[HOP:], sine[HOP:]])
        imag = np.concatenate([-sine[:HOP], cosine[:HOP], -sine[HOP:], cosine[HOP:]])
        return real, imag

    upper = KW + upper_order()
    for group in range(groups):
        lower = group * width + lower_order(width)
        real, imag = columns(upper[: LW // 2])
        even[group, :, 0:64], even[group, :, 64:128] = real, imag
        real, imag = columns(upper[LW // 2 :])
        odd[group, :, 0:64], odd[group, :, 64:128] = imag, real
        real, imag = columns(lower[:half])
        even[group, :, 128 : 128 + half] = real
        even[group, :, 192 : 192 + half] = imag
        real, imag = columns(lower[half:])
        odd[group, :, 128 + half : 128 + width] = real
        odd[group, :, 192 + half : 192 + width] = imag
    return halves(even) + halves(odd)


def turn_tables(bins, width):
    pairs = bins // 2
    rows = -(-(6 + pairs) // 8) * 8
    frame = np.arange(LANES)
    fixed = np.zeros((3, rows, LANES), np.int64)
    ticks = np.zeros((3, rows, LANES), np.int64)
    for place, kappa in enumerate((0, 2, 1, 3)):
        ticks[0, place] = bins - 1
        ticks[1, place] = 2 * bins
        fixed[0, place] = (bins - 1) * HOP * frame + (TURN // 4) * kappa * frame
        fixed[1, place] = 2 * bins * HOP * frame
    for pair in range(pairs):
        ticks[0, 4 + pair] = 2 * pair + 1
        fixed[0, 4 + pair] = (2 * pair + 1) * HOP * frame
    order = lower_order(width)
    scale = TURN // NCH
    ticks[0, 4 + pairs] = scale * np.concatenate([order, order])
    ticks[2, 4 + pairs] = scale * width
    ticks[0, 5 + pairs] = scale * (KW + upper_order())
    return fixed.astype(np.int32), ticks.astype(np.int32)


def cos_sin(angle):
    shifted = angle + TURN // 8
    quadrant = lax.shift_right_logical(shifted, int(math.log2(TURN // 4))) & 3
    remain = (shifted & (TURN // 4 - 1)) - TURN // 8
    x = remain.astype(jnp.float32) * np.float32(2.0 * math.pi / TURN)
    y = x * x
    sine = x * (1.0 + y * (-1.0 / 6 + y * (1.0 / 120 + y * (-1.0 / 5040 + y * (1.0 / 362880)))))
    cosine = 1.0 + y * (-0.5 + y * (1.0 / 24 + y * (-1.0 / 720 + y * (1.0 / 40320))))
    swap = (quadrant & 1) == 1
    out_cos = jnp.where(swap, sine, cosine)
    out_sin = jnp.where(swap, cosine, sine)
    out_cos = jnp.where((quadrant == 1) | (quadrant == 2), -out_cos, out_cos)
    out_sin = jnp.where(quadrant >= 2, -out_sin, out_sin)
    return out_cos, out_sin


def split(value):
    high = value.astype(jnp.bfloat16)
    low = (value - high.astype(jnp.float32)).astype(jnp.bfloat16)
    return high, low


def dot32(left, right):
    return lax.dot_general(
        left, right, (((1,), (0,)), ((), ())), preferred_element_type=jnp.float32
    )


def dot3(left, right):
    return dot32(left[0], right[0]) + dot32(left[1], right[0]) + dot32(left[0], right[1])


def small_table(width):
    order = KW + upper_order()
    phase = (np.arange(8)[:, None] * order[None, :]) % 4
    quarter_cos = np.array([1.0, 0.0, -1.0, 0.0])[phase]
    quarter_sin = np.array([0.0, 1.0, 0.0, -1.0])[phase]
    sign = np.where(np.arange(LANES) < width, 1.0, -1.0)[None, :]
    parts = [window_rows(), quarter_cos, quarter_sin, np.tile(sign, (8, 1))]
    return np.concatenate(parts).astype(np.float32)


def packed(capture, dropped):
    hops = capture.shape[1] // HOP
    rows = capture.reshape(2, hops // 2, LANES).transpose(1, 0, 2).reshape(hops, LANES)

    def kernel(ticks_ref, rows_ref, out_ref):
        value = rows_ref[...]
        row = lax.broadcasted_iota(jnp.int32, value.shape, 0)
        lane = lax.broadcasted_iota(jnp.int32, value.shape, 1)
        turned = pltpu.roll(value, LANES // 2, 1)
        odd = (row & 1) == 1
        other = jnp.where(odd, pltpu.roll(turned, 1, 0), pltpu.roll(turned, hops - 1, 0))
        keep = odd == (lane >= LANES // 2)
        out_ref[0, pl.ds(0, hops), :] = jnp.where(keep, value, other)
        out_ref[0, pl.ds(hops, PAD), :] = jnp.full((PAD, LANES), ticks_ref[0], jnp.int32).astype(
            jnp.float32
        )

    return pl.pallas_call(
        kernel,
        in_specs=[
            pl.BlockSpec(memory_space=pltpu.SMEM),
            pl.BlockSpec(memory_space=pltpu.VMEM),
        ],
        out_specs=pl.BlockSpec(memory_space=pltpu.VMEM),
        out_shape=jax.ShapeDtypeStruct((1, hops + PAD, LANES), jnp.float32),
        name="packed",
    )(dropped, rows)


def surfaces(plan, pieces, slabs, groups, count):
    bins = Q // slabs
    pairs = bins // 2
    width = KW // groups
    quarter = width // 4
    blocks = slabs * BLOCKS
    fixed, ticks = turn_tables(bins, width)
    rows = fixed.shape[1]
    weights = channel_tables(groups)
    small = small_table(width)
    arrays = len(pieces)
    depth = pieces[0].shape[0]
    norm = 1.0 / math.sqrt(Q)
    blend = 1.0 / math.sqrt(slabs * BLOCKS)
    first_block = 2 + arrays * depth

    def kernel(plan_ref, fixed_ref, ticks_ref, small_ref, even_h, even_l, odd_h, odd_l, *rest):
        piece_refs = rest[:arrays]
        held_ref, coherent_ref = rest[arrays : arrays + 2]
        frames, drops, cos_ref, sin_ref, acc_re, acc_im, acc_sq = rest[arrays + 2 : arrays + 9]
        slots = (rest[arrays + 9 : arrays + 13], rest[arrays + 13 : arrays + 17])
        slab = plan_ref[0]
        group = plan_ref[1]
        frames[pl.ds(0, PAD), :] = jnp.zeros((PAD, LANES), jnp.float32)
        for array in range(arrays):
            for item in range(depth):
                place = plan_ref[2 + array * depth + item]
                start = pl.multiple_of(PAD + place * Q, 8)
                frames[pl.ds(start, Q), :] = piece_refs[array][item, pl.ds(0, Q), :]
                start = pl.multiple_of(place * PAD, 8)
                drops[pl.ds(start, PAD), :] = piece_refs[array][item, pl.ds(Q, PAD), :]
        acc_re[...] = jnp.zeros_like(acc_re)
        acc_im[...] = jnp.zeros_like(acc_im)
        acc_sq[...] = jnp.zeros_like(acc_sq)
        base = fixed_ref[0] + slab * fixed_ref[1] + group * fixed_ref[2]
        rate = ticks_ref[0] + slab * ticks_ref[1] + group * ticks_ref[2]

        def stamp_step(n, total):
            dropped = drops[pl.ds(pl.multiple_of(n * BLOCKS * PAD, 8), PAD), :].astype(jnp.int32)
            total = (total + dropped) & (PERIOD - 1)
            wide = jnp.concatenate([total] * (rows // PAD), axis=0)
            cosine, sine = cos_sin((base + rate * wide) & (TURN - 1))
            at = pl.ds(pl.multiple_of(n * rows, 8), rows)
            cos_ref[at, :] = cosine
            sin_ref[at, :] = sine
            return total

        lax.fori_loop(0, slabs, stamp_step, jnp.zeros((PAD, LANES), jnp.int32))
        lane = lax.broadcasted_iota(jnp.int32, (Q, LANES), 1)
        left_half = lane < LANES // 2

        def channelize(place, slot):
            rhs_h, rhs_l, center_re, center_im = slot
            turn = pl.multiple_of((place // BLOCKS) * rows, 8)
            cos_rows = cos_ref[pl.ds(turn, rows), :]
            sin_rows = sin_ref[pl.ds(turn, rows), :]
            row_k, row_l = 4 + pairs, 5 + pairs
            low_cos = cos_rows[row_k : row_k + 1]
            low_sin = sin_rows[row_k : row_k + 1] * small_ref[24:25]
            up_cos = cos_rows[row_l : row_l + 1]
            up_sin = sin_rows[row_l : row_l + 1]
            table_cos = small_ref[8:16] * up_cos - small_ref[16:24] * up_sin
            table_sin = small_ref[16:24] * up_cos + small_ref[8:16] * up_sin
            table_cos = jnp.concatenate([table_cos] * (Q // 8), axis=0)
            table_sin = jnp.concatenate([table_sin] * (Q // 8), axis=0)
            start = pl.multiple_of(place * Q, Q)
            lags = [
                frames[pl.ds(start + (PAD - 3 + lag), Q), :] * small_ref[lag : lag + 1]
                for lag in range(4)
            ]
            even = split(jnp.concatenate([lags[0] + lags[2], lags[1] + lags[3]], axis=1))
            odd = split(jnp.concatenate([lags[0] - lags[2], lags[1] - lags[3]], axis=1))
            from_even = dot3(even, (even_h[group], even_l[group]))
            from_odd = dot3(odd, (odd_h[group], odd_l[group]))
            up_even, up_odd = from_even[:, :LANES], from_odd[:, :LANES]
            up_re = jnp.where(left_half, up_even, up_odd)
            up_im = pltpu.roll(jnp.where(left_half, up_odd, up_even), LANES // 2, 1)
            re_h, re_l = split(up_re * table_cos + up_im * table_sin)
            im_h, im_l = split(up_im * table_cos - up_re * table_sin)
            for ref, real, imag in ((rhs_h, re_h, im_h), (rhs_l, re_l, im_l)):
                ref[0:Q, 0:LW] = real
                ref[0:Q, LW : 2 * LW] = -imag
                ref[Q : 2 * Q, 0:LW] = imag
                ref[Q : 2 * Q, LW : 2 * LW] = real
            low = from_even[:, LANES:] + from_odd[:, LANES:]
            low = low * low_cos + pltpu.roll(low, LANES // 2, 1) * low_sin
            low = low.T * norm
            low_re, low_im = low[:width], low[width:]
            for part in range(4):
                at = slice(part * quarter, (part + 1) * quarter)
                c = cos_rows[part : part + 1]
                s = sin_rows[part : part + 1]
                center_re[at] = low_re[at] * c + low_im[at] * s
                center_im[at] = low_im[at] * c - low_re[at] * s

        def correlate(place, slot):
            rhs_h, rhs_l, center_re, center_im = slot
            turn = pl.multiple_of((place // BLOCKS) * rows, 8)
            cos_rows = cos_ref[pl.ds(turn, rows), :]
            sin_rows = sin_ref[pl.ds(turn, rows), :]
            right = (rhs_h[...], rhs_l[...])
            for pair in range(pairs):
                c = cos_rows[4 + pair : 5 + pair]
                s = sin_rows[4 + pair : 5 + pair]
                above = (pairs + pair) * width
                below = (pairs - 1 - pair) * width
                t1 = center_re[...] * c
                t2 = center_im[...] * s
                t3 = center_im[...] * c
                t4 = center_re[...] * s
                top = jnp.concatenate([t1 + t2, t3 - t4], axis=1)
                bottom = jnp.concatenate([t1 - t2, t3 + t4], axis=1)
                left = split(jnp.concatenate([top, bottom], axis=0))
                total = dot3(left, right)
                for side, at in enumerate((above, below)):
                    put = slice(at, at + width)
                    re = total[side * width : (side + 1) * width, :LW]
                    im = total[side * width : (side + 1) * width, LW:]
                    acc_re[put] = acc_re[put] + re
                    acc_im[put] = acc_im[put] + im
                    acc_sq[put] = jnp.maximum(acc_sq[put], re * re + im * im)

        def block_at(index):
            return plan_ref[first_block + jnp.minimum(index, count - 1)]

        channelize(block_at(0), slots[0])

        def step(index, carry):
            for side in range(2):
                correlate(block_at(2 * index + side), slots[side])
                channelize(block_at(2 * index + side + 1), slots[1 - side])
            return carry

        lax.fori_loop(0, count // 2, step, 0)
        lanes = lax.broadcasted_iota(jnp.int32, (quarter, LW), 1)
        source = lax.shift_right_logical(lanes, 1) + (LW // 2) * (lanes & 1)

        def natural(value):
            return jnp.take_along_axis(value, source, axis=1, mode="promise_in_bounds")

        for bin_index in range(bins):
            for part, kappa in enumerate((0, 2, 1, 3)):
                first = bin_index * width + part * quarter
                take = slice(first, first + quarter)
                put = pl.ds(kappa, quarter, stride=4)
                held_ref[bin_index, put, :] = natural(jnp.sqrt(acc_sq[take]))
                coherent_ref[0, bin_index, put, :] = natural(acc_re[take] * blend)
                coherent_ref[1, bin_index, put, :] = natural(acc_im[take] * blend)

    vmem = pl.BlockSpec(memory_space=pltpu.VMEM)
    slot = [
        pltpu.VMEM((2 * Q, 2 * LW), jnp.bfloat16),
        pltpu.VMEM((2 * Q, 2 * LW), jnp.bfloat16),
        pltpu.VMEM((width, Q), jnp.float32),
        pltpu.VMEM((width, Q), jnp.float32),
    ]
    return pl.pallas_call(
        kernel,
        in_specs=[pl.BlockSpec(memory_space=pltpu.SMEM)] + [vmem] * (7 + arrays),
        out_specs=[vmem, vmem],
        scratch_shapes=[
            pltpu.VMEM((PAD + blocks * Q, LANES), jnp.float32),
            pltpu.VMEM((blocks * PAD, LANES), jnp.float32),
            pltpu.VMEM((slabs * rows, LANES), jnp.float32),
            pltpu.VMEM((slabs * rows, LANES), jnp.float32),
            pltpu.VMEM((bins * width, LW), jnp.float32),
            pltpu.VMEM((bins * width, LW), jnp.float32),
            pltpu.VMEM((bins * width, LW), jnp.float32),
        ]
        + slot
        + slot,
        out_shape=[
            jax.ShapeDtypeStruct((bins, width, LW), jnp.float32),
            jax.ShapeDtypeStruct((2, bins, width, LW), jnp.float32),
        ],
        compiler_params=pltpu.CompilerParams(vmem_limit_bytes=48 * 1024 * 1024),
        name="surfaces",
    )(
        plan,
        jnp.asarray(fixed),
        jnp.asarray(ticks),
        jnp.asarray(small),
        *[jnp.asarray(table) for table in weights],
        *pieces,
    )


def on_device(capture, dropped):
    slabs = lax.axis_size("slab")
    groups = lax.axis_size("grp")
    slab = lax.axis_index("slab")
    group = lax.axis_index("grp")
    axes = ("slab", "grp")
    total = slabs * groups
    outer = slabs // 4
    own = packed(capture, dropped)

    def split_index(flat):
        return flat // (4 * groups), (flat // (2 * groups)) % 2, (flat // groups) % 2, flat % groups

    def joined(far, side, core, member):
        return ((far * 2 + side) * 2 + core) * groups + member

    def moved(array, by):
        pairs = []
        for flat in range(total):
            far, side, core, member = split_index(flat)
            target = joined(
                (far + by[0]) % outer, (side + by[1]) % 2, (core + by[2]) % 2, (member + by[3]) % groups
            )
            pairs.append((flat, target))
        return lax.ppermute(array, axes, pairs)

    line = [own] + [moved(own, (step, 0, 0, 0)) for step in range(1, outer)]
    line = jnp.concatenate(line, axis=0)
    steps = [(side, member) for member in range(groups) for side in range(2)]
    arrays = []
    offsets = []
    for side, member in steps:
        arrays.append(moved(line, (0, side, 0, member)) if (side, member) != (0, 0) else line)
        offsets.append((side, 0, member))
    for index, (side, member) in enumerate(steps):
        arrays.append(moved(arrays[index], (0, 0, 1, 0)))
        offsets.append((side, 1, member))
    me_far, me_side, me_core, me_member = split_index(slab * groups + group)
    places = [slab, group]
    for side, core, member in offsets:
        for step in range(outer):
            places.append(
                joined(
                    (me_far - step) % outer,
                    (me_side - side) % 2,
                    (me_core - core) % 2,
                    (me_member - member) % groups,
                )
            )
    places += list(range(total))
    plan = jnp.stack([jnp.asarray(place, jnp.int32) for place in places])
    held, coherent = surfaces(plan, arrays, slabs, groups, total)
    return held, coherent


def solution(mesh):
    in_specs = (P(None, ("slab", "grp")), P("slab"))
    out_specs = (P("slab", "grp", None), P(None, "slab", "grp", None))
    return jax.shard_map(
        on_device, mesh=mesh, in_specs=in_specs, out_specs=out_specs, check_vma=False
    )
```

```python
import math

import jax
import jax.numpy as jnp
import ml_dtypes
import numpy as np
from jax import lax
from jax.experimental import pallas as pl
from jax.experimental.pallas import tpu as pltpu
from jax.sharding import PartitionSpec as P

NCH = 256
HOP = 64
KW = 128
LW = 128
Q = 128
BLOCKS = 2
PERIOD = Q * HOP
TURN = 2 * PERIOD
LANES = 128
PAD = 8


def halves(table):
    high = table.astype(ml_dtypes.bfloat16)
    low = (table - high.astype(np.float64)).astype(ml_dtypes.bfloat16)
    return high, low


def lower_order(width):
    quarter = width // 4
    return np.concatenate([4 * np.arange(quarter) + kappa for kappa in (0, 2, 1, 3)])


def upper_order():
    return np.concatenate([np.arange(0, LW, 2), np.arange(1, LW, 2)])


def window_rows():
    taps = np.arange(NCH)
    window = 0.5 - 0.5 * np.cos(2.0 * np.pi * taps / NCH)
    scaled = window / np.sqrt(np.sum(window * window))
    rows = np.zeros((8, LANES))
    for lag in range(NCH // HOP):
        piece = scaled[lag * HOP : (lag + 1) * HOP]
        rows[lag] = np.concatenate([piece, piece])
    return rows.astype(np.float32)


def channel_tables(groups):
    width = KW // groups
    half = width // 2
    taps = np.arange(NCH // 2)
    even = np.zeros((groups, NCH, NCH))
    odd = np.zeros((groups, NCH, NCH))

    def columns(channels):
        turns = 2.0 * np.pi * (taps[:, None] * channels[None, :] % NCH) / NCH
        cosine, sine = np.cos(turns), np.sin(turns)
        real = np.concatenate([cosine[:HOP], sine[:HOP], cosine[HOP:], sine[HOP:]])
        imag = np.concatenate([-sine[:HOP], cosine[:HOP], -sine[HOP:], cosine[HOP:]])
        return real, imag

    upper = KW + upper_order()
    for group in range(groups):
        lower = group * width + lower_order(width)
        real, imag = columns(upper[: LW // 2])
        even[group, :, 0:64], even[group, :, 64:128] = real, imag
        real, imag = columns(upper[LW // 2 :])
        odd[group, :, 0:64], odd[group, :, 64:128] = imag, real
        real, imag = columns(lower[:half])
        even[group, :, 128 : 128 + half] = real
        even[group, :, 192 : 192 + half] = imag
        real, imag = columns(lower[half:])
        odd[group, :, 128 + half : 128 + width] = real
        odd[group, :, 192 + half : 192 + width] = imag
    return halves(even) + halves(odd)


def turn_tables(bins, width):
    pairs = bins // 2
    rows = -(-(6 + pairs) // 8) * 8
    frame = np.arange(LANES)
    fixed = np.zeros((3, rows, LANES), np.int64)
    ticks = np.zeros((3, rows, LANES), np.int64)
    for place, kappa in enumerate((0, 2, 1, 3)):
        ticks[0, place] = bins - 1
        ticks[1, place] = 2 * bins
        fixed[0, place] = (bins - 1) * HOP * frame + (TURN // 4) * kappa * frame
        fixed[1, place] = 2 * bins * HOP * frame
    for pair in range(pairs):
        ticks[0, 4 + pair] = 2 * pair + 1
        fixed[0, 4 + pair] = (2 * pair + 1) * HOP * frame
    order = lower_order(width)
    scale = TURN // NCH
    ticks[0, 4 + pairs] = scale * np.concatenate([order, order])
    ticks[2, 4 + pairs] = scale * width
    ticks[0, 5 + pairs] = scale * (KW + upper_order())
    return fixed.astype(np.int32), ticks.astype(np.int32)


def cos_sin(angle):
    shifted = angle + TURN // 8
    quadrant = lax.shift_right_logical(shifted, int(math.log2(TURN // 4))) & 3
    remain = (shifted & (TURN // 4 - 1)) - TURN // 8
    x = remain.astype(jnp.float32) * np.float32(2.0 * math.pi / TURN)
    y = x * x
    sine = x * (1.0 + y * (-1.0 / 6 + y * (1.0 / 120 + y * (-1.0 / 5040 + y * (1.0 / 362880)))))
    cosine = 1.0 + y * (-0.5 + y * (1.0 / 24 + y * (-1.0 / 720 + y * (1.0 / 40320))))
    swap = (quadrant & 1) == 1
    out_cos = jnp.where(swap, sine, cosine)
    out_sin = jnp.where(swap, cosine, sine)
    out_cos = jnp.where((quadrant == 1) | (quadrant == 2), -out_cos, out_cos)
    out_sin = jnp.where(quadrant >= 2, -out_sin, out_sin)
    return out_cos, out_sin


def split(value):
    high = value.astype(jnp.bfloat16)
    low = (value - high.astype(jnp.float32)).astype(jnp.bfloat16)
    return high, low


def dot32(left, right):
    return lax.dot_general(
        left, right, (((1,), (0,)), ((), ())), preferred_element_type=jnp.float32
    )


def dot3(left, right):
    return dot32(left[0], right[0]) + dot32(left[1], right[0]) + dot32(left[0], right[1])


def small_table(width):
    order = KW + upper_order()
    phase = (np.arange(8)[:, None] * order[None, :]) % 4
    quarter_cos = np.array([1.0, 0.0, -1.0, 0.0])[phase]
    quarter_sin = np.array([0.0, 1.0, 0.0, -1.0])[phase]
    sign = np.where(np.arange(LANES) < width, 1.0, -1.0)[None, :]
    parts = [window_rows(), quarter_cos, quarter_sin, np.tile(sign, (8, 1))]
    return np.concatenate(parts).astype(np.float32)


def packed(capture, dropped):
    hops = capture.shape[1] // HOP
    rows = capture.reshape(2, hops // 2, LANES).transpose(1, 0, 2).reshape(hops, LANES)

    def kernel(ticks_ref, rows_ref, out_ref):
        value = rows_ref[...]
        row = lax.broadcasted_iota(jnp.int32, value.shape, 0)
        lane = lax.broadcasted_iota(jnp.int32, value.shape, 1)
        turned = pltpu.roll(value, LANES // 2, 1)
        odd = (row & 1) == 1
        other = jnp.where(odd, pltpu.roll(turned, 1, 0), pltpu.roll(turned, hops - 1, 0))
        keep = odd == (lane >= LANES // 2)
        out_ref[0, pl.ds(0, hops), :] = jnp.where(keep, value, other)
        out_ref[0, pl.ds(hops, PAD), :] = jnp.full((PAD, LANES), ticks_ref[0], jnp.int32).astype(
            jnp.float32
        )

    return pl.pallas_call(
        kernel,
        in_specs=[
            pl.BlockSpec(memory_space=pltpu.SMEM),
            pl.BlockSpec(memory_space=pltpu.VMEM),
        ],
        out_specs=pl.BlockSpec(memory_space=pltpu.VMEM),
        out_shape=jax.ShapeDtypeStruct((1, hops + PAD, LANES), jnp.float32),
        name="packed",
    )(dropped, rows)


def surfaces(plan, pieces, slabs, groups, count, notes=(), carried=None):
    bins = Q // slabs
    pairs = bins // 2
    width = KW // groups
    quarter = width // 4
    blocks = slabs * BLOCKS
    fixed, ticks = turn_tables(bins, width)
    rows = fixed.shape[1]
    weights = channel_tables(groups)
    small = small_table(width)
    arrays = len(pieces)
    depth = pieces[0].shape[0]
    norm = 1.0 / math.sqrt(Q)
    blend = 1.0 / math.sqrt(slabs * BLOCKS)
    first_block = 2 + (arrays + len(notes)) * depth
    opening = carried is None
    inputs = arrays + len(notes) + (0 if opening else 5)
    outputs = 5 if opening else 2

    def kernel(plan_ref, fixed_ref, ticks_ref, small_ref, even_h, even_l, odd_h, odd_l, *rest):
        piece_refs = rest[:arrays]
        note_refs = rest[arrays : arrays + len(notes)]
        out_refs = rest[inputs : inputs + outputs]
        rest = rest[inputs + outputs :] if opening else rest[arrays:]
        if opening:
            acc_re, acc_im, acc_sq, cos_ref, sin_ref = out_refs
            frames, drops = rest[:2]
            scratch = rest[2:]
        else:
            old_re, old_im, old_sq, cos_ref, sin_ref = rest[:5]
            held_ref, coherent_ref = out_refs
            frames, acc_re, acc_im, acc_sq = rest[7:11]
            scratch = rest[11:]
        slots = (scratch[0:4], scratch[4:8])
        slab = plan_ref[0]
        group = plan_ref[1]
        frames[pl.ds(0, PAD), :] = jnp.zeros((PAD, LANES), jnp.float32)
        for array in range(arrays):
            for item in range(depth):
                place = plan_ref[2 + array * depth + item]
                start = pl.multiple_of(PAD + place * Q, 8)
                frames[pl.ds(start, Q), :] = piece_refs[array][item, pl.ds(0, Q), :]
                if opening:
                    start = pl.multiple_of(place * PAD, 8)
                    drops[pl.ds(start, PAD), :] = piece_refs[array][item, pl.ds(Q, PAD), :]
        def make_turns():
            for array in range(len(notes)):
                for item in range(depth):
                    place = plan_ref[2 + (arrays + array) * depth + item]
                    start = pl.multiple_of((place // BLOCKS) * BLOCKS * PAD, 8)
                    drops[pl.ds(start, PAD), :] = note_refs[array][item]
            base = fixed_ref[0] + slab * fixed_ref[1] + group * fixed_ref[2]
            rate = ticks_ref[0] + slab * ticks_ref[1] + group * ticks_ref[2]

            def stamp_step(n, total):
                at = pl.ds(pl.multiple_of(n * BLOCKS * PAD, 8), PAD)
                total = (total + drops[at, :].astype(jnp.int32)) & (PERIOD - 1)
                wide = jnp.concatenate([total] * (rows // PAD), axis=0)
                cosine, sine = cos_sin((base + rate * wide) & (TURN - 1))
                at = pl.ds(pl.multiple_of(n * rows, 8), rows)
                cos_ref[at, :] = cosine
                sin_ref[at, :] = sine
                return total

            lax.fori_loop(0, slabs, stamp_step, jnp.zeros((PAD, LANES), jnp.int32), unroll=4)

        if opening:
            acc_re[...] = jnp.zeros_like(acc_re)
            acc_im[...] = jnp.zeros_like(acc_im)
            acc_sq[...] = jnp.zeros_like(acc_sq)
            make_turns()
        else:
            acc_re[...] = old_re[...]
            acc_im[...] = old_im[...]
            acc_sq[...] = old_sq[...]
        lane = lax.broadcasted_iota(jnp.int32, (Q, LANES), 1)
        left_half = lane < LANES // 2

        def channelize(place, slot):
            rhs_h, rhs_l, center_re, center_im = slot
            turn = pl.multiple_of((place // BLOCKS) * rows, 8)
            cos_rows = cos_ref[pl.ds(turn, rows), :]
            sin_rows = sin_ref[pl.ds(turn, rows), :]
            row_k, row_l = 4 + pairs, 5 + pairs
            low_cos = cos_rows[row_k : row_k + 1]
            low_sin = sin_rows[row_k : row_k + 1] * small_ref[24:25]
            up_cos = cos_rows[row_l : row_l + 1]
            up_sin = sin_rows[row_l : row_l + 1]
            table_cos = small_ref[8:16] * up_cos - small_ref[16:24] * up_sin
            table_sin = small_ref[16:24] * up_cos + small_ref[8:16] * up_sin
            table_cos = jnp.concatenate([table_cos] * (Q // 8), axis=0)
            table_sin = jnp.concatenate([table_sin] * (Q // 8), axis=0)
            start = pl.multiple_of(place * Q, Q)
            lags = [
                frames[pl.ds(start + (PAD - 3 + lag), Q), :] * small_ref[lag : lag + 1]
                for lag in range(4)
            ]
            even = split(jnp.concatenate([lags[0] + lags[2], lags[1] + lags[3]], axis=1))
            odd = split(jnp.concatenate([lags[0] - lags[2], lags[1] - lags[3]], axis=1))
            from_even = dot3(even, (even_h[group], even_l[group]))
            from_odd = dot3(odd, (odd_h[group], odd_l[group]))
            up_even, up_odd = from_even[:, :LANES], from_odd[:, :LANES]
            up_re = jnp.where(left_half, up_even, up_odd)
            up_im = pltpu.roll(jnp.where(left_half, up_odd, up_even), LANES // 2, 1)
            re_h, re_l = split(up_re * table_cos + up_im * table_sin)
            im_h, im_l = split(up_im * table_cos - up_re * table_sin)
            for ref, real, imag in ((rhs_h, re_h, im_h), (rhs_l, re_l, im_l)):
                ref[0:Q, 0:LW] = real
                ref[0:Q, LW : 2 * LW] = -imag
                ref[Q : 2 * Q, 0:LW] = imag
                ref[Q : 2 * Q, LW : 2 * LW] = real
            low = from_even[:, LANES:] + from_odd[:, LANES:]
            low = low * low_cos + pltpu.roll(low, LANES // 2, 1) * low_sin
            low = low.T * norm
            low_re, low_im = low[:width], low[width:]
            for part in range(4):
                at = slice(part * quarter, (part + 1) * quarter)
                c = cos_rows[part : part + 1]
                s = sin_rows[part : part + 1]
                center_re[at] = low_re[at] * c + low_im[at] * s
                center_im[at] = low_im[at] * c - low_re[at] * s

        def correlate(place, slot):
            rhs_h, rhs_l, center_re, center_im = slot
            turn = pl.multiple_of((place // BLOCKS) * rows, 8)
            cos_rows = cos_ref[pl.ds(turn, rows), :]
            sin_rows = sin_ref[pl.ds(turn, rows), :]
            right = (rhs_h[...], rhs_l[...])
            group_size = min(pairs, 2)
            for base_pair in range(0, pairs, group_size):
                parts = []
                for pair in range(base_pair, base_pair + group_size):
                    c = cos_rows[4 + pair : 5 + pair]
                    s = sin_rows[4 + pair : 5 + pair]
                    t1 = center_re[...] * c
                    t2 = center_im[...] * s
                    t3 = center_im[...] * c
                    t4 = center_re[...] * s
                    parts.append(jnp.concatenate([t1 + t2, t3 - t4], axis=1))
                    parts.append(jnp.concatenate([t1 - t2, t3 + t4], axis=1))
                left = split(jnp.concatenate(parts, axis=0))
                total = dot3(left, right)
                for index in range(2 * group_size):
                    pair = base_pair + index // 2
                    at = (pairs - 1 - pair if index % 2 else pairs + pair) * width
                    put = slice(at, at + width)
                    re = total[index * width : (index + 1) * width, :LW]
                    im = total[index * width : (index + 1) * width, LW:]
                    acc_re[put] = acc_re[put] + re
                    acc_im[put] = acc_im[put] + im
                    acc_sq[put] = jnp.maximum(acc_sq[put], re * re + im * im)

        def block_at(index):
            return plan_ref[first_block + jnp.minimum(index, count - 1)]

        channelize(block_at(0), slots[0])

        def step(index, carry):
            for side in range(2):
                channelize(block_at(2 * index + side + 1), slots[1 - side])
                correlate(block_at(2 * index + side), slots[side])
            return carry

        lax.fori_loop(0, count // 2, step, 0)
        if opening:
            return
        lanes = lax.broadcasted_iota(jnp.int32, (quarter, LW), 1)
        source = lax.shift_right_logical(lanes, 1) + (LW // 2) * (lanes & 1)

        def natural(value):
            return jnp.take_along_axis(value, source, axis=1, mode="promise_in_bounds")

        for bin_index in range(bins):
            for part, kappa in enumerate((0, 2, 1, 3)):
                first = bin_index * width + part * quarter
                take = slice(first, first + quarter)
                put = pl.ds(kappa, quarter, stride=4)
                held_ref[bin_index, put, :] = natural(jnp.sqrt(acc_sq[take]))
                coherent_ref[0, bin_index, put, :] = natural(acc_re[take] * blend)
                coherent_ref[1, bin_index, put, :] = natural(acc_im[take] * blend)

    vmem = pl.BlockSpec(memory_space=pltpu.VMEM)
    slot = [
        pltpu.VMEM((2 * Q, 2 * LW), jnp.bfloat16),
        pltpu.VMEM((2 * Q, 2 * LW), jnp.bfloat16),
        pltpu.VMEM((width, Q), jnp.float32),
        pltpu.VMEM((width, Q), jnp.float32),
    ]
    sums = [(bins * width, LW)] * 3
    if opening:
        shapes = sums + [(slabs * rows, LANES)] * 2
        scratch = [(PAD + blocks * Q, LANES), (blocks * PAD, LANES)]
    else:
        shapes = [(bins, width, LW), (2, bins, width, LW)]
        scratch = [(PAD + blocks * Q, LANES)] + sums
    work = 2 * 3 * count * NCH * NCH * (2 * Q + 2 * bins * width // 2)
    return pl.pallas_call(
        kernel,
        in_specs=[pl.BlockSpec(memory_space=pltpu.SMEM)] + [vmem] * (7 + inputs),
        out_specs=[vmem] * outputs,
        scratch_shapes=[pltpu.VMEM(shape, jnp.float32) for shape in scratch] + slot + slot,
        out_shape=[jax.ShapeDtypeStruct(shape, jnp.float32) for shape in shapes],
        compiler_params=pltpu.CompilerParams(vmem_limit_bytes=40 * 1024 * 1024),
        cost_estimate=pl.CostEstimate(flops=work, transcendentals=0, bytes_accessed=4 * 1024 * 1024),
        name="surfaces_first" if opening else "surfaces_last",
    )(
        plan,
        jnp.asarray(fixed),
        jnp.asarray(ticks),
        jnp.asarray(small),
        *[jnp.asarray(table) for table in weights],
        *pieces,
        *notes,
        *(() if opening else carried),
    )


def on_device(capture, dropped):
    slabs = lax.axis_size("slab")
    groups = lax.axis_size("grp")
    slab = lax.axis_index("slab")
    group = lax.axis_index("grp")
    axes = ("slab", "grp")
    total = slabs * groups
    outer = slabs // 4
    hops = capture.shape[1] // HOP
    own = packed(capture, dropped)

    def split_index(flat):
        return flat // (4 * groups), (flat // (2 * groups)) % 2, (flat // groups) % 2, flat % groups

    def joined(far, side, core, member):
        return ((far * 2 + side) * 2 + core) * groups + member

    def moved(array, by):
        pairs = []
        for flat in range(total):
            far, side, core, member = split_index(flat)
            target = joined(
                (far + by[0]) % outer, (side + by[1]) % 2, (core + by[2]) % 2, (member + by[3]) % groups
            )
            pairs.append((flat, target))
        return lax.ppermute(array, axes, pairs)

    line = [own] + [moved(own, (step, 0, 0, 0)) for step in range(1, outer)]
    line = jnp.concatenate(line, axis=0)
    ticks = line[:, hops:, :]
    note_steps = [(1, 0, 0), (1, 1, 0)]
    notes = [moved(ticks, (0,) + by) for by in note_steps]
    others = range(1, groups)
    near = [line] + [moved(line, (0, 0, 0, member)) for member in others]
    far = [moved(line, (0, 1, 0, member)) for member in range(groups)]
    near_steps = [(0, 0, member) for member in range(groups)]
    far_steps = [(1, 0, member) for member in range(groups)]
    near += [moved(piece, (0, 0, 1, 0)) for piece in near]
    near_steps += [(side, 1, member) for side, _, member in near_steps]
    me_far, me_side, me_core, me_member = split_index(slab * groups + group)

    def places(steps):
        return [
            joined(
                (me_far - step) % outer,
                (me_side - side) % 2,
                (me_core - core) % 2,
                (me_member - member) % groups,
            )
            for side, core, member in steps
            for step in range(outer)
        ]

    def stack(values):
        return jnp.stack([jnp.asarray(value, jnp.int32) for value in values])

    first_blocks = []
    last_blocks = []
    for step in range(outer):
        for core in range(2):
            for member in range(groups):
                block = joined(step, me_side, core, member)
                (last_blocks if core == member == 0 else first_blocks).append(block)
                last_blocks.append(joined(step, 1 - me_side, core, member))
    plan = [slab, group] + places(near_steps) + places(note_steps) + first_blocks
    carried = surfaces(stack(plan), near, slabs, groups, len(first_blocks), notes=notes)
    far += [moved(piece, (0, 0, 1, 0)) for piece in far]
    far_steps += [(side, 1, member) for side, _, member in far_steps]
    plan = [slab, group] + places(near_steps) + places(far_steps) + last_blocks
    held, coherent = surfaces(
        stack(plan), near + far, slabs, groups, len(last_blocks), carried=carried
    )
    return held, coherent


def solution(mesh):
    in_specs = (P(None, ("slab", "grp")), P("slab"))
    out_specs = (P("slab", "grp", None), P(None, "slab", "grp", None))
    return jax.shard_map(
        on_device, mesh=mesh, in_specs=in_specs, out_specs=out_specs, check_vma=False
    )
```

```python
import math

import jax
import jax.numpy as jnp
import ml_dtypes
import numpy as np
from jax import lax
from jax.experimental import pallas as pl
from jax.experimental.pallas import tpu as pltpu
from jax.sharding import PartitionSpec as P


NCH = 256
HOP = 64
KW = 128
LW = 128
Q = 128
BLOCKS = 2
PERIOD = Q * HOP
TURN = 2 * PERIOD
LANES = 128
PAD = 8


def halves(table):
    high = table.astype(ml_dtypes.bfloat16)
    low = (table - high.astype(np.float64)).astype(ml_dtypes.bfloat16)
    return high, low


def lower_order(width):
    quarter = width // 4
    return np.concatenate([4 * np.arange(quarter) + kappa for kappa in (0, 2, 1, 3)])


def upper_order():
    return np.concatenate([np.arange(0, LW, 2), np.arange(1, LW, 2)])


def window_rows():
    taps = np.arange(NCH)
    window = 0.5 - 0.5 * np.cos(2.0 * np.pi * taps / NCH)
    scaled = window / np.sqrt(np.sum(window * window))
    rows = np.zeros((8, LANES))
    for lag in range(NCH // HOP):
        piece = scaled[lag * HOP : (lag + 1) * HOP]
        rows[lag] = np.concatenate([piece, piece])
    return rows.astype(np.float32)


def channel_tables(groups):
    width = KW // groups
    half = width // 2
    taps = np.arange(NCH // 2)
    even = np.zeros((groups, NCH, NCH))
    odd = np.zeros((groups, NCH, NCH))

    def columns(channels):
        turns = 2.0 * np.pi * (taps[:, None] * channels[None, :] % NCH) / NCH
        cosine, sine = np.cos(turns), np.sin(turns)
        real = np.concatenate([cosine[:HOP], sine[:HOP], cosine[HOP:], sine[HOP:]])
        imag = np.concatenate([-sine[:HOP], cosine[:HOP], -sine[HOP:], cosine[HOP:]])
        return real, imag

    upper = KW + upper_order()
    for group in range(groups):
        lower = group * width + lower_order(width)
        real, imag = columns(upper[: LW // 2])
        even[group, :, 0:64], even[group, :, 64:128] = real, imag
        real, imag = columns(upper[LW // 2 :])
        odd[group, :, 0:64], odd[group, :, 64:128] = imag, real
        real, imag = columns(lower[:half])
        even[group, :, 128 : 128 + half] = real
        even[group, :, 192 : 192 + half] = imag
        real, imag = columns(lower[half:])
        odd[group, :, 128 + half : 128 + width] = real
        odd[group, :, 192 + half : 192 + width] = imag
    return halves(even) + halves(odd)


def turn_tables(bins, width):
    pairs = bins // 2
    rows = -(-(6 + pairs) // 8) * 8
    frame = np.arange(LANES)
    fixed = np.zeros((3, rows, LANES), np.int64)
    ticks = np.zeros((3, rows, LANES), np.int64)
    for place, kappa in enumerate((0, 2, 1, 3)):
        ticks[0, place] = bins - 1
        ticks[1, place] = 2 * bins
        fixed[0, place] = (bins - 1) * HOP * frame + (TURN // 4) * kappa * frame
        fixed[1, place] = 2 * bins * HOP * frame
    for pair in range(pairs):
        ticks[0, 4 + pair] = 2 * pair + 1
        fixed[0, 4 + pair] = (2 * pair + 1) * HOP * frame
    order = lower_order(width)
    scale = TURN // NCH
    ticks[0, 4 + pairs] = scale * np.concatenate([order, order])
    ticks[2, 4 + pairs] = scale * width
    ticks[0, 5 + pairs] = scale * (KW + upper_order())
    return fixed.astype(np.int32), ticks.astype(np.int32)


def cos_sin(angle):
    shifted = angle + TURN // 8
    quadrant = lax.shift_right_logical(shifted, int(math.log2(TURN // 4))) & 3
    remain = (shifted & (TURN // 4 - 1)) - TURN // 8
    x = remain.astype(jnp.float32) * np.float32(2.0 * math.pi / TURN)
    y = x * x
    sine = x * (1.0 + y * (-1.0 / 6 + y * (1.0 / 120 + y * (-1.0 / 5040 + y * (1.0 / 362880)))))
    cosine = 1.0 + y * (-0.5 + y * (1.0 / 24 + y * (-1.0 / 720 + y * (1.0 / 40320))))
    swap = (quadrant & 1) == 1
    out_cos = jnp.where(swap, sine, cosine)
    out_sin = jnp.where(swap, cosine, sine)
    out_cos = jnp.where((quadrant == 1) | (quadrant == 2), -out_cos, out_cos)
    out_sin = jnp.where(quadrant >= 2, -out_sin, out_sin)
    return out_cos, out_sin


def split(value):
    high = value.astype(jnp.bfloat16)
    low = (value - high.astype(jnp.float32)).astype(jnp.bfloat16)
    return high, low


def dot32(left, right):
    return lax.dot_general(
        left, right, (((1,), (0,)), ((), ())), preferred_element_type=jnp.float32
    )


def dot3(left, right):
    return dot32(left[0], right[0]) + dot32(left[1], right[0]) + dot32(left[0], right[1])


def small_table(width):
    order = KW + upper_order()
    phase = (np.arange(8)[:, None] * order[None, :]) % 4
    quarter_cos = np.array([1.0, 0.0, -1.0, 0.0])[phase]
    quarter_sin = np.array([0.0, 1.0, 0.0, -1.0])[phase]
    sign = np.where(np.arange(LANES) < width, 1.0, -1.0)[None, :]
    parts = [window_rows(), quarter_cos, quarter_sin, np.tile(sign, (8, 1))]
    return np.concatenate(parts).astype(np.float32)


def surfaces(plan, spots, pieces, slabs, groups, count, notes=(), carried=None):
    piece_at, note_at, tail_at, first_block = spots
    bins = Q // slabs
    pairs = bins // 2
    width = KW // groups
    quarter = width // 4
    blocks = slabs * BLOCKS
    fixed, ticks = turn_tables(bins, width)
    rows = fixed.shape[1]
    weights = channel_tables(groups)
    small = small_table(width)
    arrays = len(pieces)
    depth = pieces[0].shape[0]
    norm = 1.0 / math.sqrt(Q)
    blend = 1.0 / math.sqrt(slabs * BLOCKS)
    opening = carried is None
    inputs = arrays + len(notes) + (0 if opening else 6)
    outputs = 6 if opening else 2

    def kernel(plan_ref, fixed_ref, ticks_ref, small_ref, even_h, even_l, odd_h, odd_l, *rest):
        piece_refs = rest[:arrays]
        note_refs = rest[arrays : arrays + len(notes)]
        out_refs = rest[inputs : inputs + outputs]
        rest = rest[inputs + outputs :] if opening else rest[arrays:]
        if opening:
            acc_re, acc_im, acc_sq, cos_ref, sin_ref, tails = out_refs
            frames, drops = rest[:2]
            scratch = rest[2:]
        else:
            old_re, old_im, old_sq, cos_ref, sin_ref, tails = rest[:6]
            held_ref, coherent_ref = out_refs
            frames, acc_re, acc_im, acc_sq = rest[8:12]
            scratch = rest[12:]
        slots = ((scratch[0:4], scratch[4:8]), (scratch[8:12], scratch[12:16]))
        slab = plan_ref[0]
        group = plan_ref[1]
        frames[pl.ds(0, PAD), :] = jnp.zeros((PAD, LANES), jnp.float32)
        for array in range(arrays):
            for item in range(depth):
                place = plan_ref[piece_at + array * depth + item]
                start = pl.multiple_of(PAD + place * Q, 8)
                frames[pl.ds(start, Q), :] = piece_refs[array][item, pl.ds(0, Q), :]
                if opening:
                    start = pl.multiple_of((place // BLOCKS) * PAD, 8)
                    drops[pl.ds(start, PAD), :] = piece_refs[array][item, pl.ds(Q, PAD), :]
        for array in range(len(notes)):
            for item in range(depth):
                place = plan_ref[note_at + array * depth + item]
                tile = note_refs[array][item]
                frames[pl.ds(pl.multiple_of((place + 1) * Q, 8), PAD), :] = tile
                drops[pl.ds(pl.multiple_of((place // BLOCKS) * PAD, 8), PAD), :] = tile
        for item in range(depth):
            at = pl.ds(pl.multiple_of((plan_ref[tail_at + item] + 1) * Q, 8), PAD)
            if opening:
                tails[item] = frames[at, :]
            else:
                frames[at, :] = tails[item]

        def make_turns():
            base = fixed_ref[0] + slab * fixed_ref[1] + group * fixed_ref[2]
            rate = ticks_ref[0] + slab * ticks_ref[1] + group * ticks_ref[2]

            def stamp_step(n, total):
                dropped = drops[pl.ds(pl.multiple_of(n * PAD, 8), PAD), :][0:1]
                dropped = jnp.broadcast_to(dropped, (PAD, LANES)).astype(jnp.int32)
                total = (total + dropped) & (PERIOD - 1)
                wide = jnp.concatenate([total] * (rows // PAD), axis=0)
                cosine, sine = cos_sin((base + rate * wide) & (TURN - 1))
                at = pl.ds(pl.multiple_of(n * rows, 8), rows)
                cos_ref[at, :] = cosine
                sin_ref[at, :] = sine
                return total

            start = jnp.zeros((PAD, LANES), jnp.int32)
            lax.fori_loop(0, slabs, stamp_step, start, unroll=min(slabs, 16))

        if opening:
            acc_re[...] = jnp.zeros_like(acc_re)
            acc_im[...] = jnp.zeros_like(acc_im)
            acc_sq[...] = jnp.zeros_like(acc_sq)
            make_turns()
        else:
            acc_re[...] = old_re[...]
            acc_im[...] = old_im[...]
            acc_sq[...] = old_sq[...]
        lane = lax.broadcasted_iota(jnp.int32, (Q, LANES), 1)
        left_half = lane < LANES // 2

        def channelize(places, targets):
            evens = []
            odds = []
            for place in places:
                start = pl.multiple_of(place * Q, Q)
                lags = [
                    frames[pl.ds(start + (PAD - 3 + lag), Q), :] * small_ref[lag : lag + 1]
                    for lag in range(4)
                ]
                evens.append(jnp.concatenate([lags[0] + lags[2], lags[1] + lags[3]], axis=1))
                odds.append(jnp.concatenate([lags[0] - lags[2], lags[1] - lags[3]], axis=1))
            both_even = split(jnp.concatenate(evens, axis=0))
            both_odd = split(jnp.concatenate(odds, axis=0))
            from_even = dot3(both_even, (even_h[group], even_l[group]))
            from_odd = dot3(both_odd, (odd_h[group], odd_l[group]))
            for index, (place, slot) in enumerate(zip(places, targets)):
                part = slice(index * Q, (index + 1) * Q)
                finish(place, slot, from_even[part], from_odd[part])

        def finish(place, slot, from_even, from_odd):
            rhs_h, rhs_l, center_re, center_im = slot
            turn = pl.multiple_of((place // BLOCKS) * rows, 8)
            cos_rows = cos_ref[pl.ds(turn, rows), :]
            sin_rows = sin_ref[pl.ds(turn, rows), :]
            row_k, row_l = 4 + pairs, 5 + pairs
            low_cos = cos_rows[row_k : row_k + 1]
            low_sin = sin_rows[row_k : row_k + 1] * small_ref[24:25]
            up_cos = cos_rows[row_l : row_l + 1]
            up_sin = sin_rows[row_l : row_l + 1]
            table_cos = small_ref[8:16] * up_cos - small_ref[16:24] * up_sin
            table_sin = small_ref[16:24] * up_cos + small_ref[8:16] * up_sin
            table_cos = jnp.concatenate([table_cos] * (Q // 8), axis=0)
            table_sin = jnp.concatenate([table_sin] * (Q // 8), axis=0)
            up_even, up_odd = from_even[:, :LANES], from_odd[:, :LANES]
            up_re = jnp.where(left_half, up_even, up_odd)
            up_im = pltpu.roll(jnp.where(left_half, up_odd, up_even), LANES // 2, 1)
            re_h, re_l = split(up_re * table_cos + up_im * table_sin)
            im_h, im_l = split(up_im * table_cos - up_re * table_sin)
            for ref, real, imag in ((rhs_h, re_h, im_h), (rhs_l, re_l, im_l)):
                ref[0:Q, 0:LW] = real
                ref[0:Q, LW : 2 * LW] = -imag
                ref[Q : 2 * Q, 0:LW] = imag
                ref[Q : 2 * Q, LW : 2 * LW] = real
            low = from_even[:, LANES:] + from_odd[:, LANES:]
            low = low * low_cos + pltpu.roll(low, LANES // 2, 1) * low_sin
            low = low.T * norm
            low_re, low_im = low[:width], low[width:]
            for part in range(4):
                at = slice(part * quarter, (part + 1) * quarter)
                c = cos_rows[part : part + 1]
                s = sin_rows[part : part + 1]
                center_re[at] = low_re[at] * c + low_im[at] * s
                center_im[at] = low_im[at] * c - low_re[at] * s

        def correlate(place, slot):
            rhs_h, rhs_l, center_re, center_im = slot
            turn = pl.multiple_of((place // BLOCKS) * rows, 8)
            cos_rows = cos_ref[pl.ds(turn, rows), :]
            sin_rows = sin_ref[pl.ds(turn, rows), :]
            right = (rhs_h[...], rhs_l[...])
            group_size = min(pairs, 4)
            for base_pair in range(0, pairs, group_size):
                parts = []
                for pair in range(base_pair, base_pair + group_size):
                    c = cos_rows[4 + pair : 5 + pair]
                    s = sin_rows[4 + pair : 5 + pair]
                    t1 = center_re[...] * c
                    t2 = center_im[...] * s
                    t3 = center_im[...] * c
                    t4 = center_re[...] * s
                    parts.append(jnp.concatenate([t1 + t2, t3 - t4], axis=1))
                    parts.append(jnp.concatenate([t1 - t2, t3 + t4], axis=1))
                left = split(jnp.concatenate(parts, axis=0))
                total = dot3(left, right)
                for index in range(2 * group_size):
                    pair = base_pair + index // 2
                    at = (pairs - 1 - pair if index % 2 else pairs + pair) * width
                    put = slice(at, at + width)
                    re = total[index * width : (index + 1) * width, :LW]
                    im = total[index * width : (index + 1) * width, LW:]
                    acc_re[put] = acc_re[put] + re
                    acc_im[put] = acc_im[put] + im
                    acc_sq[put] = jnp.maximum(acc_sq[put], re * re + im * im)

        def block_at(index):
            return plan_ref[first_block + index]

        def work(first, side, more):
            if more:
                channelize((block_at(first + 2), block_at(first + 3)), slots[1 - side])
            for item in range(2):
                correlate(block_at(first + item), slots[side][item])

        def step(index, carry):
            work(4 * index, 0, True)
            work(4 * index + 2, 1, True)
            return carry

        channelize((block_at(0), block_at(1)), slots[0])
        lax.fori_loop(0, count // 4 - 1, step, 0)
        work(count - 4, 0, True)
        work(count - 2, 1, False)
        if opening:
            return
        lanes = lax.broadcasted_iota(jnp.int32, (quarter, LW), 1)
        source = lax.shift_right_logical(lanes, 1) + (LW // 2) * (lanes & 1)

        def natural(value):
            return jnp.take_along_axis(value, source, axis=1, mode="promise_in_bounds")

        for bin_index in range(bins):
            for part, kappa in enumerate((0, 2, 1, 3)):
                first = bin_index * width + part * quarter
                take = slice(first, first + quarter)
                put = pl.ds(kappa, quarter, stride=4)
                held_ref[bin_index, put, :] = natural(jnp.sqrt(acc_sq[take]))
                coherent_ref[0, bin_index, put, :] = natural(acc_re[take] * blend)
                coherent_ref[1, bin_index, put, :] = natural(acc_im[take] * blend)

    vmem = pl.BlockSpec(memory_space=pltpu.VMEM)
    slot = [
        pltpu.VMEM((2 * Q, 2 * LW), jnp.bfloat16),
        pltpu.VMEM((2 * Q, 2 * LW), jnp.bfloat16),
        pltpu.VMEM((width, Q), jnp.float32),
        pltpu.VMEM((width, Q), jnp.float32),
    ]
    sums = [(bins * width, LW)] * 3
    if opening:
        shapes = sums + [(slabs * rows, LANES)] * 2 + [(depth, PAD, LANES)]
        scratch = [(PAD + blocks * Q, LANES), (slabs * PAD, LANES)]
    else:
        shapes = [(bins, width, LW), (2, bins, width, LW)]
        scratch = [(PAD + blocks * Q, LANES)] + sums
    work = 2 * 3 * count * NCH * NCH * (2 * Q + 2 * bins * width // 2)
    return pl.pallas_call(
        kernel,
        in_specs=[pl.BlockSpec(memory_space=pltpu.SMEM)] + [vmem] * (7 + inputs),
        out_specs=[vmem] * outputs,
        scratch_shapes=[pltpu.VMEM(shape, jnp.float32) for shape in scratch] + slot * 4,
        out_shape=[jax.ShapeDtypeStruct(shape, jnp.float32) for shape in shapes],
        compiler_params=pltpu.CompilerParams(vmem_limit_bytes=(PAD + blocks * Q) * 4 * LANES + 12 * 1024 * 1024),
        cost_estimate=pl.CostEstimate(flops=work, transcendentals=0, bytes_accessed=4 * 1024 * 1024),
        name="surfaces_first" if opening else "surfaces_last",
    )(
        plan,
        jnp.asarray(fixed),
        jnp.asarray(ticks),
        jnp.asarray(small),
        *[jnp.asarray(table) for table in weights],
        *pieces,
        *notes,
        *(() if opening else carried),
    )


def on_device(capture, dropped):
    slabs = lax.axis_size("slab")
    groups = lax.axis_size("grp")
    slab = lax.axis_index("slab")
    group = lax.axis_index("grp")
    axes = ("slab", "grp")
    total = slabs * groups
    outer = slabs // 4
    hops = capture.shape[1] // HOP
    own = capture.reshape(2, hops, HOP).transpose(1, 0, 2).reshape(hops, 2 * HOP)
    lead = NCH // HOP - 1
    ticks = jnp.broadcast_to(dropped.astype(jnp.float32)[:, None], (PAD - lead, LANES))
    own = jnp.concatenate([own, ticks, own[hops - lead :]], axis=0)[None]

    def split_index(flat):
        return flat // (4 * groups), (flat // (2 * groups)) % 2, (flat // groups) % 2, flat % groups

    def joined(far, side, core, member):
        return ((far * 2 + side) * 2 + core) * groups + member

    def moved(array, by):
        pairs = []
        for flat in range(total):
            far, side, core, member = split_index(flat)
            target = joined(
                (far + by[0]) % outer, (side + by[1]) % 2, (core + by[2]) % 2, (member + by[3]) % groups
            )
            pairs.append((flat, target))
        return lax.ppermute(array, axes, pairs)

    line = [own] + [moved(own, (step, 0, 0, 0)) for step in range(1, outer)]
    line = jnp.concatenate(line, axis=0)
    tiles = line[:, hops:, :]
    note_steps = [(1, core, member) for core in range(2) for member in range(groups)]
    notes = []
    for by in note_steps:
        notes.append(moved(tiles, (0,) + by))
    near = [line] + [moved(line, (0, 0, 0, member)) for member in range(1, groups)]
    far = [moved(line, (0, 1, 0, 0))]
    far += [moved(piece, (0, 1, 0, 0)) for piece in near[1:]]
    near_steps = [(0, 0, member) for member in range(groups)]
    far_steps = [(1, 0, member) for member in range(groups)]
    cores = []
    for piece in near:
        cores.append(moved(piece, (0, 0, 1, 0)))
    near += cores
    near_steps += [(side, 1, member) for side, _, member in near_steps]
    me_far, me_side, me_core, me_member = split_index(slab * groups + group)

    def places(steps):
        return [
            joined(
                (me_far - step) % outer,
                (me_side - side) % 2,
                (me_core - core) % 2,
                (me_member - member) % groups,
            )
            for side, core, member in steps
            for step in range(outer)
        ]

    first_blocks = []
    last_blocks = []
    for step in range(outer):
        for core in range(2):
            for member in range(groups):
                first_blocks.append(joined(step, me_side, core, member))
                last_blocks.append(joined(step, 1 - me_side, core, member))
    tail_places = [joined(step, me_side, 1, groups - 1) for step in range(outer)]
    far_steps += [(side, 1, member) for side, _, member in far_steps]
    parts = [places(near_steps), places(far_steps), places(note_steps), tail_places]
    parts += [first_blocks, last_blocks]
    begins = np.cumsum([2] + [len(part) for part in parts])
    near_at, far_at, note_at, tail_at, first_at, last_at = (int(at) for at in begins[:-1])
    plan = [slab, group] + sum(parts, [])
    plan = jnp.stack([jnp.asarray(value, jnp.int32) for value in plan])
    spots = (near_at, note_at, tail_at, first_at)
    carried = surfaces(plan, spots, near, slabs, groups, len(first_blocks), notes=notes)
    far += [moved(far[0], (0, 0, 1, 0))]
    far += [moved(piece, (0, 0, 1, 0)) for piece in far[1:groups]]
    spots = (far_at, note_at, tail_at, last_at)
    held, coherent = surfaces(
        plan, spots, far, slabs, groups, len(last_blocks), carried=carried
    )
    return held, coherent


def solution(mesh):
    in_specs = (P(None, ("slab", "grp")), P("slab"))
    out_specs = (P("slab", "grp", None), P(None, "slab", "grp", None))

    return jax.shard_map(
        on_device, mesh=mesh, in_specs=in_specs, out_specs=out_specs, check_vma=False
    )
```

```python
import math

import jax
import jax.numpy as jnp
import ml_dtypes
import numpy as np
from jax import lax
from jax.experimental import pallas as pl
from jax.experimental.pallas import tpu as pltpu
from jax.sharding import PartitionSpec as P


NCH = 256
HOP = 64
KW = 128
LW = 128
Q = 128
BLOCKS = 2
PERIOD = Q * HOP
TURN = 2 * PERIOD
LANES = 128
PAD = 8


def halves(table):
    high = table.astype(ml_dtypes.bfloat16)
    low = (table - high.astype(np.float64)).astype(ml_dtypes.bfloat16)
    return high, low


def lower_order(width):
    quarter = width // 4
    return np.concatenate([4 * np.arange(quarter) + kappa for kappa in (0, 2, 1, 3)])


def upper_order():
    return np.concatenate([np.arange(0, LW, 2), np.arange(1, LW, 2)])


def window_rows():
    taps = np.arange(NCH)
    window = 0.5 - 0.5 * np.cos(2.0 * np.pi * taps / NCH)
    scaled = window / np.sqrt(np.sum(window * window))
    rows = np.zeros((8, LANES))
    for lag in range(NCH // HOP):
        piece = scaled[lag * HOP : (lag + 1) * HOP]
        rows[lag] = np.concatenate([piece, piece])
    return rows.astype(np.float32)


def channel_tables(groups):
    width = KW // groups
    half = width // 2
    taps = np.arange(NCH // 2)
    even = np.zeros((groups, NCH, NCH))
    odd = np.zeros((groups, NCH, NCH))

    def columns(channels):
        turns = 2.0 * np.pi * (taps[:, None] * channels[None, :] % NCH) / NCH
        cosine, sine = np.cos(turns), np.sin(turns)
        real = np.concatenate([cosine[:HOP], sine[:HOP], cosine[HOP:], sine[HOP:]])
        imag = np.concatenate([-sine[:HOP], cosine[:HOP], -sine[HOP:], cosine[HOP:]])
        return real, imag

    upper = KW + upper_order()
    for group in range(groups):
        lower = group * width + lower_order(width)
        real, imag = columns(upper[: LW // 2])
        even[group, :, 0:64], even[group, :, 64:128] = real, imag
        real, imag = columns(upper[LW // 2 :])
        odd[group, :, 0:64], odd[group, :, 64:128] = imag, real
        real, imag = columns(lower[:half])
        even[group, :, 128 : 128 + half] = real
        even[group, :, 192 : 192 + half] = imag
        real, imag = columns(lower[half:])
        odd[group, :, 128 + half : 128 + width] = real
        odd[group, :, 192 + half : 192 + width] = imag
    return halves(even) + halves(odd)


def turn_tables(bins, width):
    pairs = bins // 2
    rows = -(-(6 + pairs) // 8) * 8
    frame = np.arange(LANES)
    fixed = np.zeros((3, rows, LANES), np.int64)
    ticks = np.zeros((3, rows, LANES), np.int64)
    for place, kappa in enumerate((0, 2, 1, 3)):
        ticks[0, place] = bins - 1
        ticks[1, place] = 2 * bins
        fixed[0, place] = (bins - 1) * HOP * frame + (TURN // 4) * kappa * frame
        fixed[1, place] = 2 * bins * HOP * frame
    for pair in range(pairs):
        ticks[0, 4 + pair] = 2 * pair + 1
        fixed[0, 4 + pair] = (2 * pair + 1) * HOP * frame
    order = lower_order(width)
    scale = TURN // NCH
    ticks[0, 4 + pairs] = scale * np.concatenate([order, order])
    ticks[2, 4 + pairs] = scale * width
    ticks[0, 5 + pairs] = scale * (KW + upper_order())
    return fixed.astype(np.int32), ticks.astype(np.int32)


def cos_sin(angle):
    shifted = angle + TURN // 8
    quadrant = lax.shift_right_logical(shifted, int(math.log2(TURN // 4))) & 3
    remain = (shifted & (TURN // 4 - 1)) - TURN // 8
    x = remain.astype(jnp.float32) * np.float32(2.0 * math.pi / TURN)
    y = x * x
    sine = x * (1.0 + y * (-1.0 / 6 + y * (1.0 / 120 + y * (-1.0 / 5040 + y * (1.0 / 362880)))))
    cosine = 1.0 + y * (-0.5 + y * (1.0 / 24 + y * (-1.0 / 720 + y * (1.0 / 40320))))
    swap = (quadrant & 1) == 1
    out_cos = jnp.where(swap, sine, cosine)
    out_sin = jnp.where(swap, cosine, sine)
    out_cos = jnp.where((quadrant == 1) | (quadrant == 2), -out_cos, out_cos)
    out_sin = jnp.where(quadrant >= 2, -out_sin, out_sin)
    return out_cos, out_sin


def split(value):
    high = value.astype(jnp.bfloat16)
    low = (value - high.astype(jnp.float32)).astype(jnp.bfloat16)
    return high, low


def dot32(left, right):
    return lax.dot_general(
        left, right, (((1,), (0,)), ((), ())), preferred_element_type=jnp.float32
    )


def dot3(left, right):
    return dot32(left[0], right[0]) + dot32(left[1], right[0]) + dot32(left[0], right[1])


def small_table(width):
    order = KW + upper_order()
    phase = (np.arange(8)[:, None] * order[None, :]) % 4
    quarter_cos = np.array([1.0, 0.0, -1.0, 0.0])[phase]
    quarter_sin = np.array([0.0, 1.0, 0.0, -1.0])[phase]
    sign = np.where(np.arange(LANES) < width, 1.0, -1.0)[None, :]
    parts = [window_rows(), quarter_cos, quarter_sin, np.tile(sign, (8, 1))]
    return np.concatenate(parts).astype(np.float32)


def surfaces(plan, spots, pieces, slabs, groups, count, notes=(), carried=None):
    piece_at, note_at, tail_at, first_block = spots
    bins = Q // slabs
    pairs = bins // 2
    width = KW // groups
    quarter = width // 4
    blocks = slabs * BLOCKS
    fixed, ticks = turn_tables(bins, width)
    rows = fixed.shape[1]
    weights = channel_tables(groups)
    small = small_table(width)
    arrays = len(pieces)
    depth = pieces[0].shape[0]
    norm = 1.0 / math.sqrt(Q)
    blend = 1.0 / math.sqrt(slabs * BLOCKS)
    opening = carried is None
    inputs = arrays + len(notes) + (0 if opening else 6)
    outputs = 6 if opening else 2

    def kernel(plan_ref, fixed_ref, ticks_ref, small_ref, even_h, even_l, odd_h, odd_l, *rest):
        piece_refs = rest[:arrays]
        note_refs = rest[arrays : arrays + len(notes)]
        out_refs = rest[inputs : inputs + outputs]
        rest = rest[inputs + outputs :] if opening else rest[arrays:]
        if opening:
            acc_re, acc_im, acc_sq, cos_ref, sin_ref, tails = out_refs
            frames, drops = rest[:2]
            scratch = rest[2:]
        else:
            old_re, old_im, old_sq, cos_ref, sin_ref, tails = rest[:6]
            held_ref, coherent_ref = out_refs
            frames, acc_re, acc_im, acc_sq = rest[8:12]
            scratch = rest[12:]
        slots = ((scratch[0:4], scratch[4:8]), (scratch[8:12], scratch[12:16]))
        slab = plan_ref[0]
        group = plan_ref[1]
        frames[pl.ds(0, PAD), :] = jnp.zeros((PAD, LANES), jnp.float32)
        for array in range(arrays):
            for item in range(depth):
                place = plan_ref[piece_at + array * depth + item]
                start = pl.multiple_of(PAD + place * Q, 8)
                frames[pl.ds(start, Q), :] = piece_refs[array][item, pl.ds(0, Q), :]
                if opening:
                    start = pl.multiple_of((place // BLOCKS) * PAD, 8)
                    drops[pl.ds(start, PAD), :] = piece_refs[array][item, pl.ds(Q, PAD), :]
        for array in range(len(notes)):
            for item in range(depth):
                place = plan_ref[note_at + array * depth + item]
                tile = note_refs[array][item]
                frames[pl.ds(pl.multiple_of((place + 1) * Q, 8), PAD), :] = tile
                drops[pl.ds(pl.multiple_of((place // BLOCKS) * PAD, 8), PAD), :] = tile
        for item in range(depth):
            at = pl.ds(pl.multiple_of((plan_ref[tail_at + item] + 1) * Q, 8), PAD)
            if opening:
                tails[item] = frames[at, :]
            else:
                frames[at, :] = tails[item]

        def make_turns():
            base = fixed_ref[0] + slab * fixed_ref[1] + group * fixed_ref[2]
            rate = ticks_ref[0] + slab * ticks_ref[1] + group * ticks_ref[2]

            def stamp_step(n, total):
                dropped = drops[pl.ds(pl.multiple_of(n * PAD, 8), PAD), :][0:1]
                dropped = jnp.broadcast_to(dropped, (PAD, LANES)).astype(jnp.int32)
                total = (total + dropped) & (PERIOD - 1)
                wide = jnp.concatenate([total] * (rows // PAD), axis=0)
                cosine, sine = cos_sin((base + rate * wide) & (TURN - 1))
                at = pl.ds(pl.multiple_of(n * rows, 8), rows)
                cos_ref[at, :] = cosine
                sin_ref[at, :] = sine
                return total

            start = jnp.zeros((PAD, LANES), jnp.int32)
            lax.fori_loop(0, slabs, stamp_step, start, unroll=min(slabs, 16))

        if opening:
            acc_re[...] = jnp.zeros_like(acc_re)
            acc_im[...] = jnp.zeros_like(acc_im)
            acc_sq[...] = jnp.zeros_like(acc_sq)
            make_turns()
        else:
            acc_re[...] = old_re[...]
            acc_im[...] = old_im[...]
            acc_sq[...] = old_sq[...]
        lane = lax.broadcasted_iota(jnp.int32, (Q, LANES), 1)
        left_half = lane < LANES // 2

        def channelize(places, targets):
            evens = []
            odds = []
            for place in places:
                start = pl.multiple_of(place * Q, Q)
                lags = [
                    frames[pl.ds(start + (PAD - 3 + lag), Q), :] * small_ref[lag : lag + 1]
                    for lag in range(4)
                ]
                evens.append(jnp.concatenate([lags[0] + lags[2], lags[1] + lags[3]], axis=1))
                odds.append(jnp.concatenate([lags[0] - lags[2], lags[1] - lags[3]], axis=1))
            both_even = split(jnp.concatenate(evens, axis=0))
            both_odd = split(jnp.concatenate(odds, axis=0))
            from_even = dot3(both_even, (even_h[group], even_l[group]))
            from_odd = dot3(both_odd, (odd_h[group], odd_l[group]))
            for index, (place, slot) in enumerate(zip(places, targets)):
                part = slice(index * Q, (index + 1) * Q)
                finish(place, slot, from_even[part], from_odd[part])

        def finish(place, slot, from_even, from_odd):
            rhs_h, rhs_l, center_re, center_im = slot
            turn = pl.multiple_of((place // BLOCKS) * rows, 8)
            cos_rows = cos_ref[pl.ds(turn, rows), :]
            sin_rows = sin_ref[pl.ds(turn, rows), :]
            row_k, row_l = 4 + pairs, 5 + pairs
            low_cos = cos_rows[row_k : row_k + 1]
            low_sin = sin_rows[row_k : row_k + 1] * small_ref[24:25]
            up_cos = cos_rows[row_l : row_l + 1]
            up_sin = sin_rows[row_l : row_l + 1]
            table_cos = small_ref[8:16] * up_cos - small_ref[16:24] * up_sin
            table_sin = small_ref[16:24] * up_cos + small_ref[8:16] * up_sin
            table_cos = jnp.concatenate([table_cos] * (Q // 8), axis=0)
            table_sin = jnp.concatenate([table_sin] * (Q // 8), axis=0)
            up_even, up_odd = from_even[:, :LANES], from_odd[:, :LANES]
            up_re = jnp.where(left_half, up_even, up_odd)
            up_im = pltpu.roll(jnp.where(left_half, up_odd, up_even), LANES // 2, 1)
            re_h, re_l = split(up_re * table_cos + up_im * table_sin)
            im_h, im_l = split(up_im * table_cos - up_re * table_sin)
            for ref, real, imag in ((rhs_h, re_h, im_h), (rhs_l, re_l, im_l)):
                ref[0:Q, 0:LW] = real
                ref[0:Q, LW : 2 * LW] = -imag
                ref[Q : 2 * Q, 0:LW] = imag
                ref[Q : 2 * Q, LW : 2 * LW] = real
            low = from_even[:, LANES:] + from_odd[:, LANES:]
            low = low * low_cos + pltpu.roll(low, LANES // 2, 1) * low_sin
            low = low.T * norm
            low_re, low_im = low[:width], low[width:]
            for part in range(4):
                at = slice(part * quarter, (part + 1) * quarter)
                c = cos_rows[part : part + 1]
                s = sin_rows[part : part + 1]
                center_re[at] = low_re[at] * c + low_im[at] * s
                center_im[at] = low_im[at] * c - low_re[at] * s

        def correlate(place, slot):
            rhs_h, rhs_l, center_re, center_im = slot
            turn = pl.multiple_of((place // BLOCKS) * rows, 8)
            cos_rows = cos_ref[pl.ds(turn, rows), :]
            sin_rows = sin_ref[pl.ds(turn, rows), :]
            right = (rhs_h[...], rhs_l[...])
            group_size = min(pairs, 4)
            for base_pair in range(0, pairs, group_size):
                parts = []
                for pair in range(base_pair, base_pair + group_size):
                    c = cos_rows[4 + pair : 5 + pair]
                    s = sin_rows[4 + pair : 5 + pair]
                    t1 = center_re[...] * c
                    t2 = center_im[...] * s
                    t3 = center_im[...] * c
                    t4 = center_re[...] * s
                    parts.append(jnp.concatenate([t1 + t2, t3 - t4], axis=1))
                    parts.append(jnp.concatenate([t1 - t2, t3 + t4], axis=1))
                left = split(jnp.concatenate(parts, axis=0))
                total = dot3(left, right)
                for index in range(2 * group_size):
                    pair = base_pair + index // 2
                    at = (pairs - 1 - pair if index % 2 else pairs + pair) * width
                    put = slice(at, at + width)
                    re = total[index * width : (index + 1) * width, :LW]
                    im = total[index * width : (index + 1) * width, LW:]
                    acc_re[put] = acc_re[put] + re
                    acc_im[put] = acc_im[put] + im
                    acc_sq[put] = jnp.maximum(acc_sq[put], re * re + im * im)

        def block_at(index):
            return plan_ref[first_block + index]

        def work(first, side, more):
            if more:
                channelize((block_at(first + 2), block_at(first + 3)), slots[1 - side])
            for item in range(2):
                correlate(block_at(first + item), slots[side][item])

        def step(index, carry):
            work(4 * index, 0, True)
            work(4 * index + 2, 1, True)
            return carry

        channelize((block_at(0), block_at(1)), slots[0])
        lax.fori_loop(0, count // 4 - 1, step, 0)
        work(count - 4, 0, True)
        work(count - 2, 1, False)
        if opening:
            return
        lanes = lax.broadcasted_iota(jnp.int32, (quarter, LW), 1)
        source = lax.shift_right_logical(lanes, 1) + (LW // 2) * (lanes & 1)

        def natural(value):
            return jnp.take_along_axis(value, source, axis=1, mode="promise_in_bounds")

        for bin_index in range(bins):
            for part, kappa in enumerate((0, 2, 1, 3)):
                first = bin_index * width + part * quarter
                take = slice(first, first + quarter)
                put = pl.ds(kappa, quarter, stride=4)
                held_ref[bin_index, put, :] = natural(jnp.sqrt(acc_sq[take]))
                coherent_ref[0, bin_index, put, :] = natural(acc_re[take] * blend)
                coherent_ref[1, bin_index, put, :] = natural(acc_im[take] * blend)

    vmem = pl.BlockSpec(memory_space=pltpu.VMEM)
    slot = [
        pltpu.VMEM((2 * Q, 2 * LW), jnp.bfloat16),
        pltpu.VMEM((2 * Q, 2 * LW), jnp.bfloat16),
        pltpu.VMEM((width, Q), jnp.float32),
        pltpu.VMEM((width, Q), jnp.float32),
    ]
    sums = [(bins * width, LW)] * 3
    if opening:
        shapes = sums + [(slabs * rows, LANES)] * 2 + [(depth, PAD, LANES)]
        scratch = [(PAD + blocks * Q, LANES), (slabs * PAD, LANES)]
    else:
        shapes = [(bins, width, LW), (2, bins, width, LW)]
        scratch = [(PAD + blocks * Q, LANES)] + sums
    work = 2 * 3 * count * NCH * NCH * (2 * Q + 2 * bins * width // 2)
    return pl.pallas_call(
        kernel,
        in_specs=[pl.BlockSpec(memory_space=pltpu.SMEM)] + [vmem] * (7 + inputs),
        out_specs=[vmem] * outputs,
        scratch_shapes=[pltpu.VMEM(shape, jnp.float32) for shape in scratch] + slot * 4,
        out_shape=[jax.ShapeDtypeStruct(shape, jnp.float32) for shape in shapes],
        compiler_params=pltpu.CompilerParams(vmem_limit_bytes=(PAD + blocks * Q) * 4 * LANES + 12 * 1024 * 1024),
        cost_estimate=pl.CostEstimate(flops=work, transcendentals=0, bytes_accessed=4 * 1024 * 1024),
        name="surfaces_first" if opening else "surfaces_last",
    )(
        plan,
        jnp.asarray(fixed),
        jnp.asarray(ticks),
        jnp.asarray(small),
        *[jnp.asarray(table) for table in weights],
        *pieces,
        *notes,
        *(() if opening else carried),
    )


def on_device(capture, dropped):
    slabs = lax.axis_size("slab")
    groups = lax.axis_size("grp")
    slab = lax.axis_index("slab")
    group = lax.axis_index("grp")
    axes = ("slab", "grp")
    total = slabs * groups
    outer = slabs // 4
    hops = capture.shape[1] // HOP
    own = capture.reshape(2, hops, HOP).transpose(1, 0, 2).reshape(hops, 2 * HOP)
    ticks = jnp.broadcast_to(dropped.astype(jnp.float32)[:, None], (PAD, LANES))
    own = jnp.concatenate([own, ticks], axis=0)[None]
    lead = NCH // HOP - 1

    def split_index(flat):
        return flat // (4 * groups), (flat // (2 * groups)) % 2, (flat // groups) % 2, flat % groups

    def joined(far, side, core, member):
        return ((far * 2 + side) * 2 + core) * groups + member

    def moved(array, by):
        pairs = []
        for flat in range(total):
            far, side, core, member = split_index(flat)
            target = joined(
                (far + by[0]) % outer, (side + by[1]) % 2, (core + by[2]) % 2, (member + by[3]) % groups
            )
            pairs.append((flat, target))
        return lax.ppermute(array, axes, pairs)

    line = [own]
    for step in range(1, outer):
        line.append(moved(own, (step, 0, 0, 0)))
    line = jnp.concatenate(line, axis=0)
    tiles = jnp.concatenate([line[:, hops : hops + PAD - lead], line[:, hops - lead : hops]], axis=1)
    notes = []
    for member in range(groups):
        notes.append(moved(tiles, (0, 1, 0, member)))
    notes += [moved(note, (0, 0, 1, 0)) for note in notes]
    note_steps = [(1, core, member) for core in range(2) for member in range(groups)]
    near = [line] + [moved(line, (0, 0, 0, member)) for member in range(1, groups)]
    far = []
    for member in range(groups):
        far.append(moved(line, (0, 1, 0, member)))
    near_steps = [(0, 0, member) for member in range(groups)]
    far_steps = [(1, 0, member) for member in range(groups)]
    cores = []
    for piece in near:
        cores.append(moved(piece, (0, 0, 1, 0)))
    near += cores
    near_steps += [(side, 1, member) for side, _, member in near_steps]
    me_far, me_side, me_core, me_member = split_index(slab * groups + group)

    def places(steps):
        return [
            joined(
                (me_far - step) % outer,
                (me_side - side) % 2,
                (me_core - core) % 2,
                (me_member - member) % groups,
            )
            for side, core, member in steps
            for step in range(outer)
        ]

    first_blocks = []
    last_blocks = []
    for step in range(outer):
        for core in range(2):
            for member in range(groups):
                first_blocks.append(joined(step, me_side, core, member))
                last_blocks.append(joined(step, 1 - me_side, core, member))
    tail_places = [joined(step, me_side, 1, groups - 1) for step in range(outer)]
    far_steps += [(side, 1, member) for side, _, member in far_steps]
    parts = [places(near_steps), places(far_steps), places(note_steps), tail_places]
    parts += [first_blocks, last_blocks]
    begins = np.cumsum([2] + [len(part) for part in parts])
    near_at, far_at, note_at, tail_at, first_at, last_at = (int(at) for at in begins[:-1])
    plan = [slab, group] + sum(parts, [])
    plan = jnp.stack([jnp.asarray(value, jnp.int32) for value in plan])
    spots = (near_at, note_at, tail_at, first_at)
    carried = surfaces(plan, spots, near, slabs, groups, len(first_blocks), notes=notes)
    far += [moved(far[0], (0, 0, 1, 0))]
    far += [moved(piece, (0, 0, 1, 0)) for piece in far[1:groups]]
    spots = (far_at, note_at, tail_at, last_at)
    held, coherent = surfaces(
        plan, spots, far, slabs, groups, len(last_blocks), carried=carried
    )
    return held, coherent


def solution(mesh):
    in_specs = (P(None, ("slab", "grp")), P("slab"))
    out_specs = (P("slab", "grp", None), P(None, "slab", "grp", None))

    return jax.shard_map(
        on_device, mesh=mesh, in_specs=in_specs, out_specs=out_specs, check_vma=False
    )
```

```python
import math

import jax
import jax.numpy as jnp
import ml_dtypes
import numpy as np
from jax import lax
from jax.experimental import pallas as pl
from jax.experimental.pallas import tpu as pltpu
from jax.sharding import PartitionSpec as P


NCH = 256
HOP = 64
KW = 128
LW = 128
Q = 128
BLOCKS = 2
PERIOD = Q * HOP
TURN = 2 * PERIOD
LANES = 128
PAD = 8


def halves(table):
    high = table.astype(ml_dtypes.bfloat16)
    low = (table - high.astype(np.float64)).astype(ml_dtypes.bfloat16)
    return high, low


def lower_order(width):
    quarter = width // 4
    return np.concatenate([4 * np.arange(quarter) + kappa for kappa in (0, 2, 1, 3)])


def upper_order():
    return np.concatenate([np.arange(0, LW, 2), np.arange(1, LW, 2)])


def window_rows():
    taps = np.arange(NCH)
    window = 0.5 - 0.5 * np.cos(2.0 * np.pi * taps / NCH)
    scaled = window / np.sqrt(np.sum(window * window))
    rows = np.zeros((8, LANES))
    for lag in range(NCH // HOP):
        piece = scaled[lag * HOP : (lag + 1) * HOP]
        rows[lag] = np.concatenate([piece, piece])
    return rows.astype(np.float32)


def channel_tables(groups):
    width = KW // groups
    half = width // 2
    taps = np.arange(NCH // 2)
    even = np.zeros((groups, NCH, NCH))
    odd = np.zeros((groups, NCH, NCH))

    def columns(channels):
        turns = 2.0 * np.pi * (taps[:, None] * channels[None, :] % NCH) / NCH
        cosine, sine = np.cos(turns), np.sin(turns)
        real = np.concatenate([cosine[:HOP], sine[:HOP], cosine[HOP:], sine[HOP:]])
        imag = np.concatenate([-sine[:HOP], cosine[:HOP], -sine[HOP:], cosine[HOP:]])
        return real, imag

    upper = KW + upper_order()
    for group in range(groups):
        lower = group * width + lower_order(width)
        real, imag = columns(upper[: LW // 2])
        even[group, :, 0:64], even[group, :, 64:128] = real, imag
        real, imag = columns(upper[LW // 2 :])
        odd[group, :, 0:64], odd[group, :, 64:128] = imag, real
        real, imag = columns(lower[:half])
        even[group, :, 128 : 128 + half] = real
        even[group, :, 192 : 192 + half] = imag
        real, imag = columns(lower[half:])
        odd[group, :, 128 + half : 128 + width] = real
        odd[group, :, 192 + half : 192 + width] = imag
    return halves(even) + halves(odd)


def turn_tables(bins, width):
    pairs = bins // 2
    rows = -(-(6 + pairs) // 8) * 8
    frame = np.arange(LANES)
    fixed = np.zeros((3, rows, LANES), np.int64)
    ticks = np.zeros((3, rows, LANES), np.int64)
    for place, kappa in enumerate((0, 2, 1, 3)):
        ticks[0, place] = bins - 1
        ticks[1, place] = 2 * bins
        fixed[0, place] = (bins - 1) * HOP * frame + (TURN // 4) * kappa * frame
        fixed[1, place] = 2 * bins * HOP * frame
    for pair in range(pairs):
        ticks[0, 4 + pair] = 2 * pair + 1
        fixed[0, 4 + pair] = (2 * pair + 1) * HOP * frame
    order = lower_order(width)
    scale = TURN // NCH
    ticks[0, 4 + pairs] = scale * np.concatenate([order, order])
    ticks[2, 4 + pairs] = scale * width
    ticks[0, 5 + pairs] = scale * (KW + upper_order())
    return fixed.astype(np.int32), ticks.astype(np.int32)


def cos_sin(angle):
    shifted = angle + TURN // 8
    quadrant = lax.shift_right_logical(shifted, int(math.log2(TURN // 4))) & 3
    remain = (shifted & (TURN // 4 - 1)) - TURN // 8
    x = remain.astype(jnp.float32) * np.float32(2.0 * math.pi / TURN)
    y = x * x
    sine = x * (1.0 + y * (-1.0 / 6 + y * (1.0 / 120 + y * (-1.0 / 5040 + y * (1.0 / 362880)))))
    cosine = 1.0 + y * (-0.5 + y * (1.0 / 24 + y * (-1.0 / 720 + y * (1.0 / 40320))))
    swap = (quadrant & 1) == 1
    out_cos = jnp.where(swap, sine, cosine)
    out_sin = jnp.where(swap, cosine, sine)
    out_cos = jnp.where((quadrant == 1) | (quadrant == 2), -out_cos, out_cos)
    out_sin = jnp.where(quadrant >= 2, -out_sin, out_sin)
    return out_cos, out_sin


def split(value):
    high = value.astype(jnp.bfloat16)
    low = (value - high.astype(jnp.float32)).astype(jnp.bfloat16)
    return high, low


def dot32(left, right):
    return lax.dot_general(
        left, right, (((1,), (0,)), ((), ())), preferred_element_type=jnp.float32
    )


def dot3(left, right):
    return dot32(left[0], right[0]) + dot32(left[1], right[0]) + dot32(left[0], right[1])


def small_table(width):
    order = KW + upper_order()
    phase = (np.arange(8)[:, None] * order[None, :]) % 4
    quarter_cos = np.array([1.0, 0.0, -1.0, 0.0])[phase]
    quarter_sin = np.array([0.0, 1.0, 0.0, -1.0])[phase]
    sign = np.where(np.arange(LANES) < width, 1.0, -1.0)[None, :]
    parts = [window_rows(), quarter_cos, quarter_sin, np.tile(sign, (8, 1))]
    return np.concatenate(parts).astype(np.float32)


def surfaces(plan, spots, pieces, slabs, groups, count, notes=(), carried=None):
    piece_at, note_at, tail_at, first_block = spots
    bins = Q // slabs
    pairs = bins // 2
    width = KW // groups
    quarter = width // 4
    blocks = slabs * BLOCKS
    fixed, ticks = turn_tables(bins, width)
    rows = fixed.shape[1]
    weights = channel_tables(groups)
    small = small_table(width)
    arrays = len(pieces)
    depth = pieces[0].shape[0]
    norm = 1.0 / math.sqrt(Q)
    blend = 1.0 / math.sqrt(slabs * BLOCKS)
    opening = carried is None
    inputs = arrays + len(notes) + (0 if opening else 6)
    outputs = 6 if opening else 2

    def kernel(plan_ref, fixed_ref, ticks_ref, small_ref, even_h, even_l, odd_h, odd_l, *rest):
        piece_refs = rest[:arrays]
        note_refs = rest[arrays : arrays + len(notes)]
        out_refs = rest[inputs : inputs + outputs]
        rest = rest[inputs + outputs :] if opening else rest[arrays:]
        if opening:
            acc_re, acc_im, acc_sq, cos_ref, sin_ref, tails = out_refs
            frames, drops = rest[:2]
            scratch = rest[2:]
        else:
            old_re, old_im, old_sq, cos_ref, sin_ref, tails = rest[:6]
            held_ref, coherent_ref = out_refs
            frames, acc_re, acc_im, acc_sq = rest[8:12]
            scratch = rest[12:]
        slots = ((scratch[0:4], scratch[4:8]), (scratch[8:12], scratch[12:16]))
        slab = plan_ref[0]
        group = plan_ref[1]
        frames[pl.ds(0, PAD), :] = jnp.zeros((PAD, LANES), jnp.float32)
        for array in range(arrays):
            for item in range(depth):
                place = plan_ref[piece_at + array * depth + item]
                start = pl.multiple_of(PAD + place * Q, 8)
                frames[pl.ds(start, Q), :] = piece_refs[array][item, pl.ds(0, Q), :]
                if opening:
                    start = pl.multiple_of((place // BLOCKS) * PAD, 8)
                    drops[pl.ds(start, PAD), :] = piece_refs[array][item, pl.ds(Q, PAD), :]
        for array in range(len(notes)):
            for item in range(depth):
                place = plan_ref[note_at + array * depth + item]
                tile = note_refs[array][item]
                frames[pl.ds(pl.multiple_of((place + 1) * Q, 8), PAD), :] = tile
                drops[pl.ds(pl.multiple_of((place // BLOCKS) * PAD, 8), PAD), :] = tile
        for item in range(depth):
            at = pl.ds(pl.multiple_of((plan_ref[tail_at + item] + 1) * Q, 8), PAD)
            if opening:
                tails[item] = frames[at, :]
            else:
                frames[at, :] = tails[item]

        def make_turns():
            base = fixed_ref[0] + slab * fixed_ref[1] + group * fixed_ref[2]
            rate = ticks_ref[0] + slab * ticks_ref[1] + group * ticks_ref[2]

            def stamp_step(n, total):
                dropped = drops[pl.ds(pl.multiple_of(n * PAD, 8), PAD), :][0:1]
                dropped = jnp.broadcast_to(dropped, (PAD, LANES)).astype(jnp.int32)
                total = (total + dropped) & (PERIOD - 1)
                wide = jnp.concatenate([total] * (rows // PAD), axis=0)
                cosine, sine = cos_sin((base + rate * wide) & (TURN - 1))
                at = pl.ds(pl.multiple_of(n * rows, 8), rows)
                cos_ref[at, :] = cosine
                sin_ref[at, :] = sine
                return total

            start = jnp.zeros((PAD, LANES), jnp.int32)
            lax.fori_loop(0, slabs, stamp_step, start, unroll=min(slabs, 16))

        if opening:
            acc_re[...] = jnp.zeros_like(acc_re)
            acc_im[...] = jnp.zeros_like(acc_im)
            acc_sq[...] = jnp.zeros_like(acc_sq)
            make_turns()
        else:
            acc_re[...] = old_re[...]
            acc_im[...] = old_im[...]
            acc_sq[...] = old_sq[...]
        lane = lax.broadcasted_iota(jnp.int32, (Q, LANES), 1)
        left_half = lane < LANES // 2

        def channelize(places, targets):
            evens = []
            odds = []
            for place in places:
                start = pl.multiple_of(place * Q, Q)
                lags = [
                    frames[pl.ds(start + (PAD - 3 + lag), Q), :] * small_ref[lag : lag + 1]
                    for lag in range(4)
                ]
                evens.append(jnp.concatenate([lags[0] + lags[2], lags[1] + lags[3]], axis=1))
                odds.append(jnp.concatenate([lags[0] - lags[2], lags[1] - lags[3]], axis=1))
            both_even = split(jnp.concatenate(evens, axis=0))
            both_odd = split(jnp.concatenate(odds, axis=0))
            from_even = dot3(both_even, (even_h[group], even_l[group]))
            from_odd = dot3(both_odd, (odd_h[group], odd_l[group]))
            for index, (place, slot) in enumerate(zip(places, targets)):
                part = slice(index * Q, (index + 1) * Q)
                finish(place, slot, from_even[part], from_odd[part])

        def finish(place, slot, from_even, from_odd):
            rhs_h, rhs_l, center_re, center_im = slot
            turn = pl.multiple_of((place // BLOCKS) * rows, 8)
            cos_rows = cos_ref[pl.ds(turn, rows), :]
            sin_rows = sin_ref[pl.ds(turn, rows), :]
            row_k, row_l = 4 + pairs, 5 + pairs
            low_cos = cos_rows[row_k : row_k + 1]
            low_sin = sin_rows[row_k : row_k + 1] * small_ref[24:25]
            up_cos = cos_rows[row_l : row_l + 1]
            up_sin = sin_rows[row_l : row_l + 1]
            table_cos = small_ref[8:16] * up_cos - small_ref[16:24] * up_sin
            table_sin = small_ref[16:24] * up_cos + small_ref[8:16] * up_sin
            table_cos = jnp.concatenate([table_cos] * (Q // 8), axis=0)
            table_sin = jnp.concatenate([table_sin] * (Q // 8), axis=0)
            up_even, up_odd = from_even[:, :LANES], from_odd[:, :LANES]
            up_re = jnp.where(left_half, up_even, up_odd)
            up_im = pltpu.roll(jnp.where(left_half, up_odd, up_even), LANES // 2, 1)
            re_h, re_l = split(up_re * table_cos + up_im * table_sin)
            im_h, im_l = split(up_im * table_cos - up_re * table_sin)
            for ref, real, imag in ((rhs_h, re_h, im_h), (rhs_l, re_l, im_l)):
                ref[0:Q, 0:LW] = real
                ref[0:Q, LW : 2 * LW] = -imag
                ref[Q : 2 * Q, 0:LW] = imag
                ref[Q : 2 * Q, LW : 2 * LW] = real
            low = from_even[:, LANES:] + from_odd[:, LANES:]
            low = low * low_cos + pltpu.roll(low, LANES // 2, 1) * low_sin
            low = low.T * norm
            low_re, low_im = low[:width], low[width:]
            for part in range(4):
                at = slice(part * quarter, (part + 1) * quarter)
                c = cos_rows[part : part + 1]
                s = sin_rows[part : part + 1]
                center_re[at] = low_re[at] * c + low_im[at] * s
                center_im[at] = low_im[at] * c - low_re[at] * s

        def correlate(place, slot):
            rhs_h, rhs_l, center_re, center_im = slot
            turn = pl.multiple_of((place // BLOCKS) * rows, 8)
            cos_rows = cos_ref[pl.ds(turn, rows), :]
            sin_rows = sin_ref[pl.ds(turn, rows), :]
            right = (rhs_h[...], rhs_l[...])
            group_size = min(pairs, 4)
            for base_pair in range(0, pairs, group_size):
                parts = []
                for pair in range(base_pair, base_pair + group_size):
                    c = cos_rows[4 + pair : 5 + pair]
                    s = sin_rows[4 + pair : 5 + pair]
                    t1 = center_re[...] * c
                    t2 = center_im[...] * s
                    t3 = center_im[...] * c
                    t4 = center_re[...] * s
                    parts.append(jnp.concatenate([t1 + t2, t3 - t4], axis=1))
                    parts.append(jnp.concatenate([t1 - t2, t3 + t4], axis=1))
                left = split(jnp.concatenate(parts, axis=0))
                total = dot3(left, right)
                for index in range(2 * group_size):
                    pair = base_pair + index // 2
                    at = (pairs - 1 - pair if index % 2 else pairs + pair) * width
                    put = slice(at, at + width)
                    re = total[index * width : (index + 1) * width, :LW]
                    im = total[index * width : (index + 1) * width, LW:]
                    acc_re[put] = acc_re[put] + re
                    acc_im[put] = acc_im[put] + im
                    acc_sq[put] = jnp.maximum(acc_sq[put], re * re + im * im)

        def block_at(index):
            return plan_ref[first_block + index]

        def work(first, side, more):
            if more:
                channelize((block_at(first + 2), block_at(first + 3)), slots[1 - side])
            for item in range(2):
                correlate(block_at(first + item), slots[side][item])

        def step(index, carry):
            work(4 * index, 0, True)
            work(4 * index + 2, 1, True)
            return carry

        channelize((block_at(0), block_at(1)), slots[0])
        lax.fori_loop(0, count // 4 - 1, step, 0)
        work(count - 4, 0, True)
        work(count - 2, 1, False)
        if opening:
            return
        lanes = lax.broadcasted_iota(jnp.int32, (quarter, LW), 1)
        source = lax.shift_right_logical(lanes, 1) + (LW // 2) * (lanes & 1)

        def natural(value):
            return jnp.take_along_axis(value, source, axis=1, mode="promise_in_bounds")

        for bin_index in range(bins):
            for part, kappa in enumerate((0, 2, 1, 3)):
                first = bin_index * width + part * quarter
                take = slice(first, first + quarter)
                put = pl.ds(kappa, quarter, stride=4)
                held_ref[bin_index, put, :] = natural(jnp.sqrt(acc_sq[take]))
                coherent_ref[0, bin_index, put, :] = natural(acc_re[take] * blend)
                coherent_ref[1, bin_index, put, :] = natural(acc_im[take] * blend)

    vmem = pl.BlockSpec(memory_space=pltpu.VMEM)
    slot = [
        pltpu.VMEM((2 * Q, 2 * LW), jnp.bfloat16),
        pltpu.VMEM((2 * Q, 2 * LW), jnp.bfloat16),
        pltpu.VMEM((width, Q), jnp.float32),
        pltpu.VMEM((width, Q), jnp.float32),
    ]
    sums = [(bins * width, LW)] * 3
    if opening:
        shapes = sums + [(slabs * rows, LANES)] * 2 + [(depth, PAD, LANES)]
        scratch = [(PAD + blocks * Q, LANES), (slabs * PAD, LANES)]
    else:
        shapes = [(bins, width, LW), (2, bins, width, LW)]
        scratch = [(PAD + blocks * Q, LANES)] + sums
    work = 2 * 3 * count * NCH * NCH * (2 * Q + 2 * bins * width // 2)
    return pl.pallas_call(
        kernel,
        in_specs=[pl.BlockSpec(memory_space=pltpu.SMEM)] + [vmem] * (7 + inputs),
        out_specs=[vmem] * outputs,
        scratch_shapes=[pltpu.VMEM(shape, jnp.float32) for shape in scratch] + slot * 4,
        out_shape=[jax.ShapeDtypeStruct(shape, jnp.float32) for shape in shapes],
        compiler_params=pltpu.CompilerParams(vmem_limit_bytes=(PAD + blocks * Q) * 4 * LANES + 12 * 1024 * 1024),
        cost_estimate=pl.CostEstimate(flops=work, transcendentals=0, bytes_accessed=4 * 1024 * 1024),
        name="surfaces_first" if opening else "surfaces_last",
    )(
        plan,
        jnp.asarray(fixed),
        jnp.asarray(ticks),
        jnp.asarray(small),
        *[jnp.asarray(table) for table in weights],
        *pieces,
        *notes,
        *(() if opening else carried),
    )


def on_device(capture, dropped):
    slabs = lax.axis_size("slab")
    groups = lax.axis_size("grp")
    slab = lax.axis_index("slab")
    group = lax.axis_index("grp")
    axes = ("slab", "grp")
    total = slabs * groups
    outer = slabs // 4
    hops = capture.shape[1] // HOP
    own = capture.reshape(2, hops, HOP).transpose(1, 0, 2).reshape(hops, 2 * HOP)
    ticks = jnp.broadcast_to(dropped.astype(jnp.float32)[:, None], (PAD, LANES))
    own = jnp.concatenate([own, ticks], axis=0)[None]
    lead = NCH // HOP - 1

    def split_index(flat):
        return flat // (4 * groups), (flat // (2 * groups)) % 2, (flat // groups) % 2, flat % groups

    def joined(far, side, core, member):
        return ((far * 2 + side) * 2 + core) * groups + member

    def moved(array, by):
        pairs = []
        for flat in range(total):
            far, side, core, member = split_index(flat)
            target = joined(
                (far + by[0]) % outer, (side + by[1]) % 2, (core + by[2]) % 2, (member + by[3]) % groups
            )
            pairs.append((flat, target))
        return lax.ppermute(array, axes, pairs)

    line = [own]
    for step in range(1, outer):
        line.append(moved(own, (step, 0, 0, 0)))
    line = jnp.concatenate(line, axis=0)
    tiles = jnp.concatenate([line[:, hops : hops + PAD - lead], line[:, hops - lead : hops]], axis=1)
    note_steps = [(1, core, member) for core in range(2) for member in range(groups)]
    notes = []
    for by in note_steps:
        notes.append(moved(tiles, (0,) + by))
    near = [line] + [moved(line, (0, 0, 0, member)) for member in range(1, groups)]
    far = [moved(line, (0, 1, 0, 0))]
    far += [moved(piece, (0, 1, 0, 0)) for piece in near[1:]]
    near_steps = [(0, 0, member) for member in range(groups)]
    far_steps = [(1, 0, member) for member in range(groups)]
    cores = []
    for piece in near:
        cores.append(moved(piece, (0, 0, 1, 0)))
    near += cores
    near_steps += [(side, 1, member) for side, _, member in near_steps]
    me_far, me_side, me_core, me_member = split_index(slab * groups + group)

    def places(steps):
        return [
            joined(
                (me_far - step) % outer,
                (me_side - side) % 2,
                (me_core - core) % 2,
                (me_member - member) % groups,
            )
            for side, core, member in steps
            for step in range(outer)
        ]

    first_blocks = []
    last_blocks = []
    for step in range(outer):
        for core in range(2):
            for member in range(groups):
                first_blocks.append(joined(step, me_side, core, member))
                last_blocks.append(joined(step, 1 - me_side, core, member))
    tail_places = [joined(step, me_side, 1, groups - 1) for step in range(outer)]
    far_steps += [(side, 1, member) for side, _, member in far_steps]
    parts = [places(near_steps), places(far_steps), places(note_steps), tail_places]
    parts += [first_blocks, last_blocks]
    begins = np.cumsum([2] + [len(part) for part in parts])
    near_at, far_at, note_at, tail_at, first_at, last_at = (int(at) for at in begins[:-1])
    plan = [slab, group] + sum(parts, [])
    plan = jnp.stack([jnp.asarray(value, jnp.int32) for value in plan])
    spots = (near_at, note_at, tail_at, first_at)
    carried = surfaces(plan, spots, near, slabs, groups, len(first_blocks), notes=notes)
    far += [moved(far[0], (0, 0, 1, 0))]
    far += [moved(piece, (0, 0, 1, 0)) for piece in far[1:groups]]
    spots = (far_at, note_at, tail_at, last_at)
    held, coherent = surfaces(
        plan, spots, far, slabs, groups, len(last_blocks), carried=carried
    )
    return held, coherent


def solution(mesh):
    in_specs = (P(None, ("slab", "grp")), P("slab"))
    out_specs = (P("slab", "grp", None), P(None, "slab", "grp", None))

    return jax.shard_map(
        on_device, mesh=mesh, in_specs=in_specs, out_specs=out_specs, check_vma=False
    )
```

```python
import math

import jax
import jax.numpy as jnp
import ml_dtypes
import numpy as np
from jax import lax
from jax.experimental import pallas as pl
from jax.experimental.pallas import tpu as pltpu
from jax.sharding import PartitionSpec as P


NCH = 256
HOP = 64
KW = 128
LW = 128
Q = 128
BLOCKS = 2
PERIOD = Q * HOP
TURN = 2 * PERIOD
LANES = 128
PAD = 8


def halves(table):
    high = table.astype(ml_dtypes.bfloat16)
    low = (table - high.astype(np.float64)).astype(ml_dtypes.bfloat16)
    return high, low


def lower_order(width):
    quarter = width // 4
    return np.concatenate([4 * np.arange(quarter) + kappa for kappa in (0, 2, 1, 3)])


def upper_order():
    return np.concatenate([np.arange(0, LW, 2), np.arange(1, LW, 2)])


def window_rows():
    taps = np.arange(NCH)
    window = 0.5 - 0.5 * np.cos(2.0 * np.pi * taps / NCH)
    scaled = window / np.sqrt(np.sum(window * window))
    rows = np.zeros((8, LANES))
    for lag in range(NCH // HOP):
        piece = scaled[lag * HOP : (lag + 1) * HOP]
        rows[lag] = np.concatenate([piece, piece])
    return rows.astype(np.float32)


def channel_tables(groups):
    width = KW // groups
    half = width // 2
    taps = np.arange(NCH // 2)
    even = np.zeros((groups, NCH, NCH))
    odd = np.zeros((groups, NCH, NCH))

    def columns(channels):
        turns = 2.0 * np.pi * (taps[:, None] * channels[None, :] % NCH) / NCH
        cosine, sine = np.cos(turns), np.sin(turns)
        real = np.concatenate([cosine[:HOP], sine[:HOP], cosine[HOP:], sine[HOP:]])
        imag = np.concatenate([-sine[:HOP], cosine[:HOP], -sine[HOP:], cosine[HOP:]])
        return real, imag

    upper = KW + upper_order()
    for group in range(groups):
        lower = group * width + lower_order(width)
        real, imag = columns(upper[: LW // 2])
        even[group, :, 0:64], even[group, :, 64:128] = real, imag
        real, imag = columns(upper[LW // 2 :])
        odd[group, :, 0:64], odd[group, :, 64:128] = imag, real
        real, imag = columns(lower[:half])
        even[group, :, 128 : 128 + half] = real
        even[group, :, 192 : 192 + half] = imag
        real, imag = columns(lower[half:])
        odd[group, :, 128 + half : 128 + width] = real
        odd[group, :, 192 + half : 192 + width] = imag
    return halves(even) + halves(odd)


def turn_tables(bins, width):
    pairs = bins // 2
    rows = -(-(6 + pairs) // 8) * 8
    frame = np.arange(LANES)
    fixed = np.zeros((3, rows, LANES), np.int64)
    ticks = np.zeros((3, rows, LANES), np.int64)
    for place, kappa in enumerate((0, 2, 1, 3)):
        ticks[0, place] = bins - 1
        ticks[1, place] = 2 * bins
        fixed[0, place] = (bins - 1) * HOP * frame + (TURN // 4) * kappa * frame
        fixed[1, place] = 2 * bins * HOP * frame
    for pair in range(pairs):
        ticks[0, 4 + pair] = 2 * pair + 1
        fixed[0, 4 + pair] = (2 * pair + 1) * HOP * frame
    order = lower_order(width)
    scale = TURN // NCH
    ticks[0, 4 + pairs] = scale * np.concatenate([order, order])
    ticks[2, 4 + pairs] = scale * width
    ticks[0, 5 + pairs] = scale * (KW + upper_order())
    return fixed.astype(np.int32), ticks.astype(np.int32)


def cos_sin(angle):
    shifted = angle + TURN // 8
    quadrant = lax.shift_right_logical(shifted, int(math.log2(TURN // 4))) & 3
    remain = (shifted & (TURN // 4 - 1)) - TURN // 8
    x = remain.astype(jnp.float32) * np.float32(2.0 * math.pi / TURN)
    y = x * x
    sine = x * (1.0 + y * (-1.0 / 6 + y * (1.0 / 120 + y * (-1.0 / 5040 + y * (1.0 / 362880)))))
    cosine = 1.0 + y * (-0.5 + y * (1.0 / 24 + y * (-1.0 / 720 + y * (1.0 / 40320))))
    swap = (quadrant & 1) == 1
    out_cos = jnp.where(swap, sine, cosine)
    out_sin = jnp.where(swap, cosine, sine)
    out_cos = jnp.where((quadrant == 1) | (quadrant == 2), -out_cos, out_cos)
    out_sin = jnp.where(quadrant >= 2, -out_sin, out_sin)
    return out_cos, out_sin


def split(value):
    high = value.astype(jnp.bfloat16)
    low = (value - high.astype(jnp.float32)).astype(jnp.bfloat16)
    return high, low


def dot32(left, right):
    return lax.dot_general(
        left, right, (((1,), (0,)), ((), ())), preferred_element_type=jnp.float32
    )


def dot3(left, right):
    return dot32(left[0], right[0]) + dot32(left[1], right[0]) + dot32(left[0], right[1])


def small_table(width):
    order = KW + upper_order()
    phase = (np.arange(8)[:, None] * order[None, :]) % 4
    quarter_cos = np.array([1.0, 0.0, -1.0, 0.0])[phase]
    quarter_sin = np.array([0.0, 1.0, 0.0, -1.0])[phase]
    sign = np.where(np.arange(LANES) < width, 1.0, -1.0)[None, :]
    parts = [window_rows(), quarter_cos, quarter_sin, np.tile(sign, (8, 1))]
    return np.concatenate(parts).astype(np.float32)


def surfaces(plan, spots, pieces, slabs, groups, count, notes=(), carried=None):
    piece_at, note_at, tail_at, first_block = spots
    bins = Q // slabs
    pairs = bins // 2
    width = KW // groups
    quarter = width // 4
    blocks = slabs * BLOCKS
    fixed, ticks = turn_tables(bins, width)
    rows = fixed.shape[1]
    weights = channel_tables(groups)
    small = small_table(width)
    arrays = len(pieces)
    depth = pieces[0].shape[0]
    norm = 1.0 / math.sqrt(Q)
    blend = 1.0 / math.sqrt(slabs * BLOCKS)
    opening = carried is None
    inputs = arrays + len(notes) + (0 if opening else 5)
    outputs = 5 if opening else 2

    def kernel(plan_ref, fixed_ref, ticks_ref, small_ref, even_h, even_l, odd_h, odd_l, *rest):
        piece_refs = rest[:arrays]
        note_refs = rest[arrays : arrays + len(notes)]
        out_refs = rest[inputs : inputs + outputs]
        rest = rest[inputs + outputs :] if opening else rest[arrays:]
        if opening:
            acc_re, acc_im, acc_sq, stamps, tails = out_refs
            frames, drops = rest[:2]
            scratch = rest[2:]
        else:
            old_re, old_im, old_sq, stamps, tails = rest[:5]
            held_ref, coherent_ref = out_refs
            frames, acc_re, acc_im, acc_sq = rest[7:11]
            scratch = rest[11:]
        slots = ((scratch[0:4], scratch[4:8]), (scratch[8:12], scratch[12:16]))
        turns = (scratch[16:18], scratch[18:20])
        base = fixed_ref[0] + plan_ref[0] * fixed_ref[1] + plan_ref[1] * fixed_ref[2]
        rate = ticks_ref[0] + plan_ref[0] * ticks_ref[1] + plan_ref[1] * ticks_ref[2]
        group = plan_ref[1]
        frames[pl.ds(0, PAD), :] = jnp.zeros((PAD, LANES), jnp.float32)
        for array in range(arrays):
            for item in range(depth):
                place = plan_ref[piece_at + array * depth + item]
                start = pl.multiple_of(PAD + place * Q, 8)
                frames[pl.ds(start, Q), :] = piece_refs[array][item, pl.ds(0, Q), :]
                if opening:
                    start = pl.multiple_of((place // BLOCKS) * PAD, 8)
                    drops[pl.ds(start, PAD), :] = piece_refs[array][item, pl.ds(Q, PAD), :]
        for array in range(len(notes)):
            for item in range(depth):
                place = plan_ref[note_at + array * depth + item]
                tile = note_refs[array][item]
                frames[pl.ds(pl.multiple_of((place + 1) * Q, 8), PAD), :] = tile
                drops[pl.ds(pl.multiple_of((place // BLOCKS) * PAD, 8), PAD), :] = tile
        for item in range(depth):
            at = pl.ds(pl.multiple_of((plan_ref[tail_at + item] + 1) * Q, 8), PAD)
            if opening:
                tails[item] = frames[at, :]
            else:
                frames[at, :] = tails[item]

        def make_stamps():
            def stamp_step(n, total):
                at = pl.ds(pl.multiple_of(n * PAD, 8), PAD)
                dropped = jnp.broadcast_to(drops[at, :][0:1], (PAD, LANES)).astype(jnp.int32)
                total = (total + dropped) & (PERIOD - 1)
                stamps[at, :] = total
                return total

            start = jnp.zeros((PAD, LANES), jnp.int32)
            lax.fori_loop(0, slabs, stamp_step, start, unroll=min(slabs, 16))

        if opening:
            acc_re[...] = jnp.zeros_like(acc_re)
            acc_im[...] = jnp.zeros_like(acc_im)
            acc_sq[...] = jnp.zeros_like(acc_sq)
            make_stamps()
        else:
            acc_re[...] = old_re[...]
            acc_im[...] = old_im[...]
            acc_sq[...] = old_sq[...]
        lane = lax.broadcasted_iota(jnp.int32, (Q, LANES), 1)
        left_half = lane < LANES // 2

        def channelize(places, side):
            targets = slots[side]
            at = pl.ds(pl.multiple_of((places[0] // BLOCKS) * PAD, 8), PAD)
            wide = jnp.concatenate([stamps[at, :]] * (rows // PAD), axis=0)
            cos_rows, sin_rows = cos_sin((base + rate * wide) & (TURN - 1))
            turns[side][0][...] = cos_rows
            turns[side][1][...] = sin_rows
            evens = []
            odds = []
            for place in places:
                start = pl.multiple_of(place * Q, Q)
                lags = [
                    frames[pl.ds(start + (PAD - 3 + lag), Q), :] * small_ref[lag : lag + 1]
                    for lag in range(4)
                ]
                evens.append(jnp.concatenate([lags[0] + lags[2], lags[1] + lags[3]], axis=1))
                odds.append(jnp.concatenate([lags[0] - lags[2], lags[1] - lags[3]], axis=1))
            both_even = split(jnp.concatenate(evens, axis=0))
            both_odd = split(jnp.concatenate(odds, axis=0))
            from_even = dot3(both_even, (even_h[group], even_l[group]))
            from_odd = dot3(both_odd, (odd_h[group], odd_l[group]))
            for index, slot in enumerate(targets):
                part = slice(index * Q, (index + 1) * Q)
                finish(cos_rows, sin_rows, slot, from_even[part], from_odd[part])

        def finish(cos_rows, sin_rows, slot, from_even, from_odd):
            rhs_h, rhs_l, center_re, center_im = slot
            row_k, row_l = 4 + pairs, 5 + pairs
            low_cos = cos_rows[row_k : row_k + 1]
            low_sin = sin_rows[row_k : row_k + 1] * small_ref[24:25]
            up_cos = cos_rows[row_l : row_l + 1]
            up_sin = sin_rows[row_l : row_l + 1]
            table_cos = small_ref[8:16] * up_cos - small_ref[16:24] * up_sin
            table_sin = small_ref[16:24] * up_cos + small_ref[8:16] * up_sin
            table_cos = jnp.concatenate([table_cos] * (Q // 8), axis=0)
            table_sin = jnp.concatenate([table_sin] * (Q // 8), axis=0)
            up_even, up_odd = from_even[:, :LANES], from_odd[:, :LANES]
            up_re = jnp.where(left_half, up_even, up_odd)
            up_im = pltpu.roll(jnp.where(left_half, up_odd, up_even), LANES // 2, 1)
            re_h, re_l = split(up_re * table_cos + up_im * table_sin)
            im_h, im_l = split(up_im * table_cos - up_re * table_sin)
            for ref, real, imag in ((rhs_h, re_h, im_h), (rhs_l, re_l, im_l)):
                ref[0:Q, 0:LW] = real
                ref[0:Q, LW : 2 * LW] = -imag
                ref[Q : 2 * Q, 0:LW] = imag
                ref[Q : 2 * Q, LW : 2 * LW] = real
            low = from_even[:, LANES:] + from_odd[:, LANES:]
            low = low * low_cos + pltpu.roll(low, LANES // 2, 1) * low_sin
            low = low.T * norm
            low_re, low_im = low[:width], low[width:]
            for part in range(4):
                at = slice(part * quarter, (part + 1) * quarter)
                c = cos_rows[part : part + 1]
                s = sin_rows[part : part + 1]
                center_re[at] = low_re[at] * c + low_im[at] * s
                center_im[at] = low_im[at] * c - low_re[at] * s

        def correlate(turn, slot):
            rhs_h, rhs_l, center_re, center_im = slot
            cos_rows = turn[0][...]
            sin_rows = turn[1][...]
            right = (rhs_h[...], rhs_l[...])
            group_size = min(pairs, 4)
            for base_pair in range(0, pairs, group_size):
                parts = []
                for pair in range(base_pair, base_pair + group_size):
                    c = cos_rows[4 + pair : 5 + pair]
                    s = sin_rows[4 + pair : 5 + pair]
                    t1 = center_re[...] * c
                    t2 = center_im[...] * s
                    t3 = center_im[...] * c
                    t4 = center_re[...] * s
                    parts.append(jnp.concatenate([t1 + t2, t3 - t4], axis=1))
                    parts.append(jnp.concatenate([t1 - t2, t3 + t4], axis=1))
                left = split(jnp.concatenate(parts, axis=0))
                total = dot3(left, right)
                for index in range(2 * group_size):
                    pair = base_pair + index // 2
                    at = (pairs - 1 - pair if index % 2 else pairs + pair) * width
                    put = slice(at, at + width)
                    re = total[index * width : (index + 1) * width, :LW]
                    im = total[index * width : (index + 1) * width, LW:]
                    acc_re[put] = acc_re[put] + re
                    acc_im[put] = acc_im[put] + im
                    acc_sq[put] = jnp.maximum(acc_sq[put], re * re + im * im)

        def block_at(index):
            return plan_ref[first_block + index]

        def work(first, side, more):
            if more:
                channelize((block_at(first + 2), block_at(first + 3)), 1 - side)
            for item in range(2):
                correlate(turns[side], slots[side][item])

        def step(index, carry):
            work(4 * index, 0, True)
            work(4 * index + 2, 1, True)
            return carry

        channelize((block_at(0), block_at(1)), 0)
        lax.fori_loop(0, count // 4 - 1, step, 0)
        work(count - 4, 0, True)
        work(count - 2, 1, False)
        if opening:
            return
        lanes = lax.broadcasted_iota(jnp.int32, (quarter, LW), 1)
        source = lax.shift_right_logical(lanes, 1) + (LW // 2) * (lanes & 1)

        def natural(value):
            return jnp.take_along_axis(value, source, axis=1, mode="promise_in_bounds")

        for bin_index in range(bins):
            for part, kappa in enumerate((0, 2, 1, 3)):
                first = bin_index * width + part * quarter
                take = slice(first, first + quarter)
                put = pl.ds(kappa, quarter, stride=4)
                held_ref[bin_index, put, :] = natural(jnp.sqrt(acc_sq[take]))
                coherent_ref[0, bin_index, put, :] = natural(acc_re[take] * blend)
                coherent_ref[1, bin_index, put, :] = natural(acc_im[take] * blend)

    vmem = pl.BlockSpec(memory_space=pltpu.VMEM)
    slot = [
        pltpu.VMEM((2 * Q, 2 * LW), jnp.bfloat16),
        pltpu.VMEM((2 * Q, 2 * LW), jnp.bfloat16),
        pltpu.VMEM((width, Q), jnp.float32),
        pltpu.VMEM((width, Q), jnp.float32),
    ]
    sums = [(bins * width, LW)] * 3
    if opening:
        shapes = sums + [(slabs * PAD, LANES), (depth, PAD, LANES)]
        scratch = [(PAD + blocks * Q, LANES), (slabs * PAD, LANES)]
    else:
        shapes = [(bins, width, LW), (2, bins, width, LW)]
        scratch = [(PAD + blocks * Q, LANES)] + sums
    work = 2 * 3 * count * NCH * NCH * (2 * Q + 2 * bins * width // 2)
    return pl.pallas_call(
        kernel,
        in_specs=[pl.BlockSpec(memory_space=pltpu.SMEM)] + [vmem] * (7 + inputs),
        out_specs=[vmem] * outputs,
        scratch_shapes=[pltpu.VMEM(shape, jnp.float32) for shape in scratch]
        + slot * 4
        + [pltpu.VMEM((rows, LANES), jnp.float32)] * 4,
        out_shape=[
            jax.ShapeDtypeStruct(shape, jnp.int32 if opening and index == 3 else jnp.float32)
            for index, shape in enumerate(shapes)
        ],
        compiler_params=pltpu.CompilerParams(vmem_limit_bytes=(PAD + blocks * Q) * 4 * LANES + 12 * 1024 * 1024),
        cost_estimate=pl.CostEstimate(flops=work, transcendentals=0, bytes_accessed=4 * 1024 * 1024),
        name="surfaces_first" if opening else "surfaces_last",
    )(
        plan,
        jnp.asarray(fixed),
        jnp.asarray(ticks),
        jnp.asarray(small),
        *[jnp.asarray(table) for table in weights],
        *pieces,
        *notes,
        *(() if opening else carried),
    )


def on_device(capture, dropped):
    slabs = lax.axis_size("slab")
    groups = lax.axis_size("grp")
    slab = lax.axis_index("slab")
    group = lax.axis_index("grp")
    axes = ("slab", "grp")
    total = slabs * groups
    outer = slabs // 4
    hops = capture.shape[1] // HOP
    own = capture.reshape(2, hops, HOP).transpose(1, 0, 2).reshape(hops, 2 * HOP)
    ticks = jnp.broadcast_to(dropped.astype(jnp.float32)[:, None], (PAD, LANES))
    own = jnp.concatenate([own, ticks], axis=0)[None]
    lead = NCH // HOP - 1

    def split_index(flat):
        return flat // (4 * groups), (flat // (2 * groups)) % 2, (flat // groups) % 2, flat % groups

    def joined(far, side, core, member):
        return ((far * 2 + side) * 2 + core) * groups + member

    def moved(array, by):
        pairs = []
        for flat in range(total):
            far, side, core, member = split_index(flat)
            target = joined(
                (far + by[0]) % outer, (side + by[1]) % 2, (core + by[2]) % 2, (member + by[3]) % groups
            )
            pairs.append((flat, target))
        return lax.ppermute(array, axes, pairs)

    line = [own]
    for step in range(1, outer):
        line.append(moved(own, (step, 0, 0, 0)))
    line = jnp.concatenate(line, axis=0)
    tiles = jnp.concatenate([line[:, hops : hops + PAD - lead], line[:, hops - lead : hops]], axis=1)
    note_steps = [(1, core, member) for core in range(2) for member in range(groups)]
    notes = []
    for by in note_steps:
        notes.append(moved(tiles, (0,) + by))
    near = [line] + [moved(line, (0, 0, 0, member)) for member in range(1, groups)]
    far = [moved(line, (0, 1, 0, 0))]
    far += [moved(piece, (0, 1, 0, 0)) for piece in near[1:]]
    near_steps = [(0, 0, member) for member in range(groups)]
    far_steps = [(1, 0, member) for member in range(groups)]
    cores = []
    for piece in near:
        cores.append(moved(piece, (0, 0, 1, 0)))
    near += cores
    near_steps += [(side, 1, member) for side, _, member in near_steps]
    me_far, me_side, me_core, me_member = split_index(slab * groups + group)

    def places(steps):
        return [
            joined(
                (me_far - step) % outer,
                (me_side - side) % 2,
                (me_core - core) % 2,
                (me_member - member) % groups,
            )
            for side, core, member in steps
            for step in range(outer)
        ]

    first_blocks = []
    last_blocks = []
    for step in range(outer):
        for core in range(2):
            for member in range(groups):
                first_blocks.append(joined(step, me_side, core, member))
                last_blocks.append(joined(step, 1 - me_side, core, member))
    tail_places = [joined(step, me_side, 1, groups - 1) for step in range(outer)]
    far_steps += [(side, 1, member) for side, _, member in far_steps]
    parts = [places(near_steps), places(far_steps), places(note_steps), tail_places]
    parts += [first_blocks, last_blocks]
    begins = np.cumsum([2] + [len(part) for part in parts])
    near_at, far_at, note_at, tail_at, first_at, last_at = (int(at) for at in begins[:-1])
    plan = [slab, group] + sum(parts, [])
    plan = jnp.stack([jnp.asarray(value, jnp.int32) for value in plan])
    spots = (near_at, note_at, tail_at, first_at)
    carried = surfaces(plan, spots, near, slabs, groups, len(first_blocks), notes=notes)
    far += [moved(far[0], (0, 0, 1, 0))]
    far += [moved(piece, (0, 0, 1, 0)) for piece in far[1:groups]]
    spots = (far_at, note_at, tail_at, last_at)
    held, coherent = surfaces(
        plan, spots, far, slabs, groups, len(last_blocks), carried=carried
    )
    return held, coherent


def solution(mesh):
    in_specs = (P(None, ("slab", "grp")), P("slab"))
    out_specs = (P("slab", "grp", None), P(None, "slab", "grp", None))

    return jax.shard_map(
        on_device, mesh=mesh, in_specs=in_specs, out_specs=out_specs, check_vma=False
    )
```

```python
import math

import jax
import jax.numpy as jnp
import ml_dtypes
import numpy as np
from jax import lax
from jax.experimental import pallas as pl
from jax.experimental.pallas import tpu as pltpu
from jax.sharding import PartitionSpec as P


NCH = 256
HOP = 64
KW = 128
LW = 128
Q = 128
BLOCKS = 2
PERIOD = Q * HOP
TURN = 2 * PERIOD
LANES = 128
PAD = 8


def halves(table):
    high = table.astype(ml_dtypes.bfloat16)
    low = (table - high.astype(np.float64)).astype(ml_dtypes.bfloat16)
    return high, low


def lower_order(width):
    quarter = width // 4
    return np.concatenate([4 * np.arange(quarter) + kappa for kappa in (0, 2, 1, 3)])


def upper_order():
    return np.concatenate([np.arange(0, LW, 2), np.arange(1, LW, 2)])


def window_rows():
    taps = np.arange(NCH)
    window = 0.5 - 0.5 * np.cos(2.0 * np.pi * taps / NCH)
    scaled = window / np.sqrt(np.sum(window * window))
    rows = np.zeros((8, LANES))
    for lag in range(NCH // HOP):
        piece = scaled[lag * HOP : (lag + 1) * HOP]
        rows[lag] = np.concatenate([piece, piece])
    return rows.astype(np.float32)


def channel_tables(groups):
    width = KW // groups
    half = width // 2
    taps = np.arange(NCH // 2)
    even = np.zeros((groups, NCH, NCH))
    odd = np.zeros((groups, NCH, NCH))

    def columns(channels):
        turns = 2.0 * np.pi * (taps[:, None] * channels[None, :] % NCH) / NCH
        cosine, sine = np.cos(turns), np.sin(turns)
        real = np.concatenate([cosine[:HOP], sine[:HOP], cosine[HOP:], sine[HOP:]])
        imag = np.concatenate([-sine[:HOP], cosine[:HOP], -sine[HOP:], cosine[HOP:]])
        return real, imag

    upper = KW + upper_order()
    for group in range(groups):
        lower = group * width + lower_order(width)
        real, imag = columns(upper[: LW // 2])
        even[group, :, 0:64], even[group, :, 64:128] = real, imag
        real, imag = columns(upper[LW // 2 :])
        odd[group, :, 0:64], odd[group, :, 64:128] = imag, real
        real, imag = columns(lower[:half])
        even[group, :, 128 : 128 + half] = real
        even[group, :, 192 : 192 + half] = imag
        real, imag = columns(lower[half:])
        odd[group, :, 128 + half : 128 + width] = real
        odd[group, :, 192 + half : 192 + width] = imag
    return halves(even) + halves(odd)


def turn_tables(bins, width):
    pairs = bins // 2
    rows = -(-(6 + pairs) // 8) * 8
    frame = np.arange(LANES)
    fixed = np.zeros((3, rows, LANES), np.int64)
    ticks = np.zeros((3, rows, LANES), np.int64)
    for place, kappa in enumerate((0, 2, 1, 3)):
        ticks[0, place] = bins - 1
        ticks[1, place] = 2 * bins
        fixed[0, place] = (bins - 1) * HOP * frame + (TURN // 4) * kappa * frame
        fixed[1, place] = 2 * bins * HOP * frame
    for pair in range(pairs):
        ticks[0, 4 + pair] = 2 * pair + 1
        fixed[0, 4 + pair] = (2 * pair + 1) * HOP * frame
    order = lower_order(width)
    scale = TURN // NCH
    ticks[0, 4 + pairs] = scale * np.concatenate([order, order])
    ticks[2, 4 + pairs] = scale * width
    ticks[0, 5 + pairs] = scale * (KW + upper_order())
    return fixed.astype(np.int32), ticks.astype(np.int32)


def cos_sin(angle):
    shifted = angle + TURN // 8
    quadrant = lax.shift_right_logical(shifted, int(math.log2(TURN // 4))) & 3
    remain = (shifted & (TURN // 4 - 1)) - TURN // 8
    x = remain.astype(jnp.float32) * np.float32(2.0 * math.pi / TURN)
    y = x * x
    sine = x * (1.0 + y * (-1.0 / 6 + y * (1.0 / 120 + y * (-1.0 / 5040 + y * (1.0 / 362880)))))
    cosine = 1.0 + y * (-0.5 + y * (1.0 / 24 + y * (-1.0 / 720 + y * (1.0 / 40320))))
    swap = (quadrant & 1) == 1
    out_cos = jnp.where(swap, sine, cosine)
    out_sin = jnp.where(swap, cosine, sine)
    out_cos = jnp.where((quadrant == 1) | (quadrant == 2), -out_cos, out_cos)
    out_sin = jnp.where(quadrant >= 2, -out_sin, out_sin)
    return out_cos, out_sin


def split(value):
    high = value.astype(jnp.bfloat16)
    low = (value - high.astype(jnp.float32)).astype(jnp.bfloat16)
    return high, low


def dot32(left, right):
    return lax.dot_general(
        left, right, (((1,), (0,)), ((), ())), preferred_element_type=jnp.float32
    )


def dot3(left, right):
    return dot32(left[0], right[0]) + dot32(left[1], right[0]) + dot32(left[0], right[1])


def small_table(width):
    order = KW + upper_order()
    phase = (np.arange(8)[:, None] * order[None, :]) % 4
    quarter_cos = np.array([1.0, 0.0, -1.0, 0.0])[phase]
    quarter_sin = np.array([0.0, 1.0, 0.0, -1.0])[phase]
    sign = np.where(np.arange(LANES) < width, 1.0, -1.0)[None, :]
    parts = [window_rows(), quarter_cos, quarter_sin, np.tile(sign, (8, 1))]
    return np.concatenate(parts).astype(np.float32)


def surfaces(plan, spots, pieces, slabs, groups, count, notes=(), carried=None):
    piece_at, note_at, tail_at, first_block = spots
    bins = Q // slabs
    pairs = bins // 2
    width = KW // groups
    quarter = width // 4
    blocks = slabs * BLOCKS
    fixed, ticks = turn_tables(bins, width)
    rows = fixed.shape[1]
    weights = channel_tables(groups)
    small = small_table(width)
    arrays = len(pieces)
    depth = pieces[0].shape[0]
    norm = 1.0 / math.sqrt(Q)
    blend = 1.0 / math.sqrt(slabs * BLOCKS)
    opening = carried is None
    inputs = arrays + len(notes) + (0 if opening else 5)
    outputs = 5 if opening else 2

    def kernel(plan_ref, fixed_ref, ticks_ref, small_ref, even_h, even_l, odd_h, odd_l, *rest):
        piece_refs = rest[:arrays]
        note_refs = rest[arrays : arrays + len(notes)]
        out_refs = rest[inputs : inputs + outputs]
        rest = rest[inputs + outputs :] if opening else rest[arrays:]
        if opening:
            acc_re, acc_im, acc_sq, stamps, tails = out_refs
            frames, drops = rest[:2]
            scratch = rest[2:]
        else:
            old_re, old_im, old_sq, stamps, tails = rest[:5]
            held_out, coherent_out = out_refs
            frames, acc_re, acc_im, acc_sq = rest[7:11]
            scratch = rest[11:]
            held_ref, coherent_ref, sems = scratch[20:23]
        slots = ((scratch[0:4], scratch[4:8]), (scratch[8:12], scratch[12:16]))
        turns = (scratch[16:18], scratch[18:20])
        base = fixed_ref[0] + plan_ref[0] * fixed_ref[1] + plan_ref[1] * fixed_ref[2]
        rate = ticks_ref[0] + plan_ref[0] * ticks_ref[1] + plan_ref[1] * ticks_ref[2]
        group = plan_ref[1]
        frames[pl.ds(0, PAD), :] = jnp.zeros((PAD, LANES), jnp.float32)
        for array in range(arrays):
            for item in range(depth):
                place = plan_ref[piece_at + array * depth + item]
                start = pl.multiple_of(PAD + place * Q, 8)
                frames[pl.ds(start, Q), :] = piece_refs[array][item, pl.ds(0, Q), :]
                if opening:
                    start = pl.multiple_of((place // BLOCKS) * PAD, 8)
                    drops[pl.ds(start, PAD), :] = piece_refs[array][item, pl.ds(Q, PAD), :]
        for array in range(len(notes)):
            for item in range(depth):
                place = plan_ref[note_at + array * depth + item]
                tile = note_refs[array][item]
                frames[pl.ds(pl.multiple_of((place + 1) * Q, 8), PAD), :] = tile
                drops[pl.ds(pl.multiple_of((place // BLOCKS) * PAD, 8), PAD), :] = tile
        for item in range(depth):
            at = pl.ds(pl.multiple_of((plan_ref[tail_at + item] + 1) * Q, 8), PAD)
            if opening:
                tails[item] = frames[at, :]
            else:
                frames[at, :] = tails[item]

        def make_stamps():
            def stamp_step(n, total):
                at = pl.ds(pl.multiple_of(n * PAD, 8), PAD)
                dropped = jnp.broadcast_to(drops[at, :][0:1], (PAD, LANES)).astype(jnp.int32)
                total = (total + dropped) & (PERIOD - 1)
                stamps[at, :] = total
                return total

            start = jnp.zeros((PAD, LANES), jnp.int32)
            lax.fori_loop(0, slabs, stamp_step, start, unroll=min(slabs, 16))

        if opening:
            acc_re[...] = jnp.zeros_like(acc_re)
            acc_im[...] = jnp.zeros_like(acc_im)
            acc_sq[...] = jnp.zeros_like(acc_sq)
            make_stamps()
        else:
            acc_re[...] = old_re[...]
            acc_im[...] = old_im[...]
            acc_sq[...] = old_sq[...]
        lane = lax.broadcasted_iota(jnp.int32, (Q, LANES), 1)
        left_half = lane < LANES // 2

        def channelize(places, side):
            targets = slots[side]
            at = pl.ds(pl.multiple_of((places[0] // BLOCKS) * PAD, 8), PAD)
            wide = jnp.concatenate([stamps[at, :]] * (rows // PAD), axis=0)
            cos_rows, sin_rows = cos_sin((base + rate * wide) & (TURN - 1))
            turns[side][0][...] = cos_rows
            turns[side][1][...] = sin_rows
            evens = []
            odds = []
            for place in places:
                start = pl.multiple_of(place * Q, Q)
                lags = [
                    frames[pl.ds(start + (PAD - 3 + lag), Q), :] * small_ref[lag : lag + 1]
                    for lag in range(4)
                ]
                evens.append(jnp.concatenate([lags[0] + lags[2], lags[1] + lags[3]], axis=1))
                odds.append(jnp.concatenate([lags[0] - lags[2], lags[1] - lags[3]], axis=1))
            both_even = split(jnp.concatenate(evens, axis=0))
            both_odd = split(jnp.concatenate(odds, axis=0))
            from_even = dot3(both_even, (even_h[group], even_l[group]))
            from_odd = dot3(both_odd, (odd_h[group], odd_l[group]))
            for index, slot in enumerate(targets):
                part = slice(index * Q, (index + 1) * Q)
                finish(cos_rows, sin_rows, slot, from_even[part], from_odd[part])

        def finish(cos_rows, sin_rows, slot, from_even, from_odd):
            rhs_h, rhs_l, center_re, center_im = slot
            row_k, row_l = 4 + pairs, 5 + pairs
            low_cos = cos_rows[row_k : row_k + 1]
            low_sin = sin_rows[row_k : row_k + 1] * small_ref[24:25]
            up_cos = cos_rows[row_l : row_l + 1]
            up_sin = sin_rows[row_l : row_l + 1]
            table_cos = small_ref[8:16] * up_cos - small_ref[16:24] * up_sin
            table_sin = small_ref[16:24] * up_cos + small_ref[8:16] * up_sin
            table_cos = jnp.concatenate([table_cos] * (Q // 8), axis=0)
            table_sin = jnp.concatenate([table_sin] * (Q // 8), axis=0)
            up_even, up_odd = from_even[:, :LANES], from_odd[:, :LANES]
            up_re = jnp.where(left_half, up_even, up_odd)
            up_im = pltpu.roll(jnp.where(left_half, up_odd, up_even), LANES // 2, 1)
            re_h, re_l = split(up_re * table_cos + up_im * table_sin)
            im_h, im_l = split(up_im * table_cos - up_re * table_sin)
            for ref, real, imag in ((rhs_h, re_h, im_h), (rhs_l, re_l, im_l)):
                ref[0:Q, 0:LW] = real
                ref[0:Q, LW : 2 * LW] = -imag
                ref[Q : 2 * Q, 0:LW] = imag
                ref[Q : 2 * Q, LW : 2 * LW] = real
            low = from_even[:, LANES:] + from_odd[:, LANES:]
            low = low * low_cos + pltpu.roll(low, LANES // 2, 1) * low_sin
            low = low.T * norm
            low_re, low_im = low[:width], low[width:]
            for part in range(4):
                at = slice(part * quarter, (part + 1) * quarter)
                c = cos_rows[part : part + 1]
                s = sin_rows[part : part + 1]
                center_re[at] = low_re[at] * c + low_im[at] * s
                center_im[at] = low_im[at] * c - low_re[at] * s

        def correlate(turn, slot):
            rhs_h, rhs_l, center_re, center_im = slot
            cos_rows = turn[0][...]
            sin_rows = turn[1][...]
            right = (rhs_h[...], rhs_l[...])
            group_size = min(pairs, 4)
            for base_pair in range(0, pairs, group_size):
                parts = []
                for pair in range(base_pair, base_pair + group_size):
                    c = cos_rows[4 + pair : 5 + pair]
                    s = sin_rows[4 + pair : 5 + pair]
                    t1 = center_re[...] * c
                    t2 = center_im[...] * s
                    t3 = center_im[...] * c
                    t4 = center_re[...] * s
                    parts.append(jnp.concatenate([t1 + t2, t3 - t4], axis=1))
                    parts.append(jnp.concatenate([t1 - t2, t3 + t4], axis=1))
                left = split(jnp.concatenate(parts, axis=0))
                total = dot3(left, right)
                for index in range(2 * group_size):
                    pair = base_pair + index // 2
                    at = (pairs - 1 - pair if index % 2 else pairs + pair) * width
                    put = slice(at, at + width)
                    re = total[index * width : (index + 1) * width, :LW]
                    im = total[index * width : (index + 1) * width, LW:]
                    acc_re[put] = acc_re[put] + re
                    acc_im[put] = acc_im[put] + im
                    acc_sq[put] = jnp.maximum(acc_sq[put], re * re + im * im)

        def block_at(index):
            return plan_ref[first_block + index]

        def work(first, side, more):
            if more:
                channelize((block_at(first + 2), block_at(first + 3)), 1 - side)
            for item in range(2):
                correlate(turns[side], slots[side][item])

        def step(index, carry):
            work(4 * index, 0, True)
            work(4 * index + 2, 1, True)
            return carry

        channelize((block_at(0), block_at(1)), 0)
        lax.fori_loop(0, count // 4 - 1, step, 0)
        work(count - 4, 0, True)
        work(count - 2, 1, False)
        if opening:
            return
        lanes = lax.broadcasted_iota(jnp.int32, (quarter, LW), 1)
        source = lax.shift_right_logical(lanes, 1) + (LW // 2) * (lanes & 1)

        def natural(value):
            return jnp.take_along_axis(value, source, axis=1, mode="promise_in_bounds")

        copies = []
        for bin_index in range(bins):
            for part, kappa in enumerate((0, 2, 1, 3)):
                first = bin_index * width + part * quarter
                take = slice(first, first + quarter)
                put = pl.ds(kappa, quarter, stride=4)
                held_ref[bin_index, put, :] = natural(jnp.sqrt(acc_sq[take]))
                coherent_ref[0, bin_index, put, :] = natural(acc_re[take] * blend)
                coherent_ref[1, bin_index, put, :] = natural(acc_im[take] * blend)
            pairs_out = [(held_ref.at[bin_index], held_out.at[bin_index])]
            for plane in range(2):
                pairs_out.append((coherent_ref.at[plane, bin_index], coherent_out.at[plane, bin_index]))
            for lane_index, (source_ref, target_ref) in enumerate(pairs_out):
                copy = pltpu.make_async_copy(source_ref, target_ref, sems.at[lane_index, bin_index])
                copy.start()
                copies.append(copy)
        for copy in copies:
            copy.wait()

    vmem = pl.BlockSpec(memory_space=pltpu.VMEM)
    slot = [
        pltpu.VMEM((2 * Q, 2 * LW), jnp.bfloat16),
        pltpu.VMEM((2 * Q, 2 * LW), jnp.bfloat16),
        pltpu.VMEM((width, Q), jnp.float32),
        pltpu.VMEM((width, Q), jnp.float32),
    ]
    sums = [(bins * width, LW)] * 3
    if opening:
        shapes = sums + [(slabs * PAD, LANES), (depth, PAD, LANES)]
        scratch = [(PAD + blocks * Q, LANES), (slabs * PAD, LANES)]
        ending = []
    else:
        shapes = [(bins, width, LW), (2, bins, width, LW)]
        scratch = [(PAD + blocks * Q, LANES)] + sums
        ending = [pltpu.VMEM(shape, jnp.float32) for shape in shapes]
        ending += [pltpu.SemaphoreType.DMA((3, bins))]
    work = 2 * 3 * count * NCH * NCH * (2 * Q + 2 * bins * width // 2)
    return pl.pallas_call(
        kernel,
        in_specs=[pl.BlockSpec(memory_space=pltpu.SMEM)] + [vmem] * (7 + inputs),
        out_specs=[vmem if opening else pl.BlockSpec(memory_space=pl.ANY)] * outputs,
        scratch_shapes=[pltpu.VMEM(shape, jnp.float32) for shape in scratch]
        + slot * 4
        + [pltpu.VMEM((rows, LANES), jnp.float32)] * 4
        + ending,
        out_shape=[
            jax.ShapeDtypeStruct(shape, jnp.int32 if opening and index == 3 else jnp.float32)
            for index, shape in enumerate(shapes)
        ],
        compiler_params=pltpu.CompilerParams(vmem_limit_bytes=(PAD + blocks * Q) * 4 * LANES + 12 * 1024 * 1024),
        cost_estimate=pl.CostEstimate(flops=work, transcendentals=0, bytes_accessed=4 * 1024 * 1024),
        name="surfaces_first" if opening else "surfaces_last",
    )(
        plan,
        jnp.asarray(fixed),
        jnp.asarray(ticks),
        jnp.asarray(small),
        *[jnp.asarray(table) for table in weights],
        *pieces,
        *notes,
        *(() if opening else carried),
    )


def on_device(capture, dropped):
    slabs = lax.axis_size("slab")
    groups = lax.axis_size("grp")
    slab = lax.axis_index("slab")
    group = lax.axis_index("grp")
    axes = ("slab", "grp")
    total = slabs * groups
    outer = slabs // 4
    hops = capture.shape[1] // HOP
    own = capture.reshape(2, hops, HOP).transpose(1, 0, 2).reshape(hops, 2 * HOP)
    ticks = jnp.broadcast_to(dropped.astype(jnp.float32)[:, None], (PAD, LANES))
    own = jnp.concatenate([own, ticks], axis=0)[None]
    lead = NCH // HOP - 1

    def split_index(flat):
        return flat // (4 * groups), (flat // (2 * groups)) % 2, (flat // groups) % 2, flat % groups

    def joined(far, side, core, member):
        return ((far * 2 + side) * 2 + core) * groups + member

    def moved(array, by):
        pairs = []
        for flat in range(total):
            far, side, core, member = split_index(flat)
            target = joined(
                (far + by[0]) % outer, (side + by[1]) % 2, (core + by[2]) % 2, (member + by[3]) % groups
            )
            pairs.append((flat, target))
        return lax.ppermute(array, axes, pairs)

    line = [own]
    for step in range(1, outer):
        line.append(moved(own, (step, 0, 0, 0)))
    own_near = [moved(own, (0, 0, 0, member)) for member in range(1, groups)]
    own_far = moved(own, (0, 1, 0, 0))
    rest = jnp.concatenate(line[1:], axis=0)
    line = jnp.concatenate(line, axis=0)
    tiles = jnp.concatenate([line[:, hops : hops + PAD - lead], line[:, hops - lead : hops]], axis=1)
    note_steps = [(1, core, member) for core in range(2) for member in range(groups)]
    notes = []
    for by in note_steps:
        notes.append(moved(tiles, (0,) + by))
    near = [moved(rest, (0, 0, 0, member)) for member in range(1, groups)]
    far = [moved(rest, (0, 1, 0, 0))]
    near = [line] + [jnp.concatenate(pair, axis=0) for pair in zip(own_near, near)]
    far = [jnp.concatenate([own_far, far[0]], axis=0)]
    far += [moved(piece, (0, 1, 0, 0)) for piece in near[1:]]
    near_steps = [(0, 0, member) for member in range(groups)]
    far_steps = [(1, 0, member) for member in range(groups)]
    cores = []
    for piece in near:
        cores.append(moved(piece, (0, 0, 1, 0)))
    near += cores
    near_steps += [(side, 1, member) for side, _, member in near_steps]
    me_far, me_side, me_core, me_member = split_index(slab * groups + group)

    def places(steps):
        return [
            joined(
                (me_far - step) % outer,
                (me_side - side) % 2,
                (me_core - core) % 2,
                (me_member - member) % groups,
            )
            for side, core, member in steps
            for step in range(outer)
        ]

    first_blocks = []
    last_blocks = []
    for step in range(outer):
        for core in range(2):
            for member in range(groups):
                first_blocks.append(joined(step, me_side, core, member))
                last_blocks.append(joined(step, 1 - me_side, core, member))
    tail_places = [joined(step, me_side, 1, groups - 1) for step in range(outer)]
    far_steps += [(side, 1, member) for side, _, member in far_steps]
    parts = [places(near_steps), places(far_steps), places(note_steps), tail_places]
    parts += [first_blocks, last_blocks]
    begins = np.cumsum([2] + [len(part) for part in parts])
    near_at, far_at, note_at, tail_at, first_at, last_at = (int(at) for at in begins[:-1])
    plan = [slab, group] + sum(parts, [])
    plan = jnp.stack([jnp.asarray(value, jnp.int32) for value in plan])
    spots = (near_at, note_at, tail_at, first_at)
    carried = surfaces(plan, spots, near, slabs, groups, len(first_blocks), notes=notes)
    far += [moved(far[0], (0, 0, 1, 0))]
    far += [moved(piece, (0, 0, 1, 0)) for piece in far[1:groups]]
    spots = (far_at, note_at, tail_at, last_at)
    held, coherent = surfaces(
        plan, spots, far, slabs, groups, len(last_blocks), carried=carried
    )
    return held, coherent


def solution(mesh):
    in_specs = (P(None, ("slab", "grp")), P("slab"))
    out_specs = (P("slab", "grp", None), P(None, "slab", "grp", None))

    return jax.shard_map(
        on_device, mesh=mesh, in_specs=in_specs, out_specs=out_specs, check_vma=False
    )
```

```python
import math

import jax
import jax.numpy as jnp
import ml_dtypes
import numpy as np
from jax import lax
from jax.experimental import pallas as pl
from jax.experimental.pallas import tpu as pltpu
from jax.sharding import PartitionSpec as P


NCH = 256
HOP = 64
KW = 128
LW = 128
Q = 128
BLOCKS = 2
PERIOD = Q * HOP
TURN = 2 * PERIOD
LANES = 128
PAD = 8


def halves(table):
    high = table.astype(ml_dtypes.bfloat16)
    low = (table - high.astype(np.float64)).astype(ml_dtypes.bfloat16)
    return high, low


def lower_order(width):
    quarter = width // 4
    return np.concatenate([4 * np.arange(quarter) + kappa for kappa in (0, 2, 1, 3)])


def upper_order():
    return np.concatenate([np.arange(0, LW, 2), np.arange(1, LW, 2)])


def window_rows():
    taps = np.arange(NCH)
    window = 0.5 - 0.5 * np.cos(2.0 * np.pi * taps / NCH)
    scaled = window / np.sqrt(np.sum(window * window))
    rows = np.zeros((8, LANES))
    for lag in range(NCH // HOP):
        piece = scaled[lag * HOP : (lag + 1) * HOP]
        rows[lag] = np.concatenate([piece, piece])
    return rows.astype(np.float32)


def channel_tables(groups):
    width = KW // groups
    half = width // 2
    taps = np.arange(NCH // 2)
    even = np.zeros((groups, NCH, NCH))
    odd = np.zeros((groups, NCH, NCH))

    def columns(channels):
        turns = 2.0 * np.pi * (taps[:, None] * channels[None, :] % NCH) / NCH
        cosine, sine = np.cos(turns), np.sin(turns)
        real = np.concatenate([cosine[:HOP], sine[:HOP], cosine[HOP:], sine[HOP:]])
        imag = np.concatenate([-sine[:HOP], cosine[:HOP], -sine[HOP:], cosine[HOP:]])
        return real, imag

    upper = KW + upper_order()
    for group in range(groups):
        lower = group * width + lower_order(width)
        real, imag = columns(upper[: LW // 2])
        even[group, :, 0:64], even[group, :, 64:128] = real, imag
        real, imag = columns(upper[LW // 2 :])
        odd[group, :, 0:64], odd[group, :, 64:128] = imag, real
        real, imag = columns(lower[:half])
        even[group, :, 128 : 128 + half] = real
        even[group, :, 192 : 192 + half] = imag
        real, imag = columns(lower[half:])
        odd[group, :, 128 + half : 128 + width] = real
        odd[group, :, 192 + half : 192 + width] = imag
    return halves(even) + halves(odd)


def turn_tables(bins, width):
    pairs = bins // 2
    rows = -(-(6 + pairs) // 8) * 8
    frame = np.arange(LANES)
    fixed = np.zeros((3, rows, LANES), np.int64)
    ticks = np.zeros((3, rows, LANES), np.int64)
    for place, kappa in enumerate((0, 2, 1, 3)):
        ticks[0, place] = bins - 1
        ticks[1, place] = 2 * bins
        fixed[0, place] = (bins - 1) * HOP * frame + (TURN // 4) * kappa * frame
        fixed[1, place] = 2 * bins * HOP * frame
    for pair in range(pairs):
        ticks[0, 4 + pair] = 2 * pair + 1
        fixed[0, 4 + pair] = (2 * pair + 1) * HOP * frame
    order = lower_order(width)
    scale = TURN // NCH
    ticks[0, 4 + pairs] = scale * np.concatenate([order, order])
    ticks[2, 4 + pairs] = scale * width
    ticks[0, 5 + pairs] = scale * (KW + upper_order())
    return fixed.astype(np.int32), ticks.astype(np.int32)


def cos_sin(angle):
    shifted = angle + TURN // 8
    quadrant = lax.shift_right_logical(shifted, int(math.log2(TURN // 4))) & 3
    remain = (shifted & (TURN // 4 - 1)) - TURN // 8
    x = remain.astype(jnp.float32) * np.float32(2.0 * math.pi / TURN)
    y = x * x
    sine = x * (1.0 + y * (-1.0 / 6 + y * (1.0 / 120 + y * (-1.0 / 5040 + y * (1.0 / 362880)))))
    cosine = 1.0 + y * (-0.5 + y * (1.0 / 24 + y * (-1.0 / 720 + y * (1.0 / 40320))))
    swap = (quadrant & 1) == 1
    out_cos = jnp.where(swap, sine, cosine)
    out_sin = jnp.where(swap, cosine, sine)
    out_cos = jnp.where((quadrant == 1) | (quadrant == 2), -out_cos, out_cos)
    out_sin = jnp.where(quadrant >= 2, -out_sin, out_sin)
    return out_cos, out_sin


def split(value):
    high = value.astype(jnp.bfloat16)
    low = (value - high.astype(jnp.float32)).astype(jnp.bfloat16)
    return high, low


def dot32(left, right):
    return lax.dot_general(
        left, right, (((1,), (0,)), ((), ())), preferred_element_type=jnp.float32
    )


def dot3(left, right):
    return dot32(left[0], right[0]) + dot32(left[1], right[0]) + dot32(left[0], right[1])


def small_table(width):
    order = KW + upper_order()
    phase = (np.arange(8)[:, None] * order[None, :]) % 4
    quarter_cos = np.array([1.0, 0.0, -1.0, 0.0])[phase]
    quarter_sin = np.array([0.0, 1.0, 0.0, -1.0])[phase]
    sign = np.where(np.arange(LANES) < width, 1.0, -1.0)[None, :]
    parts = [window_rows(), quarter_cos, quarter_sin, np.tile(sign, (8, 1))]
    return np.concatenate(parts).astype(np.float32)


def surfaces(plan, spots, pieces, slabs, groups, count, notes=(), carried=None):
    piece_at, note_at, tail_at, first_block = spots
    bins = Q // slabs
    pairs = bins // 2
    width = KW // groups
    quarter = width // 4
    blocks = slabs * BLOCKS
    fixed, ticks = turn_tables(bins, width)
    rows = fixed.shape[1]
    weights = channel_tables(groups)
    small = small_table(width)
    arrays = len(pieces)
    depth = pieces[0].shape[0]
    norm = 1.0 / math.sqrt(Q)
    blend = 1.0 / math.sqrt(slabs * BLOCKS)
    opening = carried is None
    inputs = arrays + len(notes) + (0 if opening else 5)
    outputs = 5 if opening else 2

    def kernel(plan_ref, fixed_ref, ticks_ref, small_ref, even_h, even_l, odd_h, odd_l, *rest):
        piece_refs = rest[:arrays]
        note_refs = rest[arrays : arrays + len(notes)]
        out_refs = rest[inputs : inputs + outputs]
        rest = rest[inputs + outputs :] if opening else rest[arrays:]
        if opening:
            acc_re, acc_im, acc_sq, stamps, tails = out_refs
            frames, drops = rest[:2]
            scratch = rest[2:]
        else:
            old_re, old_im, old_sq, stamps, tails = rest[:5]
            held_ref, coherent_ref = out_refs
            frames, acc_re, acc_im, acc_sq = rest[7:11]
            scratch = rest[11:]
        slots = ((scratch[0:4], scratch[4:8]), (scratch[8:12], scratch[12:16]))
        turns = (scratch[16:18], scratch[18:20])
        base = fixed_ref[0] + plan_ref[0] * fixed_ref[1] + plan_ref[1] * fixed_ref[2]
        rate = ticks_ref[0] + plan_ref[0] * ticks_ref[1] + plan_ref[1] * ticks_ref[2]
        group = plan_ref[1]
        frames[pl.ds(0, PAD), :] = jnp.zeros((PAD, LANES), jnp.float32)
        for array in range(arrays):
            for item in range(depth):
                place = plan_ref[piece_at + array * depth + item]
                start = pl.multiple_of(PAD + place * Q, 8)
                frames[pl.ds(start, Q), :] = piece_refs[array][item, pl.ds(0, Q), :]
                if opening:
                    start = pl.multiple_of((place // BLOCKS) * PAD, 8)
                    drops[pl.ds(start, PAD), :] = piece_refs[array][item, pl.ds(Q, PAD), :]
        for array in range(len(notes)):
            for item in range(depth):
                place = plan_ref[note_at + array * depth + item]
                tile = note_refs[array][item]
                frames[pl.ds(pl.multiple_of((place + 1) * Q, 8), PAD), :] = tile
                drops[pl.ds(pl.multiple_of((place // BLOCKS) * PAD, 8), PAD), :] = tile
        for item in range(depth):
            at = pl.ds(pl.multiple_of((plan_ref[tail_at + item] + 1) * Q, 8), PAD)
            if opening:
                tails[item] = frames[at, :]
            else:
                frames[at, :] = tails[item]

        def make_stamps():
            def stamp_step(n, total):
                at = pl.ds(pl.multiple_of(n * PAD, 8), PAD)
                dropped = jnp.broadcast_to(drops[at, :][0:1], (PAD, LANES)).astype(jnp.int32)
                total = (total + dropped) & (PERIOD - 1)
                stamps[at, :] = total
                return total

            start = jnp.zeros((PAD, LANES), jnp.int32)
            lax.fori_loop(0, slabs, stamp_step, start, unroll=min(slabs, 16))

        if opening:
            acc_re[...] = jnp.zeros_like(acc_re)
            acc_im[...] = jnp.zeros_like(acc_im)
            acc_sq[...] = jnp.zeros_like(acc_sq)
            make_stamps()
        else:
            acc_re[...] = old_re[...]
            acc_im[...] = old_im[...]
            acc_sq[...] = old_sq[...]
        lane = lax.broadcasted_iota(jnp.int32, (Q, LANES), 1)
        left_half = lane < LANES // 2

        def channelize(places, side):
            targets = slots[side]
            at = pl.ds(pl.multiple_of((places[0] // BLOCKS) * PAD, 8), PAD)
            wide = jnp.concatenate([stamps[at, :]] * (rows // PAD), axis=0)
            cos_rows, sin_rows = cos_sin((base + rate * wide) & (TURN - 1))
            turns[side][0][...] = cos_rows
            turns[side][1][...] = sin_rows
            evens = []
            odds = []
            for place in places:
                start = pl.multiple_of(place * Q, Q)
                lags = [
                    frames[pl.ds(start + (PAD - 3 + lag), Q), :] * small_ref[lag : lag + 1]
                    for lag in range(4)
                ]
                evens.append(jnp.concatenate([lags[0] + lags[2], lags[1] + lags[3]], axis=1))
                odds.append(jnp.concatenate([lags[0] - lags[2], lags[1] - lags[3]], axis=1))
            both_even = split(jnp.concatenate(evens, axis=0))
            both_odd = split(jnp.concatenate(odds, axis=0))
            from_even = dot3(both_even, (even_h[group], even_l[group]))
            from_odd = dot3(both_odd, (odd_h[group], odd_l[group]))
            for index, slot in enumerate(targets):
                part = slice(index * Q, (index + 1) * Q)
                finish(cos_rows, sin_rows, slot, from_even[part], from_odd[part])

        def finish(cos_rows, sin_rows, slot, from_even, from_odd):
            rhs_h, rhs_l, center_re, center_im = slot
            row_k, row_l = 4 + pairs, 5 + pairs
            low_cos = cos_rows[row_k : row_k + 1]
            low_sin = sin_rows[row_k : row_k + 1] * small_ref[24:25]
            up_cos = cos_rows[row_l : row_l + 1]
            up_sin = sin_rows[row_l : row_l + 1]
            table_cos = small_ref[8:16] * up_cos - small_ref[16:24] * up_sin
            table_sin = small_ref[16:24] * up_cos + small_ref[8:16] * up_sin
            table_cos = jnp.concatenate([table_cos] * (Q // 8), axis=0)
            table_sin = jnp.concatenate([table_sin] * (Q // 8), axis=0)
            up_even, up_odd = from_even[:, :LANES], from_odd[:, :LANES]
            up_re = jnp.where(left_half, up_even, up_odd)
            up_im = pltpu.roll(jnp.where(left_half, up_odd, up_even), LANES // 2, 1)
            re_h, re_l = split(up_re * table_cos + up_im * table_sin)
            im_h, im_l = split(up_im * table_cos - up_re * table_sin)
            for ref, real, imag in ((rhs_h, re_h, im_h), (rhs_l, re_l, im_l)):
                ref[0:Q, 0:LW] = real
                ref[0:Q, LW : 2 * LW] = -imag
                ref[Q : 2 * Q, 0:LW] = imag
                ref[Q : 2 * Q, LW : 2 * LW] = real
            low = from_even[:, LANES:] + from_odd[:, LANES:]
            low = low * low_cos + pltpu.roll(low, LANES // 2, 1) * low_sin
            low = low.T * norm
            low_re, low_im = low[:width], low[width:]
            for part in range(4):
                at = slice(part * quarter, (part + 1) * quarter)
                c = cos_rows[part : part + 1]
                s = sin_rows[part : part + 1]
                center_re[at] = low_re[at] * c + low_im[at] * s
                center_im[at] = low_im[at] * c - low_re[at] * s

        def correlate(turn, slot):
            rhs_h, rhs_l, center_re, center_im = slot
            cos_rows = turn[0][...]
            sin_rows = turn[1][...]
            right = (rhs_h[...], rhs_l[...])
            group_size = min(pairs, 4)
            for base_pair in range(0, pairs, group_size):
                parts = []
                for pair in range(base_pair, base_pair + group_size):
                    c = cos_rows[4 + pair : 5 + pair]
                    s = sin_rows[4 + pair : 5 + pair]
                    t1 = center_re[...] * c
                    t2 = center_im[...] * s
                    t3 = center_im[...] * c
                    t4 = center_re[...] * s
                    parts.append(jnp.concatenate([t1 + t2, t3 - t4], axis=1))
                    parts.append(jnp.concatenate([t1 - t2, t3 + t4], axis=1))
                left = split(jnp.concatenate(parts, axis=0))
                total = dot3(left, right)
                for index in range(2 * group_size):
                    pair = base_pair + index // 2
                    at = (pairs - 1 - pair if index % 2 else pairs + pair) * width
                    put = slice(at, at + width)
                    re = total[index * width : (index + 1) * width, :LW]
                    im = total[index * width : (index + 1) * width, LW:]
                    acc_re[put] = acc_re[put] + re
                    acc_im[put] = acc_im[put] + im
                    acc_sq[put] = jnp.maximum(acc_sq[put], re * re + im * im)

        def block_at(index):
            return plan_ref[first_block + index]

        def work(first, side, more):
            if more:
                channelize((block_at(first + 2), block_at(first + 3)), 1 - side)
            for item in range(2):
                correlate(turns[side], slots[side][item])

        def step(index, carry):
            work(4 * index, 0, True)
            work(4 * index + 2, 1, True)
            return carry

        channelize((block_at(0), block_at(1)), 0)
        lax.fori_loop(0, count // 4 - 1, step, 0, unroll=count <= 16)
        work(count - 4, 0, True)
        work(count - 2, 1, False)
        if opening:
            return
        lanes = lax.broadcasted_iota(jnp.int32, (quarter, LW), 1)
        source = lax.shift_right_logical(lanes, 1) + (LW // 2) * (lanes & 1)

        def natural(value):
            return jnp.take_along_axis(value, source, axis=1, mode="promise_in_bounds")

        for bin_index in range(bins):
            for part, kappa in enumerate((0, 2, 1, 3)):
                first = bin_index * width + part * quarter
                take = slice(first, first + quarter)
                put = pl.ds(kappa, quarter, stride=4)
                held_ref[bin_index, put, :] = natural(jnp.sqrt(acc_sq[take]))
                coherent_ref[0, bin_index, put, :] = natural(acc_re[take] * blend)
                coherent_ref[1, bin_index, put, :] = natural(acc_im[take] * blend)

    vmem = pl.BlockSpec(memory_space=pltpu.VMEM)
    slot = [
        pltpu.VMEM((2 * Q, 2 * LW), jnp.bfloat16),
        pltpu.VMEM((2 * Q, 2 * LW), jnp.bfloat16),
        pltpu.VMEM((width, Q), jnp.float32),
        pltpu.VMEM((width, Q), jnp.float32),
    ]
    sums = [(bins * width, LW)] * 3
    if opening:
        shapes = sums + [(slabs * PAD, LANES), (depth, PAD, LANES)]
        scratch = [(PAD + blocks * Q, LANES), (slabs * PAD, LANES)]
    else:
        shapes = [(bins, width, LW), (2, bins, width, LW)]
        scratch = [(PAD + blocks * Q, LANES)] + sums
    work = 2 * 3 * count * NCH * NCH * (2 * Q + 2 * bins * width // 2)
    return pl.pallas_call(
        kernel,
        in_specs=[pl.BlockSpec(memory_space=pltpu.SMEM)] + [vmem] * (7 + inputs),
        out_specs=[vmem] * outputs,
        scratch_shapes=[pltpu.VMEM(shape, jnp.float32) for shape in scratch]
        + slot * 4
        + [pltpu.VMEM((rows, LANES), jnp.float32)] * 4,
        out_shape=[
            jax.ShapeDtypeStruct(shape, jnp.int32 if opening and index == 3 else jnp.float32)
            for index, shape in enumerate(shapes)
        ],
        compiler_params=pltpu.CompilerParams(vmem_limit_bytes=(PAD + blocks * Q) * 4 * LANES + 12 * 1024 * 1024),
        cost_estimate=pl.CostEstimate(flops=work, transcendentals=0, bytes_accessed=4 * 1024 * 1024),
        name="surfaces_first" if opening else "surfaces_last",
    )(
        plan,
        jnp.asarray(fixed),
        jnp.asarray(ticks),
        jnp.asarray(small),
        *[jnp.asarray(table) for table in weights],
        *pieces,
        *notes,
        *(() if opening else carried),
    )


def on_device(capture, dropped):
    slabs = lax.axis_size("slab")
    groups = lax.axis_size("grp")
    slab = lax.axis_index("slab")
    group = lax.axis_index("grp")
    axes = ("slab", "grp")
    total = slabs * groups
    outer = slabs // 4
    hops = capture.shape[1] // HOP
    own = capture.reshape(2, hops, HOP).transpose(1, 0, 2).reshape(hops, 2 * HOP)
    ticks = jnp.broadcast_to(dropped.astype(jnp.float32)[:, None], (PAD, LANES))
    own = jnp.concatenate([own, ticks], axis=0)[None]
    lead = NCH // HOP - 1

    def split_index(flat):
        return flat // (4 * groups), (flat // (2 * groups)) % 2, (flat // groups) % 2, flat % groups

    def joined(far, side, core, member):
        return ((far * 2 + side) * 2 + core) * groups + member

    def moved(array, by):
        pairs = []
        for flat in range(total):
            far, side, core, member = split_index(flat)
            target = joined(
                (far + by[0]) % outer, (side + by[1]) % 2, (core + by[2]) % 2, (member + by[3]) % groups
            )
            pairs.append((flat, target))
        return lax.ppermute(array, axes, pairs)

    line = [own]
    for step in range(1, outer):
        line.append(moved(own, (step, 0, 0, 0)))
    own_near = [moved(own, (0, 0, 0, member)) for member in range(1, groups)]
    own_far = moved(own, (0, 1, 0, 0))
    rest = jnp.concatenate(line[1:], axis=0)
    line = jnp.concatenate(line, axis=0)
    tiles = jnp.concatenate([line[:, hops : hops + PAD - lead], line[:, hops - lead : hops]], axis=1)
    note_steps = [(1, core, member) for core in range(2) for member in range(groups)]
    notes = []
    for by in note_steps:
        notes.append(moved(tiles, (0,) + by))
    near = [moved(rest, (0, 0, 0, member)) for member in range(1, groups)]
    far = [moved(rest, (0, 1, 0, 0))]
    near = [line] + [jnp.concatenate(pair, axis=0) for pair in zip(own_near, near)]
    far = [jnp.concatenate([own_far, far[0]], axis=0)]
    far += [moved(piece, (0, 1, 0, 0)) for piece in near[1:]]
    near_steps = [(0, 0, member) for member in range(groups)]
    far_steps = [(1, 0, member) for member in range(groups)]
    cores = []
    for piece in near:
        cores.append(moved(piece, (0, 0, 1, 0)))
    near += cores
    near_steps += [(side, 1, member) for side, _, member in near_steps]
    me_far, me_side, me_core, me_member = split_index(slab * groups + group)

    def places(steps):
        return [
            joined(
                (me_far - step) % outer,
                (me_side - side) % 2,
                (me_core - core) % 2,
                (me_member - member) % groups,
            )
            for side, core, member in steps
            for step in range(outer)
        ]

    first_blocks = []
    last_blocks = []
    for step in range(outer):
        for core in range(2):
            for member in range(groups):
                first_blocks.append(joined(step, me_side, core, member))
                last_blocks.append(joined(step, 1 - me_side, core, member))
    tail_places = [joined(step, me_side, 1, groups - 1) for step in range(outer)]
    far_steps += [(side, 1, member) for side, _, member in far_steps]
    parts = [places(near_steps), places(far_steps), places(note_steps), tail_places]
    parts += [first_blocks, last_blocks]
    begins = np.cumsum([2] + [len(part) for part in parts])
    near_at, far_at, note_at, tail_at, first_at, last_at = (int(at) for at in begins[:-1])
    plan = [slab, group] + sum(parts, [])
    plan = jnp.stack([jnp.asarray(value, jnp.int32) for value in plan])
    spots = (near_at, note_at, tail_at, first_at)
    carried = surfaces(plan, spots, near, slabs, groups, len(first_blocks), notes=notes)
    far += [moved(far[0], (0, 0, 1, 0))]
    far += [moved(piece, (0, 0, 1, 0)) for piece in far[1:groups]]
    spots = (far_at, note_at, tail_at, last_at)
    held, coherent = surfaces(
        plan, spots, far, slabs, groups, len(last_blocks), carried=carried
    )
    return held, coherent


def solution(mesh):
    in_specs = (P(None, ("slab", "grp")), P("slab"))
    out_specs = (P("slab", "grp", None), P(None, "slab", "grp", None))

    return jax.shard_map(
        on_device, mesh=mesh, in_specs=in_specs, out_specs=out_specs, check_vma=False
    )
```

```python
import math

import jax
import jax.numpy as jnp
import ml_dtypes
import numpy as np
from jax import lax
from jax.experimental import pallas as pl
from jax.experimental.pallas import tpu as pltpu
from jax.sharding import PartitionSpec as P


NCH = 256
HOP = 64
KW = 128
LW = 128
Q = 128
BLOCKS = 2
PERIOD = Q * HOP
TURN = 2 * PERIOD
LANES = 128
PAD = 8


def halves(table):
    high = table.astype(ml_dtypes.bfloat16)
    low = (table - high.astype(np.float64)).astype(ml_dtypes.bfloat16)
    return high, low


def lower_order(width):
    quarter = width // 4
    return np.concatenate([4 * np.arange(quarter) + kappa for kappa in (0, 2, 1, 3)])


def upper_order():
    return np.concatenate([np.arange(0, LW, 2), np.arange(1, LW, 2)])


def window_rows():
    taps = np.arange(NCH)
    window = 0.5 - 0.5 * np.cos(2.0 * np.pi * taps / NCH)
    scaled = window / np.sqrt(np.sum(window * window))
    rows = np.zeros((8, LANES))
    for lag in range(NCH // HOP):
        piece = scaled[lag * HOP : (lag + 1) * HOP]
        rows[lag] = np.concatenate([piece, piece])
    return rows.astype(np.float32)


def channel_tables(groups):
    width = KW // groups
    half = width // 2
    taps = np.arange(NCH // 2)
    even = np.zeros((groups, NCH, NCH))
    odd = np.zeros((groups, NCH, NCH))

    def columns(channels):
        turns = 2.0 * np.pi * (taps[:, None] * channels[None, :] % NCH) / NCH
        cosine, sine = np.cos(turns), np.sin(turns)
        real = np.concatenate([cosine[:HOP], sine[:HOP], cosine[HOP:], sine[HOP:]])
        imag = np.concatenate([-sine[:HOP], cosine[:HOP], -sine[HOP:], cosine[HOP:]])
        return real, imag

    upper = KW + upper_order()
    for group in range(groups):
        lower = group * width + lower_order(width)
        real, imag = columns(upper[: LW // 2])
        even[group, :, 0:64], even[group, :, 64:128] = real, imag
        real, imag = columns(upper[LW // 2 :])
        odd[group, :, 0:64], odd[group, :, 64:128] = imag, real
        real, imag = columns(lower[:half])
        even[group, :, 128 : 128 + half] = real
        even[group, :, 192 : 192 + half] = imag
        real, imag = columns(lower[half:])
        odd[group, :, 128 + half : 128 + width] = real
        odd[group, :, 192 + half : 192 + width] = imag
    return halves(even) + halves(odd)


def turn_tables(bins, width):
    pairs = bins // 2
    rows = -(-(6 + pairs) // 8) * 8
    frame = np.arange(LANES)
    fixed = np.zeros((3, rows, LANES), np.int64)
    ticks = np.zeros((3, rows, LANES), np.int64)
    for place, kappa in enumerate((0, 2, 1, 3)):
        ticks[0, place] = bins - 1
        ticks[1, place] = 2 * bins
        fixed[0, place] = (bins - 1) * HOP * frame + (TURN // 4) * kappa * frame
        fixed[1, place] = 2 * bins * HOP * frame
    for pair in range(pairs):
        ticks[0, 4 + pair] = 2 * pair + 1
        fixed[0, 4 + pair] = (2 * pair + 1) * HOP * frame
    order = lower_order(width)
    scale = TURN // NCH
    ticks[0, 4 + pairs] = scale * np.concatenate([order, order])
    ticks[2, 4 + pairs] = scale * width
    ticks[0, 5 + pairs] = scale * (KW + upper_order())
    return fixed.astype(np.int32), ticks.astype(np.int32)


def cos_sin(angle):
    shifted = angle + TURN // 8
    quadrant = lax.shift_right_logical(shifted, int(math.log2(TURN // 4))) & 3
    remain = (shifted & (TURN // 4 - 1)) - TURN // 8
    x = remain.astype(jnp.float32) * np.float32(2.0 * math.pi / TURN)
    y = x * x
    sine = x * (1.0 + y * (-1.0 / 6 + y * (1.0 / 120 + y * (-1.0 / 5040 + y * (1.0 / 362880)))))
    cosine = 1.0 + y * (-0.5 + y * (1.0 / 24 + y * (-1.0 / 720 + y * (1.0 / 40320))))
    swap = (quadrant & 1) == 1
    out_cos = jnp.where(swap, sine, cosine)
    out_sin = jnp.where(swap, cosine, sine)
    out_cos = jnp.where((quadrant == 1) | (quadrant == 2), -out_cos, out_cos)
    out_sin = jnp.where(quadrant >= 2, -out_sin, out_sin)
    return out_cos, out_sin


def split(value):
    high = value.astype(jnp.bfloat16)
    low = (value - high.astype(jnp.float32)).astype(jnp.bfloat16)
    return high, low


def dot32(left, right):
    return lax.dot_general(
        left, right, (((1,), (0,)), ((), ())), preferred_element_type=jnp.float32
    )


def dot3(left, right):
    return dot32(left[0], right[0]) + dot32(left[1], right[0]) + dot32(left[0], right[1])


def small_table(width):
    order = KW + upper_order()
    phase = (np.arange(8)[:, None] * order[None, :]) % 4
    quarter_cos = np.array([1.0, 0.0, -1.0, 0.0])[phase]
    quarter_sin = np.array([0.0, 1.0, 0.0, -1.0])[phase]
    sign = np.where(np.arange(LANES) < width, 1.0, -1.0)[None, :]
    parts = [window_rows(), quarter_cos, quarter_sin, np.tile(sign, (8, 1))]
    return np.concatenate(parts).astype(np.float32)


def surfaces(plan, spots, pieces, slabs, groups, count, notes=(), carried=None):
    piece_at, note_at, tail_at, first_block = spots
    bins = Q // slabs
    pairs = bins // 2
    width = KW // groups
    quarter = width // 4
    blocks = slabs * BLOCKS
    fixed, ticks = turn_tables(bins, width)
    rows = fixed.shape[1]
    weights = channel_tables(groups)
    small = small_table(width)
    arrays = len(pieces)
    depth = pieces[0].shape[0]
    norm = 1.0 / math.sqrt(Q)
    blend = 1.0 / math.sqrt(slabs * BLOCKS)
    opening = carried is None
    inputs = arrays + len(notes) + (0 if opening else 5)
    outputs = 5 if opening else 2

    def kernel(plan_ref, fixed_ref, ticks_ref, small_ref, even_h, even_l, odd_h, odd_l, *rest):
        piece_refs = rest[:arrays]
        note_refs = rest[arrays : arrays + len(notes)]
        out_refs = rest[inputs : inputs + outputs]
        rest = rest[inputs + outputs :] if opening else rest[arrays:]
        if opening:
            acc_re, acc_im, acc_sq, stamps, tails = out_refs
            frames, drops = rest[:2]
            scratch = rest[2:]
        else:
            old_re, old_im, old_sq, stamps, tails = rest[:5]
            held_ref, coherent_ref = out_refs
            frames, acc_re, acc_im, acc_sq = rest[7:11]
            scratch = rest[11:]
        slots = ((scratch[0:4], scratch[4:8]), (scratch[8:12], scratch[12:16]))
        turns = (scratch[16:18], scratch[18:20])
        base = fixed_ref[0] + plan_ref[0] * fixed_ref[1] + plan_ref[1] * fixed_ref[2]
        rate = ticks_ref[0] + plan_ref[0] * ticks_ref[1] + plan_ref[1] * ticks_ref[2]
        group = plan_ref[1]
        frames[pl.ds(0, PAD), :] = jnp.zeros((PAD, LANES), jnp.float32)
        for array in range(arrays):
            for item in range(depth):
                place = plan_ref[piece_at + array * depth + item]
                start = pl.multiple_of(PAD + place * Q, 8)
                frames[pl.ds(start, Q), :] = piece_refs[array][item, pl.ds(0, Q), :]
                if opening:
                    start = pl.multiple_of((place // BLOCKS) * PAD, 8)
                    drops[pl.ds(start, PAD), :] = piece_refs[array][item, pl.ds(Q, PAD), :]
        for array in range(len(notes)):
            for item in range(depth):
                place = plan_ref[note_at + array * depth + item]
                tile = note_refs[array][item]
                frames[pl.ds(pl.multiple_of((place + 1) * Q, 8), PAD), :] = tile
                drops[pl.ds(pl.multiple_of((place // BLOCKS) * PAD, 8), PAD), :] = tile
        for item in range(depth):
            at = pl.ds(pl.multiple_of((plan_ref[tail_at + item] + 1) * Q, 8), PAD)
            if opening:
                tails[item] = frames[at, :]
            else:
                frames[at, :] = tails[item]

        def make_stamps():
            def stamp_step(n, total):
                at = pl.ds(pl.multiple_of(n * PAD, 8), PAD)
                dropped = jnp.broadcast_to(drops[at, :][0:1], (PAD, LANES)).astype(jnp.int32)
                total = (total + dropped) & (PERIOD - 1)
                stamps[at, :] = total
                return total

            start = jnp.zeros((PAD, LANES), jnp.int32)
            lax.fori_loop(0, slabs, stamp_step, start, unroll=min(slabs, 16))

        flat = count <= 16
        if opening:
            if not flat:
                acc_re[...] = jnp.zeros_like(acc_re)
                acc_im[...] = jnp.zeros_like(acc_im)
                acc_sq[...] = jnp.zeros_like(acc_sq)
            make_stamps()
        elif not flat:
            acc_re[...] = old_re[...]
            acc_im[...] = old_im[...]
            acc_sq[...] = old_sq[...]
        lane = lax.broadcasted_iota(jnp.int32, (Q, LANES), 1)
        left_half = lane < LANES // 2

        def channelize(places, side):
            targets = slots[side]
            at = pl.ds(pl.multiple_of((places[0] // BLOCKS) * PAD, 8), PAD)
            wide = jnp.concatenate([stamps[at, :]] * (rows // PAD), axis=0)
            cos_rows, sin_rows = cos_sin((base + rate * wide) & (TURN - 1))
            turns[side][0][...] = cos_rows
            turns[side][1][...] = sin_rows
            evens = []
            odds = []
            for place in places:
                start = pl.multiple_of(place * Q, Q)
                lags = [
                    frames[pl.ds(start + (PAD - 3 + lag), Q), :] * small_ref[lag : lag + 1]
                    for lag in range(4)
                ]
                evens.append(jnp.concatenate([lags[0] + lags[2], lags[1] + lags[3]], axis=1))
                odds.append(jnp.concatenate([lags[0] - lags[2], lags[1] - lags[3]], axis=1))
            both_even = split(jnp.concatenate(evens, axis=0))
            both_odd = split(jnp.concatenate(odds, axis=0))
            from_even = dot3(both_even, (even_h[group], even_l[group]))
            from_odd = dot3(both_odd, (odd_h[group], odd_l[group]))
            for index, slot in enumerate(targets):
                part = slice(index * Q, (index + 1) * Q)
                finish(cos_rows, sin_rows, slot, from_even[part], from_odd[part])

        def finish(cos_rows, sin_rows, slot, from_even, from_odd):
            rhs_h, rhs_l, center_re, center_im = slot
            row_k, row_l = 4 + pairs, 5 + pairs
            low_cos = cos_rows[row_k : row_k + 1]
            low_sin = sin_rows[row_k : row_k + 1] * small_ref[24:25]
            up_cos = cos_rows[row_l : row_l + 1]
            up_sin = sin_rows[row_l : row_l + 1]
            table_cos = small_ref[8:16] * up_cos - small_ref[16:24] * up_sin
            table_sin = small_ref[16:24] * up_cos + small_ref[8:16] * up_sin
            table_cos = jnp.concatenate([table_cos] * (Q // 8), axis=0)
            table_sin = jnp.concatenate([table_sin] * (Q // 8), axis=0)
            up_even, up_odd = from_even[:, :LANES], from_odd[:, :LANES]
            up_re = jnp.where(left_half, up_even, up_odd)
            up_im = pltpu.roll(jnp.where(left_half, up_odd, up_even), LANES // 2, 1)
            re_h, re_l = split(up_re * table_cos + up_im * table_sin)
            im_h, im_l = split(up_im * table_cos - up_re * table_sin)
            for ref, real, imag in ((rhs_h, re_h, im_h), (rhs_l, re_l, im_l)):
                ref[0:Q, 0:LW] = real
                ref[0:Q, LW : 2 * LW] = -imag
                ref[Q : 2 * Q, 0:LW] = imag
                ref[Q : 2 * Q, LW : 2 * LW] = real
            low = from_even[:, LANES:] + from_odd[:, LANES:]
            low = low * low_cos + pltpu.roll(low, LANES // 2, 1) * low_sin
            low = low.T * norm
            low_re, low_im = low[:width], low[width:]
            for part in range(4):
                at = slice(part * quarter, (part + 1) * quarter)
                c = cos_rows[part : part + 1]
                s = sin_rows[part : part + 1]
                center_re[at] = low_re[at] * c + low_im[at] * s
                center_im[at] = low_im[at] * c - low_re[at] * s

        def correlate(turn, slot, fresh):
            rhs_h, rhs_l, center_re, center_im = slot
            cos_rows = turn[0][...]
            sin_rows = turn[1][...]
            right = (rhs_h[...], rhs_l[...])
            group_size = min(pairs, 4)
            for base_pair in range(0, pairs, group_size):
                parts = []
                for pair in range(base_pair, base_pair + group_size):
                    c = cos_rows[4 + pair : 5 + pair]
                    s = sin_rows[4 + pair : 5 + pair]
                    t1 = center_re[...] * c
                    t2 = center_im[...] * s
                    t3 = center_im[...] * c
                    t4 = center_re[...] * s
                    parts.append(jnp.concatenate([t1 + t2, t3 - t4], axis=1))
                    parts.append(jnp.concatenate([t1 - t2, t3 + t4], axis=1))
                left = split(jnp.concatenate(parts, axis=0))
                total = dot3(left, right)
                for index in range(2 * group_size):
                    pair = base_pair + index // 2
                    at = (pairs - 1 - pair if index % 2 else pairs + pair) * width
                    put = slice(at, at + width)
                    re = total[index * width : (index + 1) * width, :LW]
                    im = total[index * width : (index + 1) * width, LW:]
                    square = re * re + im * im
                    if fresh and opening:
                        acc_re[put], acc_im[put], acc_sq[put] = re, im, square
                        continue
                    held = (old_re, old_im, old_sq) if fresh else (acc_re, acc_im, acc_sq)
                    acc_re[put] = held[0][put] + re
                    acc_im[put] = held[1][put] + im
                    acc_sq[put] = jnp.maximum(held[2][put], square)

        def block_at(index):
            return plan_ref[first_block + index]

        def work(first, side, more, start=False):
            if more:
                channelize((block_at(first + 2), block_at(first + 3)), 1 - side)
            for item in range(2):
                correlate(turns[side], slots[side][item], start and item == 0)

        def step(index, carry):
            work(4 * index, 0, True)
            work(4 * index + 2, 1, True)
            return carry

        channelize((block_at(0), block_at(1)), 0)
        if flat:
            for first in range(0, count - 4, 2):
                work(first, first // 2 % 2, True, start=first == 0)
        else:
            lax.fori_loop(0, count // 4 - 1, step, 0)
        work(count - 4, 0, True, start=flat and count == 4)
        work(count - 2, 1, False)
        if opening:
            return
        lanes = lax.broadcasted_iota(jnp.int32, (quarter, LW), 1)
        source = lax.shift_right_logical(lanes, 1) + (LW // 2) * (lanes & 1)

        def natural(value):
            return jnp.take_along_axis(value, source, axis=1, mode="promise_in_bounds")

        for bin_index in range(bins):
            for part, kappa in enumerate((0, 2, 1, 3)):
                first = bin_index * width + part * quarter
                take = slice(first, first + quarter)
                put = pl.ds(kappa, quarter, stride=4)
                held_ref[bin_index, put, :] = natural(jnp.sqrt(acc_sq[take]))
                coherent_ref[0, bin_index, put, :] = natural(acc_re[take] * blend)
                coherent_ref[1, bin_index, put, :] = natural(acc_im[take] * blend)

    vmem = pl.BlockSpec(memory_space=pltpu.VMEM)
    slot = [
        pltpu.VMEM((2 * Q, 2 * LW), jnp.bfloat16),
        pltpu.VMEM((2 * Q, 2 * LW), jnp.bfloat16),
        pltpu.VMEM((width, Q), jnp.float32),
        pltpu.VMEM((width, Q), jnp.float32),
    ]
    sums = [(bins * width, LW)] * 3
    if opening:
        shapes = sums + [(slabs * PAD, LANES), (depth, PAD, LANES)]
        scratch = [(PAD + blocks * Q, LANES), (slabs * PAD, LANES)]
    else:
        shapes = [(bins, width, LW), (2, bins, width, LW)]
        scratch = [(PAD + blocks * Q, LANES)] + sums
    work = 2 * 3 * count * NCH * NCH * (2 * Q + 2 * bins * width // 2)
    return pl.pallas_call(
        kernel,
        in_specs=[pl.BlockSpec(memory_space=pltpu.SMEM)] + [vmem] * (7 + inputs),
        out_specs=[vmem] * outputs,
        scratch_shapes=[pltpu.VMEM(shape, jnp.float32) for shape in scratch]
        + slot * 4
        + [pltpu.VMEM((rows, LANES), jnp.float32)] * 4,
        out_shape=[
            jax.ShapeDtypeStruct(shape, jnp.int32 if opening and index == 3 else jnp.float32)
            for index, shape in enumerate(shapes)
        ],
        compiler_params=pltpu.CompilerParams(vmem_limit_bytes=(PAD + blocks * Q) * 4 * LANES + 12 * 1024 * 1024),
        cost_estimate=pl.CostEstimate(flops=work, transcendentals=0, bytes_accessed=4 * 1024 * 1024),
        name="surfaces_first" if opening else "surfaces_last",
    )(
        plan,
        jnp.asarray(fixed),
        jnp.asarray(ticks),
        jnp.asarray(small),
        *[jnp.asarray(table) for table in weights],
        *pieces,
        *notes,
        *(() if opening else carried),
    )


def on_device(capture, dropped):
    slabs = lax.axis_size("slab")
    groups = lax.axis_size("grp")
    slab = lax.axis_index("slab")
    group = lax.axis_index("grp")
    axes = ("slab", "grp")
    total = slabs * groups
    outer = slabs // 4
    hops = capture.shape[1] // HOP
    own = capture.reshape(2, hops, HOP).transpose(1, 0, 2).reshape(hops, 2 * HOP)
    ticks = jnp.broadcast_to(dropped.astype(jnp.float32)[:, None], (PAD, LANES))
    own = jnp.concatenate([own, ticks], axis=0)[None]
    lead = NCH // HOP - 1

    def split_index(flat):
        return flat // (4 * groups), (flat // (2 * groups)) % 2, (flat // groups) % 2, flat % groups

    def joined(far, side, core, member):
        return ((far * 2 + side) * 2 + core) * groups + member

    def moved(array, by):
        pairs = []
        for flat in range(total):
            far, side, core, member = split_index(flat)
            target = joined(
                (far + by[0]) % outer, (side + by[1]) % 2, (core + by[2]) % 2, (member + by[3]) % groups
            )
            pairs.append((flat, target))
        return lax.ppermute(array, axes, pairs)

    line = [own]
    for step in range(1, outer):
        line.append(moved(own, (step, 0, 0, 0)))
    own_near = [moved(own, (0, 0, 0, member)) for member in range(1, groups)]
    own_far = moved(own, (0, 1, 0, 0))
    rest = jnp.concatenate(line[1:], axis=0)
    line = jnp.concatenate(line, axis=0)
    tiles = jnp.concatenate([line[:, hops : hops + PAD - lead], line[:, hops - lead : hops]], axis=1)
    note_steps = [(1, core, member) for core in range(2) for member in range(groups)]
    notes = []
    for by in note_steps:
        notes.append(moved(tiles, (0,) + by))
    near = [moved(rest, (0, 0, 0, member)) for member in range(1, groups)]
    far = [moved(rest, (0, 1, 0, 0))]
    near = [line] + [jnp.concatenate(pair, axis=0) for pair in zip(own_near, near)]
    far = [jnp.concatenate([own_far, far[0]], axis=0)]
    far += [moved(piece, (0, 1, 0, 0)) for piece in near[1:]]
    near_steps = [(0, 0, member) for member in range(groups)]
    far_steps = [(1, 0, member) for member in range(groups)]
    cores = []
    for piece in near:
        cores.append(moved(piece, (0, 0, 1, 0)))
    near += cores
    near_steps += [(side, 1, member) for side, _, member in near_steps]
    me_far, me_side, me_core, me_member = split_index(slab * groups + group)

    def places(steps):
        return [
            joined(
                (me_far - step) % outer,
                (me_side - side) % 2,
                (me_core - core) % 2,
                (me_member - member) % groups,
            )
            for side, core, member in steps
            for step in range(outer)
        ]

    first_blocks = []
    last_blocks = []
    for step in range(outer):
        for core in range(2):
            for member in range(groups):
                first_blocks.append(joined(step, me_side, core, member))
                last_blocks.append(joined(step, 1 - me_side, core, member))
    tail_places = [joined(step, me_side, 1, groups - 1) for step in range(outer)]
    far_steps += [(side, 1, member) for side, _, member in far_steps]
    parts = [places(near_steps), places(far_steps), places(note_steps), tail_places]
    parts += [first_blocks, last_blocks]
    begins = np.cumsum([2] + [len(part) for part in parts])
    near_at, far_at, note_at, tail_at, first_at, last_at = (int(at) for at in begins[:-1])
    plan = [slab, group] + sum(parts, [])
    plan = jnp.stack([jnp.asarray(value, jnp.int32) for value in plan])
    spots = (near_at, note_at, tail_at, first_at)
    carried = surfaces(plan, spots, near, slabs, groups, len(first_blocks), notes=notes)
    far += [moved(far[0], (0, 0, 1, 0))]
    far += [moved(piece, (0, 0, 1, 0)) for piece in far[1:groups]]
    spots = (far_at, note_at, tail_at, last_at)
    held, coherent = surfaces(
        plan, spots, far, slabs, groups, len(last_blocks), carried=carried
    )
    return held, coherent


def solution(mesh):
    in_specs = (P(None, ("slab", "grp")), P("slab"))
    out_specs = (P("slab", "grp", None), P(None, "slab", "grp", None))

    return jax.shard_map(
        on_device, mesh=mesh, in_specs=in_specs, out_specs=out_specs, check_vma=False
    )
```
